32 devices in a mesh: shard: 16 (over z, y, x), rep: 2 (over core).
Axes of the slice: x: 2, y: 2, z: 4, core: 2. Of those that a mesh axis runs over, the one named last changes fastest.
Arguments:
- tokens: float32 [32, 512, 1024], P(('shard', 'rep')), may hold values from -6 to 6
- segment_ids: int32 [32, 512], P(('shard', 'rep')), may hold values from 0 to 7, never falling along the last dimension, each value on 1 to 256 neighbouring positions
- valid_lengths: int32 [32], P(('shard', 'rep')), may hold values from 256 to 512
- qkv_weight: float32 [1024, 3072], P('shard'), may hold values from -0.1875 to 0.1875
- query_bias: float32 [1024], P('shard'), may hold values from -3 to 3
- value_bias: float32 [1024], P('shard'), may hold values from -3 to 3
- proj_weight: float32 [1024, 1024], P('shard'), may hold values from -0.5 to 0.5
- proj_bias: float32 [1024], P('shard'), may hold values from -3 to 3
- first_gain: float32 [1024], P('shard'), may hold values from 0.25 to 1.75
- first_shift: float32 [1024], P('shard'), may hold values from -3 to 3
- up_weight: float32 [1024, 4096], P('shard'), may hold values from -0.1875 to 0.1875
- up_bias: float32 [4096], P('shard'), may hold values from -3 to 3
- down_weight: float32 [4096, 1024], P('shard'), may hold values from -0.09375 to 0.09375
- down_bias: float32 [1024], P('shard'), may hold values from -3 to 3
- second_gain: float32 [1024], P('shard'), may hold values from 0.25 to 1.75
- second_shift: float32 [1024], P('shard'), may hold values from -3 to 3
- cotangent: float32 [32, 512, 1024], P(('shard', 'rep')), may hold values from -6 to 6
Outputs:
- layer_out: float32 [32, 512, 1024], P(('shard', 'rep'))
- tokens_grad: float32 [32, 512, 1024], P(('shard', 'rep'))
- qkv_grad: float32 [1024, 3072], P('shard')
- query_bias_grad: float32 [1024], P('shard')
- value_bias_grad: float32 [1024], P('shard')
- proj_grad: float32 [1024, 1024], P('shard')
- proj_bias_grad: float32 [1024], P('shard')
- first_gain_grad: float32 [1024], P('shard')
- first_shift_grad: float32 [1024], P('shard')
- up_grad: float32 [1024, 4096], P('shard')
- up_bias_grad: float32 [4096], P('shard')
- down_grad: float32 [4096, 1024], P('shard')
- down_bias_grad: float32 [1024], P('shard')
- second_gain_grad: float32 [1024], P('shard')
- second_shift_grad: float32 [1024], P('shard')
The draws below stay inside these ranges and needn't reach their ends.
Inputs may be any that keep to these rules, and one draw needn't show every extreme that they name: `segment_ids`: segment ids never fall along a sequence; heavy-tailed document sizes, one document of 256 tokens in each sequence.
All inputs are finite; a program needn't handle non-finite values.
Results may differ from the reference program's by a relative error of at most 0.0003.
Values sent between devices are 32-bit elements; how exact they have to be, the bound alone decides.
A program may use at most 256 MiB of HBM per device.

```python
import math
import jax
import jax.numpy as jnp
import numpy as np
from jax import lax

D = 1024
H = 16
HD = 64
FF = 4096
SEQ_LEN = 512
SEQS = 32
TOKENS = 16384


def with_ends(array, stream_key, smallest, largest):
    longest = array.shape.index(max(array.shape))
    spots = []
    for shift in (0, 1):
        where = [jax.random.randint(jax.random.fold_in(stream_key, axis), (), 0, length) for axis, length in enumerate(array.shape)]
        where[longest] = (where[longest] + shift) % array.shape[longest]
        spots.append(tuple(where))
    return array.at[spots[0]].set(smallest).at[spots[1]].set(largest)


def levels(stream_key, extent, shards, smallest, largest):
    def one(position, parts):
        draws = jax.random.uniform(jax.random.fold_in(jax.random.fold_in(stream_key, 6), position), (parts,), jnp.float32, smallest / len(shards), largest / len(shards))
        return jnp.repeat(jnp.exp(draws), extent[position] // parts).reshape((-1,) + (1,) * (len(extent) - position - 1))

    level = one(*shards[0])
    for cut in shards[1:]:
        level = level * one(*cut)
    return level


def length_profile(count, total, limit, lean):
    loads = [(1 << 20) // math.isqrt(standing ** lean) + 1 for standing in range(2, count + 1)]
    surplus, given = total - limit - (count - 1), [1] * (count - 1)
    while surplus > 0:
        movable = [i for i in range(count - 1) if given[i] < limit]
        whole, left = sum([loads[i] for i in movable]), surplus
        for i in movable:
            more = min(limit - given[i], max(1, left * loads[i] // whole), surplus)
            given[i] = given[i] + more
            surplus = surplus - more
    return np.array([limit] + given)


def ragged(own_key, number_of, total, most, slope):
    if number_of == 2:
        one = jax.random.randint(own_key, (), max(1, total - most), min(most, total - 1) + 1)
        return jnp.stack([one, total - one])
    sizes = jnp.asarray(length_profile(number_of, total, most, slope), jnp.int32)
    pairs = (number_of - 1) // 2
    source_of, receiver = sizes[1:1 + 2 * pairs:2], sizes[2:2 + 2 * pairs:2]
    room = jnp.minimum(source_of - 1, most - receiver)
    passed = jax.random.randint(jax.random.fold_in(own_key, 1), (pairs,), 0, 1 << 20) % (room + 1)
    sizes = sizes.at[1:1 + 2 * pairs:2].set(source_of - passed).at[2:2 + 2 * pairs:2].set(receiver + passed)
    return sizes[jax.random.permutation(jax.random.fold_in(own_key, 2), number_of)]


def centred(rng, extent, deviation, limit, split=(), kind=jnp.bfloat16):
    entries = deviation * jax.random.normal(rng, extent, jnp.float32)
    if split:
        entries = entries * levels(rng, extent, split, -0.22, 0.18)
    return jnp.clip(entries, -limit, limit).astype(kind)


def setup_inputs(seed: int = 0) -> dict:
    key_list = jax.random.split(jax.random.key(seed), 18)
    return {
        "tokens": centred(key_list[0], (SEQS, SEQ_LEN, D), 1.0, 6.0, ((0, 32),), jnp.float32),
        "segment_ids": jax.vmap(lambda own: jnp.searchsorted(jnp.cumsum(ragged(own, max(4, SEQ_LEN // 64), SEQ_LEN, SEQ_LEN // 2, 2)), jnp.arange(SEQ_LEN), side="right"))(jax.random.split(key_list[1], SEQS)).reshape((SEQS, SEQ_LEN)).astype(jnp.int32),
        "valid_lengths": with_ends(jax.random.randint(key_list[2], (SEQS,), SEQ_LEN // 2, SEQ_LEN + 1), jax.random.fold_in(key_list[2], 1), SEQ_LEN // 2, SEQ_LEN).astype(jnp.int32),
        "qkv_weight": centred(key_list[3], (D, 3 * D), D ** -0.5, 0.1875, ((0, 16),), jnp.float32),
        "query_bias": centred(key_list[4], (D,), 0.5, 3.0, ((0, 16),), jnp.float32),
        "value_bias": centred(key_list[5], (D,), 0.5, 3.0, ((0, 16),), jnp.float32),
        "proj_weight": centred(key_list[6], (D, D), (D // 8) ** -0.5, 0.5, ((0, 16),), jnp.float32),
        "proj_bias": centred(key_list[7], (D,), 0.5, 3.0, ((0, 16),), jnp.float32),
        "first_gain": jnp.clip(1.0 + 0.15 * jax.random.normal(key_list[8], (D,), jnp.float32), 0.25, 1.75),
        "first_shift": centred(key_list[9], (D,), 0.5, 3.0, ((0, 16),), jnp.float32),
        "up_weight": centred(key_list[10], (D, FF), D ** -0.5, 0.1875, ((0, 16),), jnp.float32),
        "up_bias": centred(key_list[11], (FF,), 0.5, 3.0, ((0, 16),), jnp.float32),
        "down_weight": centred(key_list[12], (FF, D), FF ** -0.5, 0.09375, ((0, 16),), jnp.float32),
        "down_bias": centred(key_list[13], (D,), 0.5, 3.0, ((0, 16),), jnp.float32),
        "second_gain": jnp.clip(1.0 + 0.15 * jax.random.normal(key_list[14], (D,), jnp.float32), 0.25, 1.75),
        "second_shift": centred(key_list[15], (D,), 0.5, 3.0, ((0, 16),), jnp.float32),
        "cotangent": centred(key_list[16], (SEQS, SEQ_LEN, D), 1.0, 6.0, ((0, 32),), jnp.float32),
    }


HIGHEST = lax.Precision.HIGHEST
EPSILON = 1e-05
MASKED = -1000000000.0

@jax.custom_vjp
def low(v):
    return lax.optimization_barrier(v.astype(jnp.bfloat16)).astype(jnp.float32)

@jax.custom_vjp
def low_back(v):
    return v

def low_keep(v):
    return (low(v), None)

def low_pass(kept, grad):
    return (grad,)

def back_keep(v):
    return (v, None)

def back_low(kept, grad):
    return (low(grad),)
low.defvjp(low_keep, low_pass)
low_back.defvjp(back_keep, back_low)

def matmul(left, right):
    return jnp.dot(left, right, precision=HIGHEST)

def layer_norm(values, gains, offset):
    center = values - lax.optimization_barrier(jnp.mean(values, axis=-1, keepdims=True))
    inverse = lax.rsqrt(lax.optimization_barrier(jnp.mean(center * center, axis=-1, keepdims=True)) + EPSILON)
    return center * inverse * gains + offset

def attend_packed(packed):
    queries, key_rows, val_rows, seg_row, valid_len = packed
    length = queries.shape[0]
    queries = queries.reshape(length, H, HD)
    key_rows = key_rows.reshape(length, H, HD)
    val_rows = val_rows.reshape(length, H, HD)
    scores = jnp.einsum('qhd,khd->hqk', queries, key_rows, precision=HIGHEST) / math.sqrt(HD)
    places = jnp.arange(length, dtype=jnp.int32)
    allowed = (seg_row[:, None] == seg_row[None, :]) & ((places[None, :] < valid_len) | (places[:, None] == places[None, :]))
    scores = jnp.where(allowed[None], scores, MASKED)
    probs = jax.nn.softmax(scores, axis=-1)
    context = jnp.einsum('hqk,khd->qhd', probs, val_rows, precision=HIGHEST)
    return context.reshape(length, H * HD)

def forward(rows_in, segments, lengths, qkv_weight, query_bias, value_bias, proj_weight, proj_bias, first_gain, first_shift, up_weight, up_bias, down_weight, down_bias, second_gain, second_shift):
    amount, length, model_dim = rows_in.shape
    row_count = amount * length
    flat_rows = rows_in.reshape(row_count, model_dim)
    mixed_qkv = matmul(flat_rows, qkv_weight)
    queries = (mixed_qkv[:, :model_dim] + query_bias).reshape(amount, length, model_dim)
    key_rows = mixed_qkv[:, model_dim:2 * model_dim].reshape(amount, length, model_dim)
    val_rows = (mixed_qkv[:, 2 * model_dim:] + value_bias).reshape(amount, length, model_dim)
    context = lax.map(jax.checkpoint(attend_packed), (queries, key_rows, val_rows, segments, lengths))
    context = context.reshape(row_count, model_dim)
    residual_one = flat_rows + matmul(context, proj_weight) + proj_bias
    normed_one = layer_norm(residual_one, first_gain, first_shift)
    hidden = matmul(normed_one, up_weight) + up_bias
    active = jax.nn.gelu(hidden, approximate=False)
    residual_two = normed_one + matmul(active, down_weight) + down_bias
    result = layer_norm(residual_two, second_gain, second_shift)
    return result.reshape(amount, length, model_dim)

def reference(tokens, segment_ids, valid_lengths, qkv_weight, query_bias, value_bias, proj_weight, proj_bias, first_gain, first_shift, up_weight, up_bias, down_weight, down_bias, second_gain, second_shift, cotangent):

    def wrapped(rows_in, *params):
        return forward(rows_in, segment_ids, valid_lengths, *params)
    output, pullback = jax.vjp(wrapped, tokens, qkv_weight, query_bias, value_bias, proj_weight, proj_bias, first_gain, first_shift, up_weight, up_bias, down_weight, down_bias, second_gain, second_shift)
    grads = pullback(cotangent)
    factor = 1.0 / math.sqrt(TOKENS)
    return (output, grads[0], grads[1] * factor, grads[2] * factor, grads[3] * factor, grads[4] * factor, grads[5] * factor, grads[6] * factor, grads[7] * factor, grads[8] * factor, grads[9] * factor, grads[10] * factor, grads[11] * factor, grads[12] * factor, grads[13] * factor)
```

```python
import functools
import math

import jax
import jax.numpy as jnp
from jax import lax
from jax.experimental import pallas as pl
from jax.experimental.pallas import tpu as pltpu
from jax.sharding import PartitionSpec as P

H = 16
HD = 64
HIGH = lax.Precision.HIGH
EPSILON = 1e-05
MASKED = -1000000000.0
MESH = pl.DeviceIdType.MESH
DMA = pltpu.SemaphoreType.DMA
F32 = jnp.float32
VMEM_LIMIT = 60 * 2**20
NW = 12


def torus(n):
    side = math.isqrt(n // 4)
    assert side * side * 4 == n
    return 4, side, side


def ds(start, size, align=8):
    return pl.ds(pl.multiple_of(start, align), size)


class Where:
    def __init__(self, n):
        self.NZ, self.NY, self.NX = torus(n)
        s = lax.axis_index("shard")
        self.s = s
        self.c = lax.axis_index("rep")
        self.z = s // (self.NY * self.NX)
        self.y = (s // self.NX) % self.NY
        self.x = s % self.NX

    def dev(self, z=None, y=None, x=None, c=None):
        z = self.z if z is None else z
        y = self.y if y is None else y
        x = self.x if x is None else x
        c = self.c if c is None else c
        return (z * (self.NY * self.NX) + y * self.NX + x, c)

    def partners(self):
        out = [self.dev(c=1 - self.c)]
        out += [self.dev(z=p) for p in self.others("z")]
        out += [self.dev(y=p) for p in self.others("y")]
        out += [self.dev(x=p) for p in self.others("x")]
        return out

    def others(self, axis):
        me, n = self.line(axis)
        return [(me + d) % n for d in range(1, n)]

    def line(self, axis):
        return {"z": (self.z, self.NZ), "y": (self.y, self.NY), "x": (self.x, self.NX)}[axis]

    def barrier(self):
        sem = pltpu.get_barrier_semaphore()
        ps = self.partners()
        for p in ps:
            pl.semaphore_signal(sem, inc=1, device_id=p, device_id_type=MESH)
        pl.semaphore_wait(sem, len(ps))


def remote(src, dst, ssem, rsem, dev):
    return pltpu.make_async_remote_copy(
        src_ref=src, dst_ref=dst, send_sem=ssem, recv_sem=rsem, device_id=dev, device_id_type=MESH
    )


FIRST = ("x", "y")
SECOND = ("y", "x")


class Gather:
    def __init__(self, at, w_ref, g_ref, v_ref, gv_ref, sems):
        self.at, self.w, self.g, self.v, self.gv = at, w_ref, g_ref, v_ref, gv_ref
        self.l, self.zs, self.zr, self.s1, self.r1, self.s2, self.r2, self.ss, self.rs, self.vs, self.vr = sems
        R = w_ref.shape[2]
        self.RH = R // 2
        self.half = ds(at.c * self.RH, self.RH)
        self.other = ds((1 - at.c) * self.RH, self.RH)

    @staticmethod
    def sems(n):
        nz, ny, nx = torus(n)
        return [DMA((NW + 1,)), DMA((NW, 2, nz)), DMA((NW, 2, nz)), DMA((NW, 2, nx)), DMA((NW, 2, nx)),
                DMA((NW, 2, nx)), DMA((NW, 2, nx)), DMA((NW, 2)), DMA((NW, 2)), DMA((3, nz)), DMA((3, nz))]

    def local(self, w):
        a = self.at
        return pltpu.make_async_copy(self.w.at[w, :, self.half], self.g.at[w, :, a.z, a.y, a.x, self.half], self.l.at[w])

    def local_v(self):
        a = self.at
        return pltpu.make_async_copy(self.v, self.gv.at[a.z, a.y, a.x], self.l.at[NW])

    def z(self, w, st, p, recv=False):
        a = self.at
        o = p if recv else a.z
        return remote(self.w.at[w, st, self.half], self.g.at[w, st, o, a.y, a.x, self.half],
                      self.zs.at[w, st, p], self.zr.at[w, st, o], a.dev(z=p))

    def one(self, w, st, p, recv=False):
        a, g, h = self.at, self.g, self.half
        if FIRST[st] == "x":
            o = p if recv else a.x
            return remote(g.at[w, st, :, a.y, a.x, h], g.at[w, st, :, a.y, o, h], self.s1.at[w, st, p], self.r1.at[w, st, o], a.dev(x=p))
        o = p if recv else a.y
        return remote(g.at[w, st, :, a.y, a.x, h], g.at[w, st, :, o, a.x, h], self.s1.at[w, st, p], self.r1.at[w, st, o], a.dev(y=p))

    def two(self, w, st, p, recv=False):
        a, g, h = self.at, self.g, self.half
        if SECOND[st] == "y":
            o = p if recv else a.y
            return remote(g.at[w, st, :, a.y, :, h], g.at[w, st, :, o, :, h], self.s2.at[w, st, p], self.r2.at[w, st, o], a.dev(y=p))
        o = p if recv else a.x
        return remote(g.at[w, st, :, :, a.x, h], g.at[w, st, :, :, o, h], self.s2.at[w, st, p], self.r2.at[w, st, o], a.dev(x=p))

    def pair(self, w, st, recv=False):
        a, g = self.at, self.g
        return remote(g.at[w, st, :, :, :, self.half], g.at[w, st, :, :, :, self.other if recv else self.half],
                      self.ss.at[w, st], self.rs.at[w, st], a.dev(c=1 - a.c))

    def small(self, hop, p, recv=False):
        a, g = self.at, self.gv
        if hop == 0:
            o = p if recv else a.z
            return remote(self.v, g.at[o, a.y, a.x], self.vs.at[0, p], self.vr.at[0, o], a.dev(z=p))
        if hop == 1:
            o = p if recv else a.x
            return remote(g.at[:, a.y, a.x], g.at[:, a.y, o], self.vs.at[1, p], self.vr.at[1, o], a.dev(x=p))
        o = p if recv else a.y
        return remote(g.at[:, a.y], g.at[:, o], self.vs.at[2, p], self.vr.at[2, o], a.dev(y=p))

    def begin_local(self):
        self.local_v().start()

        @pl.loop(0, NW)
        def _(w):
            self.local(w).start()

    def begin(self):
        a = self.at
        for p in a.others("z"):
            self.small(0, p).start()

        @pl.loop(0, NW)
        def _(w):
            for st in range(2):
                for p in a.others("z"):
                    self.z(w, st, p).start()

    def smalls(self):
        a = self.at
        self.local_v().wait()
        for hop, here, nxt in ((0, "z", "x"), (1, "x", "y"), (2, "y", None)):
            for p in a.others(here):
                self.small(hop, p, True).wait_recv()
            if nxt:
                for p in a.others(nxt):
                    self.small(hop + 1, p).start()

    def stage1(self, w):
        a = self.at
        self.local(w).wait()
        for st in range(2):
            for p in a.others("z"):
                self.z(w, st, p, True).wait_recv()
            for p in a.others(FIRST[st]):
                self.one(w, st, p).start()

    def stage2(self, w):
        a = self.at
        for st in range(2):
            for p in a.others(FIRST[st]):
                self.one(w, st, p, True).wait_recv()
            for p in a.others(SECOND[st]):
                self.two(w, st, p).start()

    def stage3(self, w):
        a = self.at
        for st in range(2):
            for p in a.others(SECOND[st]):
                self.two(w, st, p, True).wait_recv()
            self.pair(w, st).start()

    def ready(self, w, st):
        self.pair(w, st, True).wait_recv()

    def step(self, t):
        for k, stage in enumerate((self.stage1, self.stage2, self.stage3)):
            @pl.when((t >= k) & (t < NW + k))
            def _():
                stage(t - k)

    def finish(self):
        a = self.at
        for hop, here in ((0, "z"), (1, "x"), (2, "y")):
            for p in a.others(here):
                self.small(hop, p).wait_send()

        @pl.loop(0, NW)
        def _(w):
            for st in range(2):
                self.pair(w, st).wait_send()
                for p in a.others("z"):
                    self.z(w, st, p).wait_send()
                for p in a.others(FIRST[st]):
                    self.one(w, st, p).wait_send()
                for p in a.others(SECOND[st]):
                    self.two(w, st, p).wait_send()


def gather_kernel(n, w_ref, v_ref, g_ref, gv_ref, *sems):
    at = Where(n)
    ga = Gather(at, w_ref, g_ref, v_ref, gv_ref, sems)
    ga.begin_local()
    at.barrier()
    ga.begin()
    ga.smalls()

    @pl.loop(0, NW + 2)
    def _(t):
        ga.step(t)

    @pl.loop(0, NW)
    def _(w):
        for st in range(2):
            ga.ready(w, st)
    ga.finish()


def gather(n, w, v):
    nz, ny, nx = torus(n)
    _, _, R, CB = w.shape
    return pl.pallas_call(
        functools.partial(gather_kernel, n),
        out_shape=(jax.ShapeDtypeStruct((NW, 2, nz, ny, nx, R, CB), F32),
                   jax.ShapeDtypeStruct((nz, ny, nx) + v.shape, F32)),
        in_specs=[pl.BlockSpec(memory_space=pltpu.VMEM)] * 2,
        out_specs=[pl.BlockSpec(memory_space=pl.ANY)] * 2,
        scratch_shapes=Gather.sems(n),
        compiler_params=pltpu.CompilerParams(collective_id=0, has_side_effects=True, vmem_limit_bytes=VMEM_LIMIT),
        name="gather",
    )(w, v)


NI = 2 * NW
SLOTS = 4
LAG = {1: 1, 2: 3, 3: 5, 4: 7}


class Reduce:
    def __init__(self, at, o_ref, ov_ref, r_refs, bufs, sems, scale):
        self.at, self.o, self.ov, self.scale = at, o_ref, ov_ref, scale
        self.h0, self.h1, self.h2, self.h3 = r_refs
        (self.p, self.a1, self.a2, self.a3, self.a4, self.l0, self.l1, self.l2, self.l3,
         self.v0, self.v1, self.v2, self.v3, self.w0, self.w1, self.w2, self.w3) = bufs
        (self.s0, self.r0, self.s1, self.r1, self.s2, self.r2, self.s3, self.r3, self.s4, self.r4,
         self.ls, self.os, self.vs, self.vr) = sems
        self.RH = o_ref.shape[2] // 2
        self.half = ds(at.c * self.RH, self.RH)
        self.other = ds((1 - at.c) * self.RH, self.RH)

    @staticmethod
    def recv_shapes(n, R, CB):
        nz, ny, nx = torus(n)
        RH = R // 2
        S = lambda *s: jax.ShapeDtypeStruct(s, F32)
        return [S(NI, nz, ny, nx, RH, CB), S(NI, nx, nz, nx, RH, CB), S(NI, nx, nz, RH, CB), S(NI, nz, RH, CB)]

    @staticmethod
    def bufs(n, R, CB, VR):
        nz, ny, nx = torus(n)
        assert nx == ny
        RH = R // 2
        V = lambda *s: pltpu.VMEM(s, F32)
        return [V(SLOTS, nz, ny, nx, R, CB), V(SLOTS, nz, ny, nx, RH, CB), V(SLOTS, nz, nx, RH, CB),
                V(SLOTS, nz, RH, CB), V(SLOTS, RH, CB),
                V(nz, ny, nx, RH, CB), V(nx, nz, nx, RH, CB), V(nx, nz, RH, CB), V(nz, RH, CB),
                V(nz, ny, nx, VR, 128), V(nz, ny, nx, VR, 128), V(nz, nx, VR, 128), V(nz, VR, 128),
                V(nz, ny, nx, VR, 128), V(ny, nz, nx, VR, 128), V(nx, nz, VR, 128), V(nz, VR, 128)]

    @staticmethod
    def sems(n):
        nz, ny, nx = torus(n)
        return [DMA((NI,)), DMA((NI,)), DMA((NI, nx)), DMA((NI, nx)), DMA((NI, nx)), DMA((NI, nx)),
                DMA((NI, nz)), DMA((NI, nz)), DMA((NI,)), DMA((NI,)), DMA((4, nz)), DMA((NI,)), DMA((4, nz)), DMA((4, nz))]

    def hop0(self, i):
        a = self.at
        return remote(self.p.at[i % SLOTS, :, :, :, self.other], self.h0.at[i], self.s0.at[i], self.r0.at[i], a.dev(c=1 - a.c))

    def hop1(self, i, st, q, recv=False):
        a, sl = self.at, i % SLOTS
        if SECOND[st] == "y":
            me, src, dev = a.y, self.a1.at[sl, :, q], a.dev(y=q)
        else:
            me, src, dev = a.x, self.a1.at[sl, :, :, q], a.dev(x=q)
        o = q if recv else me
        return remote(src, self.h1.at[i, o], self.s1.at[i, q], self.r1.at[i, o], dev)

    def hop2(self, i, st, q, recv=False):
        a = self.at
        me, dev = (a.x, a.dev(x=q)) if FIRST[st] == "x" else (a.y, a.dev(y=q))
        o = q if recv else me
        return remote(self.a2.at[i % SLOTS, :, q], self.h2.at[i, o], self.s2.at[i, q], self.r2.at[i, o], dev)

    def hop3(self, i, q, recv=False):
        a = self.at
        o = q if recv else a.z
        return remote(self.a3.at[i % SLOTS, q], self.h3.at[i, o], self.s3.at[i, q], self.r3.at[i, o], a.dev(z=q))

    def hop4(self, i, st, recv=False):
        a = self.at
        return remote(self.a4.at[i % SLOTS], self.o.at[i // 2, st, self.other if recv else self.half], self.s4.at[i], self.r4.at[i], a.dev(c=1 - a.c))

    def keep(self, i, st):
        return pltpu.make_async_copy(self.a4.at[i % SLOTS], self.o.at[i // 2, st, self.half], self.os.at[i])

    def load(self, k, i, q=0):
        if k == 1:
            return pltpu.make_async_copy(self.h0.at[i], self.l0, self.ls.at[0, 0])
        src, dst = {2: (self.h1, self.l1), 3: (self.h2, self.l2), 4: (self.h3, self.l3)}[k]
        return pltpu.make_async_copy(src.at[i, q], dst.at[q], self.ls.at[k - 1, q])

    def lines(self, k, st):
        return self.at.others({2: SECOND[st], 3: FIRST[st], 4: "z"}[k])

    def hops(self, k, i, st, recv=False):
        if k == 1:
            return [self.hop0(i)]
        if k == 5:
            return [self.hop4(i, st, recv)]
        f = {2: lambda q: self.hop1(i, st, q, recv), 3: lambda q: self.hop2(i, st, q, recv), 4: lambda q: self.hop3(i, q, recv)}[k]
        return [f(q) for q in self.lines(k, st)]

    def free(self, k, i, st):
        @pl.when(i >= SLOTS)
        def _():
            for h in self.hops(k, i - SLOTS, st):
                h.wait_send()
            if k == 5:
                self.keep(i - SLOTS, st).wait()

    def send(self, i):
        self.hop0(i).start()

    def arrive(self, k, i, st):
        for h in self.hops(k, i, st, True):
            h.wait_recv()
        if k == 1:
            self.load(1, i).start()
        else:
            for q in self.lines(k, st):
                self.load(k, i, q).start()

    def process(self, k, i, st):
        a, sl = self.at, i % SLOTS
        nz, ny, nx = a.NZ, a.NY, a.NX
        self.free(k + 1, i, st)
        others = [] if k == 1 else self.lines(k, st)
        if k == 1:
            self.load(1, i).wait()
        for q in others:
            self.load(k, i, q).wait()
        if k == 1:
            @pl.loop(0, nz)
            def _(z):
                for y in range(ny):
                    for x in range(nx):
                        self.a1[sl, z, y, x] = self.p[sl, z, y, x, self.half] + self.l0[z, y, x]
        elif k == 2:
            @pl.loop(0, nz)
            def _(z):
                for x in range(nx):
                    own = self.a1[sl, z, a.y, x] if SECOND[st] == "y" else self.a1[sl, z, x, a.x]
                    for q in others:
                        own = own + self.l1[q, z, x]
                    self.a2[sl, z, x] = own
        elif k == 3:
            me = a.x if FIRST[st] == "x" else a.y

            @pl.loop(0, nz)
            def _(z):
                own = self.a2[sl, z, me]
                for q in others:
                    own = own + self.l2[q, z]
                self.a3[sl, z] = own
        else:
            own = self.a3[sl, a.z]
            for q in others:
                own = own + self.l3[q]
            self.a4[sl] = own * self.scale
            self.keep(i, st).start()
        for h in self.hops(k + 1, i, st):
            h.start()

    def step(self, t):
        def at_stage(k, st, f):
            i = t - LAG[k]

            @pl.when((i >= 0) & (i < NI) & (i % 2 == st))
            def _():
                f(k, i, st)
        for k in (4, 3, 2, 1):
            for st in range(2):
                at_stage(k, st, self.arrive)
        for k in (4, 3, 2, 1):
            for st in range(2):
                at_stage(k, st, self.process)

    def finish(self):
        @pl.loop(NI - SLOTS, NI, step=2)
        def _(j):
            for st in range(2):
                for k in (1, 2, 3, 4, 5):
                    for h in self.hops(k, j + st, st):
                        h.wait_send()
                self.keep(j + st, st).wait()

        @pl.loop(0, NI, step=2)
        def _(j):
            for st in range(2):
                self.hop4(j + st, st, True).wait_recv()

    def vhop(self, k, q, recv=False):
        a = self.at
        if k == 0:
            return remote(self.v0, self.w0, self.vs.at[0, 0], self.vr.at[0, 0], a.dev(c=1 - a.c))
        me, src, dst, dev = {1: (a.y, self.v1.at[:, q], self.w1, a.dev(y=q)), 2: (a.x, self.v2.at[:, q], self.w2, a.dev(x=q)),
                             3: (a.z, self.v3.at[q], self.w3, a.dev(z=q))}[k]
        o = q if recv else me
        return remote(src, dst.at[o], self.vs.at[k, q], self.vr.at[k, o], dev)

    def vlines(self, k):
        return [0] if k == 0 else self.at.others({1: "y", 2: "x", 3: "z"}[k])

    def small(self, k):
        a = self.at
        if k:
            for q in self.vlines(k - 1):
                self.vhop(k - 1, q, True).wait_recv()
        if k == 1:
            self.v1[...] = self.v0[...] + self.w0[...]
        if k == 2:
            own = self.v1[:, a.y]
            for q in self.vlines(1):
                own = own + self.w1[q]
            self.v2[...] = own
        if k == 3:
            own = self.v2[:, a.x]
            for q in self.vlines(2):
                own = own + self.w2[q]
            self.v3[...] = own
        if k == 4:
            own = self.v3[a.z]
            for q in self.vlines(3):
                own = own + self.w3[q]
            self.ov[...] = own * self.scale
        else:
            for q in self.vlines(k):
                self.vhop(k, q).start()

    def small_finish(self):
        for k in range(4):
            for q in self.vlines(k):
                self.vhop(k, q).wait_send()


def reduce_kernel(n, scale, d_ref, dv_ref, o_ref, ov_ref, h0, h1, h2, h3, psem, *rest):
    bufs, sems = rest[:17], rest[17:]
    at = Where(n)
    rd = Reduce(at, o_ref, ov_ref, (h0, h1, h2, h3), bufs, sems, scale)
    at.barrier()
    rd.v0[...] = dv_ref[...]

    def fetch(i):
        return pltpu.make_async_copy(d_ref.at[i], rd.p.at[i % SLOTS], psem.at[i % 2])

    fetch(0).start()
    for k in range(5):
        rd.small(k)

    @pl.loop(0, NI + LAG[4])
    def _(t):
        @pl.when(t < NI)
        def _():
            fetch(t).wait()
            rd.send(t)
        rd.step(t)

        @pl.when(t + 1 < NI)
        def _():
            @pl.when(t + 1 >= SLOTS)
            def _():
                rd.hop0(t + 1 - SLOTS).wait_send()
            fetch(t + 1).start()
    rd.finish()
    rd.small_finish()


def reduce(n, scale, d, dv):
    _, nz, ny, nx, R, CB = d.shape
    VR = dv.shape[-2]
    ANY = pl.BlockSpec(memory_space=pl.ANY)
    VM = pl.BlockSpec(memory_space=pltpu.VMEM)
    return pl.pallas_call(
        functools.partial(reduce_kernel, n, scale),
        out_shape=[jax.ShapeDtypeStruct((NW, 2, R, CB), F32), jax.ShapeDtypeStruct((VR, 128), F32)]
        + Reduce.recv_shapes(n, R, CB),
        in_specs=[ANY, VM],
        out_specs=[ANY, VM, ANY, ANY, ANY, ANY],
        scratch_shapes=[DMA((2,))] + Reduce.bufs(n, R, CB, VR) + Reduce.sems(n),
        compiler_params=pltpu.CompilerParams(collective_id=1, has_side_effects=True, vmem_limit_bytes=VMEM_LIMIT),
        name="reduce",
    )(d, dv)[:2]


def dot(a, b, dims=((1,), (0,))):
    return lax.dot_general(a, b, (dims, ((), ())), precision=HIGH)


def pack_weights(n, qkv, proj, up, down):
    R, D = proj.shape
    J = up.shape[1] // D
    q3 = qkv.reshape(R, 3, D).transpose(1, 0, 2)
    u4 = up.reshape(R, n, J, R).transpose(2, 0, 1, 3).reshape(J, R, D)
    d4 = down.reshape(J, R, D)
    w = jnp.concatenate([q3, proj[None], u4, d4], axis=0)
    return w.reshape(NW, R, 2, D // 2).transpose(0, 2, 1, 3)


def unpack_weights(n, w):
    _, _, R, HB = w.shape
    D = 2 * HB
    w = w.transpose(0, 2, 1, 3).reshape(NW, R, D)
    J = 4
    return (w[:3].transpose(1, 0, 2).reshape(R, 3 * D), w[3],
            w[4:8].reshape(J, R, n, R).transpose(1, 2, 0, 3).reshape(R, n * J * R), w[8:].reshape(J * R, D))


VROWS = 16


def lane(R):
    return (lax.axis_index("shard") * R) % 128


def pack_small(vectors, up_bias):
    R = vectors[0].shape[0]
    rows = jnp.concatenate([jnp.stack(vectors[:5]), up_bias.reshape(4, R), jnp.stack(vectors[5:])])
    wide = jnp.zeros((VROWS, 128), F32)
    return lax.dynamic_update_slice(wide, jnp.pad(rows, ((0, VROWS - rows.shape[0]), (0, 0))), (0, lane(R)))


def whole_small(n, gv, R):
    q = 128 // R
    return gv.reshape(n // q, q, VROWS, 128).sum(axis=1).transpose(1, 0, 2).reshape(VROWS, n // q * 128)


def spread_small(n, v, R):
    q = 128 // R
    blocks = v.reshape(VROWS, n // q, 128).transpose(1, 0, 2)
    return jnp.repeat(blocks, q, axis=0)


def attend(queries, key_rows, val_rows, seg_row, valid_len):
    length = queries.shape[0]
    queries = queries.reshape(length, H, HD)
    key_rows = key_rows.reshape(length, H, HD)
    val_rows = val_rows.reshape(length, H, HD)
    scores = jnp.einsum("qhd,khd->hqk", queries, key_rows, precision=HIGH) / math.sqrt(HD)
    places = jnp.arange(length, dtype=jnp.int32)
    allowed = (seg_row[:, None] == seg_row[None, :]) & (
        (places[None, :] < valid_len) | (places[:, None] == places[None, :])
    )
    scores = jnp.where(allowed[None], scores, MASKED)
    probs = jax.nn.softmax(scores, axis=-1)
    context = jnp.einsum("hqk,khd->qhd", probs, val_rows, precision=HIGH)
    return context.reshape(length, H * HD)


def gelu(u):
    return 0.5 * u * (1.0 + lax.erf(u * math.sqrt(0.5)))


def gelu_slope(u):
    return 0.5 * (1.0 + lax.erf(u * math.sqrt(0.5))) + u * jnp.exp(-0.5 * u * u) * (1.0 / math.sqrt(2.0 * math.pi))


def norm(v):
    center = v - jnp.mean(v, axis=-1, keepdims=True)
    inverse = lax.rsqrt(jnp.mean(center * center, axis=-1, keepdims=True) + EPSILON)
    return center * inverse, inverse


def norm_back(g, hat, inverse, gain):
    gg = g * gain
    return inverse * (gg - jnp.mean(gg, -1, keepdims=True) - hat * jnp.mean(gg * hat, -1, keepdims=True))


def shards(n, tokens, segment_ids, valid_lengths, qkv_weight, query_bias, value_bias, proj_weight, proj_bias, first_gain,
           first_shift, up_weight, up_bias, down_weight, down_bias, second_gain, second_shift, cotangent):
    amount, length, D = tokens.shape
    R = proj_weight.shape[0]
    nz, ny, nx = torus(n)
    g, gv = gather(n, pack_weights(n, qkv_weight, proj_weight, up_weight, down_weight),
                   pack_small([query_bias, value_bias, proj_bias, first_gain, first_shift, down_bias, second_gain, second_shift], up_bias))
    g = g.reshape(NW, 2, D, D // 2)
    m = [jnp.concatenate([g[w, 0], g[w, 1]], axis=1) for w in range(NW)]
    v = whole_small(n, gv, R)
    row = lambda k: v[k][None]
    ub = v[5:9].reshape(1, 4 * D)
    x = tokens.reshape(amount * length, D)
    q = dot(x, m[0]) + row(0)
    k = dot(x, m[1])
    val = dot(x, m[2]) + row(1)
    context, pull = jax.vjp(lambda a, b, c: attend(a, b, c, segment_ids[0], valid_lengths[0]), q, k, val)
    hat1, inv1 = norm(x + dot(context, m[3]) + row(2))
    n1 = hat1 * row(3) + row(4)
    up = jnp.concatenate(m[4:8], axis=1)
    down = jnp.concatenate(m[8:], axis=0)
    u = dot(n1, up) + ub
    a = gelu(u)
    hat2, inv2 = norm(n1 + dot(a, down) + row(9))
    out = hat2 * row(10) + row(11)
    ct = cotangent.reshape(amount * length, D)
    T = ((0,), (0,))
    B = ((1,), (1,))
    dr2 = norm_back(ct, hat2, inv2, row(10))
    ddown = dot(a, dr2, T)
    du = dot(dr2, down, B) * gelu_slope(u)
    dup = dot(n1, du, T)
    dn1 = dr2 + dot(du, up, B)
    dr1 = norm_back(dn1, hat1, inv1, row(3))
    dproj = dot(context, dr1, T)
    dq, dk, dv = pull(dot(dr1, m[3], B))
    dx = dr1 + dot(dq, m[0], B) + dot(dk, m[1], B) + dot(dv, m[2], B)
    col = lambda t: jnp.sum(t, axis=0)
    small = jnp.stack([col(dq), col(dv), col(dr1), col(dn1 * hat1), col(dn1)] + list(col(du).reshape(4, D))
                      + [col(dr2), col(ct * hat2), col(ct)] + [jnp.zeros((D,), F32)] * 4)
    grads = [dot(x, dq, T), dot(x, dk, T), dot(x, dv, T), dproj] + [dup[:, j * D:(j + 1) * D] for j in range(4)] \
        + [ddown[j * D:(j + 1) * D] for j in range(4)]
    d = jnp.stack([part for t in grads for part in (t[:, :D // 2], t[:, D // 2:])]).reshape(NI, nz, ny, nx, R, D // 2)
    scale = 1.0 / math.sqrt(amount * length * n * lax.axis_size("rep"))
    o, ov = reduce(n, scale, d, spread_small(n, small, R).reshape(nz, ny, nx, VROWS, 128))
    gqkv, gproj, gup, gdown = unpack_weights(n, o)
    s = lax.dynamic_slice(ov, (0, lane(R)), (VROWS, R))
    return (out.reshape(amount, length, D), dx.reshape(amount, length, D), gqkv, s[0], s[1], gproj, s[2], s[3], s[4], gup,
            s[5:9].reshape(4 * R), gdown, s[9], s[10], s[11])


def solution(mesh):
    n = mesh.shape["shard"]
    one, two, seq = P("shard"), P("shard", None), P(("shard", "rep"), None, None)
    return jax.shard_map(
        functools.partial(shards, n),
        mesh=mesh,
        in_specs=(seq, P(("shard", "rep"), None), P(("shard", "rep")), two, one, one, two, one, one, one, two, one, two, one, one, one, seq),
        out_specs=(seq, seq, two, one, one, two, one, one, one, two, one, two, one, one, one),
        check_vma=False,
    )
```

```python
import functools
import math

import jax
import jax.numpy as jnp
from jax import lax
from jax.experimental import pallas as pl
from jax.experimental.pallas import tpu as pltpu
from jax.sharding import PartitionSpec as P

H = 16
HD = 64
HIGH = lax.Precision.HIGH
EPSILON = 1e-05
MASKED = -1000000000.0
MESH = pl.DeviceIdType.MESH
DMA = pltpu.SemaphoreType.DMA
F32 = jnp.float32
VMEM_LIMIT = 60 * 2**20
NW = 12


def torus(n):
    side = math.isqrt(n // 4)
    assert side * side * 4 == n
    return 4, side, side


def ds(start, size, align=8):
    return pl.ds(pl.multiple_of(start, align), size)


class Where:
    def __init__(self, n):
        self.NZ, self.NY, self.NX = torus(n)
        s = lax.axis_index("shard")
        self.s = s
        self.c = lax.axis_index("rep")
        self.z = s // (self.NY * self.NX)
        self.y = (s // self.NX) % self.NY
        self.x = s % self.NX

    def dev(self, z=None, y=None, x=None, c=None):
        z = self.z if z is None else z
        y = self.y if y is None else y
        x = self.x if x is None else x
        c = self.c if c is None else c
        return (z * (self.NY * self.NX) + y * self.NX + x, c)

    def partners(self):
        out = [self.dev(c=1 - self.c)]
        out += [self.dev(z=p) for p in self.others("z")]
        out += [self.dev(y=p) for p in self.others("y")]
        out += [self.dev(x=p) for p in self.others("x")]
        return out

    def others(self, axis):
        me, n = self.line(axis)
        return [(me + d) % n for d in range(1, n)]

    def line(self, axis):
        return {"z": (self.z, self.NZ), "y": (self.y, self.NY), "x": (self.x, self.NX)}[axis]

    def barrier(self):
        sem = pltpu.get_barrier_semaphore()
        ps = self.partners()
        for p in ps:
            pl.semaphore_signal(sem, inc=1, device_id=p, device_id_type=MESH)
        pl.semaphore_wait(sem, len(ps))


def remote(src, dst, ssem, rsem, dev):
    return pltpu.make_async_remote_copy(
        src_ref=src, dst_ref=dst, send_sem=ssem, recv_sem=rsem, device_id=dev, device_id_type=MESH
    )


FIRST = ("x", "y")
SECOND = ("y", "x")


class Gather:
    def __init__(self, at, w_ref, g_ref, v_ref, gv_ref, sems):
        self.at, self.w, self.g, self.v, self.gv = at, w_ref, g_ref, v_ref, gv_ref
        self.l, self.zs, self.zr, self.s1, self.r1, self.s2, self.r2, self.ss, self.rs, self.vs, self.vr = sems
        R = w_ref.shape[2]
        self.RH = R // 2
        self.half = ds(at.c * self.RH, self.RH)
        self.other = ds((1 - at.c) * self.RH, self.RH)

    @staticmethod
    def sems(n):
        nz, ny, nx = torus(n)
        return [DMA((NW + 1,)), DMA((NW, 2, nz)), DMA((NW, 2, nz)), DMA((NW, 2, nx)), DMA((NW, 2, nx)),
                DMA((NW, 2, nx)), DMA((NW, 2, nx)), DMA((NW, 2)), DMA((NW, 2)), DMA((3, nz)), DMA((3, nz))]

    def local(self, w):
        a = self.at
        return pltpu.make_async_copy(self.w.at[w, :, self.half], self.g.at[w, :, a.z, a.y, a.x, self.half], self.l.at[w])

    def local_v(self):
        a = self.at
        return pltpu.make_async_copy(self.v, self.gv.at[a.z, a.y, a.x], self.l.at[NW])

    def z(self, w, st, p, recv=False):
        a = self.at
        o = p if recv else a.z
        return remote(self.w.at[w, st, self.half], self.g.at[w, st, o, a.y, a.x, self.half],
                      self.zs.at[w, st, p], self.zr.at[w, st, o], a.dev(z=p))

    def one(self, w, st, p, recv=False):
        a, g, h = self.at, self.g, self.half
        if FIRST[st] == "x":
            o = p if recv else a.x
            return remote(g.at[w, st, :, a.y, a.x, h], g.at[w, st, :, a.y, o, h], self.s1.at[w, st, p], self.r1.at[w, st, o], a.dev(x=p))
        o = p if recv else a.y
        return remote(g.at[w, st, :, a.y, a.x, h], g.at[w, st, :, o, a.x, h], self.s1.at[w, st, p], self.r1.at[w, st, o], a.dev(y=p))

    def two(self, w, st, p, recv=False):
        a, g, h = self.at, self.g, self.half
        if SECOND[st] == "y":
            o = p if recv else a.y
            return remote(g.at[w, st, :, a.y, :, h], g.at[w, st, :, o, :, h], self.s2.at[w, st, p], self.r2.at[w, st, o], a.dev(y=p))
        o = p if recv else a.x
        return remote(g.at[w, st, :, :, a.x, h], g.at[w, st, :, :, o, h], self.s2.at[w, st, p], self.r2.at[w, st, o], a.dev(x=p))

    def pair(self, w, st, recv=False):
        a, g = self.at, self.g
        return remote(g.at[w, st, :, :, :, self.half], g.at[w, st, :, :, :, self.other if recv else self.half],
                      self.ss.at[w, st], self.rs.at[w, st], a.dev(c=1 - a.c))

    def small(self, hop, p, recv=False):
        a, g = self.at, self.gv
        if hop == 0:
            o = p if recv else a.z
            return remote(self.v, g.at[o, a.y, a.x], self.vs.at[0, p], self.vr.at[0, o], a.dev(z=p))
        if hop == 1:
            o = p if recv else a.x
            return remote(g.at[:, a.y, a.x], g.at[:, a.y, o], self.vs.at[1, p], self.vr.at[1, o], a.dev(x=p))
        o = p if recv else a.y
        return remote(g.at[:, a.y], g.at[:, o], self.vs.at[2, p], self.vr.at[2, o], a.dev(y=p))

    def begin_local(self):
        self.local_v().start()

        @pl.loop(0, NW)
        def _(w):
            self.local(w).start()

    def begin(self):
        a = self.at
        for p in a.others("z"):
            self.small(0, p).start()

        @pl.loop(0, NW)
        def _(w):
            for st in range(2):
                for p in a.others("z"):
                    self.z(w, st, p).start()

    def smalls(self):
        a = self.at
        self.local_v().wait()
        for hop, here, nxt in ((0, "z", "x"), (1, "x", "y"), (2, "y", None)):
            for p in a.others(here):
                self.small(hop, p, True).wait_recv()
            if nxt:
                for p in a.others(nxt):
                    self.small(hop + 1, p).start()

    def stage1(self, w):
        a = self.at
        self.local(w).wait()
        for st in range(2):
            for p in a.others("z"):
                self.z(w, st, p, True).wait_recv()
            for p in a.others(FIRST[st]):
                self.one(w, st, p).start()

    def stage2(self, w):
        a = self.at
        for st in range(2):
            for p in a.others(FIRST[st]):
                self.one(w, st, p, True).wait_recv()
            for p in a.others(SECOND[st]):
                self.two(w, st, p).start()

    def stage3(self, w):
        a = self.at
        for st in range(2):
            for p in a.others(SECOND[st]):
                self.two(w, st, p, True).wait_recv()
            self.pair(w, st).start()

    def ready(self, w, st):
        self.pair(w, st, True).wait_recv()

    def step(self, t):
        for k, stage in enumerate((self.stage1, self.stage2, self.stage3)):
            @pl.when((t >= k) & (t < NW + k))
            def _():
                stage(t - k)

    def finish(self):
        a = self.at
        for hop, here in ((0, "z"), (1, "x"), (2, "y")):
            for p in a.others(here):
                self.small(hop, p).wait_send()

        @pl.loop(0, NW)
        def _(w):
            for st in range(2):
                self.pair(w, st).wait_send()
                for p in a.others("z"):
                    self.z(w, st, p).wait_send()
                for p in a.others(FIRST[st]):
                    self.one(w, st, p).wait_send()
                for p in a.others(SECOND[st]):
                    self.two(w, st, p).wait_send()


NI = 2 * NW
SLOTS = 4
LAG = {1: 0, 2: 2, 3: 4, 4: 6}


class Reduce:
    def __init__(self, at, o_ref, ov_ref, r_refs, bufs, sems, scale):
        self.at, self.o, self.ov, self.scale = at, o_ref, ov_ref, scale
        self.h0, self.h1, self.h2, self.h3 = r_refs
        (self.p, self.a1, self.a2, self.a3, self.a4, self.l0, self.l1, self.l2, self.l3,
         self.v0, self.v1, self.v2, self.v3, self.w0, self.w1, self.w2, self.w3) = bufs
        (self.s0, self.r0, self.s1, self.r1, self.s2, self.r2, self.s3, self.r3, self.s4, self.r4,
         self.ls, self.os, self.vs, self.vr) = sems
        self.RH = o_ref.shape[1] // 2
        self.half = ds(at.c * self.RH, self.RH)
        self.other = ds((1 - at.c) * self.RH, self.RH)

    @staticmethod
    def recv_shapes(n, R, CB):
        nz, ny, nx = torus(n)
        RH = R // 2
        S = lambda *s: jax.ShapeDtypeStruct(s, F32)
        return [S(NI, nz, ny, nx, RH, CB), S(NI, nx, nz, nx, RH, CB), S(NI, nx, nz, RH, CB), S(NI, nz, RH, CB)]

    @staticmethod
    def bufs(n, R, CB, VR):
        nz, ny, nx = torus(n)
        assert nx == ny
        RH = R // 2
        V = lambda *s: pltpu.VMEM(s, F32)
        return [V(2, nz, ny, nx, R, CB), V(SLOTS, nz, ny, nx, RH, CB), V(SLOTS, nz, nx, RH, CB),
                V(SLOTS, nz, RH, CB), V(SLOTS, RH, CB),
                V(nz, ny, nx, RH, CB), V(nx, nz, nx, RH, CB), V(nx, nz, RH, CB), V(nz, RH, CB),
                V(nz, ny, nx, VR, 128), V(nz, ny, nx, VR, 128), V(nz, nx, VR, 128), V(nz, VR, 128),
                V(nz, ny, nx, VR, 128), V(ny, nz, nx, VR, 128), V(nx, nz, VR, 128), V(nz, VR, 128)]

    @staticmethod
    def sems(n):
        nz, ny, nx = torus(n)
        return [DMA((NI,)), DMA((NI,)), DMA((NI, nx)), DMA((NI, nx)), DMA((NI, nx)), DMA((NI, nx)),
                DMA((NI, nz)), DMA((NI, nz)), DMA((NI,)), DMA((NI,)), DMA((4, nz)), DMA((NI,)), DMA((4, nz)), DMA((4, nz))]

    def hop0(self, i):
        a = self.at
        return remote(self.p.at[i % 2, :, :, :, self.other], self.h0.at[i], self.s0.at[i], self.r0.at[i], a.dev(c=1 - a.c))

    def hop1(self, i, st, q, recv=False):
        a, sl = self.at, i % SLOTS
        if SECOND[st] == "y":
            me, src, dev = a.y, self.a1.at[sl, :, q], a.dev(y=q)
        else:
            me, src, dev = a.x, self.a1.at[sl, :, :, q], a.dev(x=q)
        o = q if recv else me
        return remote(src, self.h1.at[i, o], self.s1.at[i, q], self.r1.at[i, o], dev)

    def hop2(self, i, st, q, recv=False):
        a = self.at
        me, dev = (a.x, a.dev(x=q)) if FIRST[st] == "x" else (a.y, a.dev(y=q))
        o = q if recv else me
        return remote(self.a2.at[i % SLOTS, :, q], self.h2.at[i, o], self.s2.at[i, q], self.r2.at[i, o], dev)

    def hop3(self, i, q, recv=False):
        a = self.at
        o = q if recv else a.z
        return remote(self.a3.at[i % SLOTS, q], self.h3.at[i, o], self.s3.at[i, q], self.r3.at[i, o], a.dev(z=q))

    def hop4(self, i, st, recv=False):
        a = self.at
        return remote(self.a4.at[i % SLOTS], self.o.at[i, self.other if recv else self.half], self.s4.at[i], self.r4.at[i], a.dev(c=1 - a.c))

    def keep(self, i, st):
        return pltpu.make_async_copy(self.a4.at[i % SLOTS], self.o.at[i, self.half], self.os.at[i])

    def load(self, k, i, q=0):
        if k == 1:
            return pltpu.make_async_copy(self.h0.at[i], self.l0, self.ls.at[0, 0])
        src, dst = {2: (self.h1, self.l1), 3: (self.h2, self.l2), 4: (self.h3, self.l3)}[k]
        return pltpu.make_async_copy(src.at[i, q], dst.at[q], self.ls.at[k - 1, q])

    def lines(self, k, st):
        return self.at.others({2: SECOND[st], 3: FIRST[st], 4: "z"}[k])

    def hops(self, k, i, st, recv=False):
        if k == 1:
            return [self.hop0(i)]
        if k == 5:
            return [self.hop4(i, st, recv)]
        f = {2: lambda q: self.hop1(i, st, q, recv), 3: lambda q: self.hop2(i, st, q, recv), 4: lambda q: self.hop3(i, q, recv)}[k]
        return [f(q) for q in self.lines(k, st)]

    def free(self, k, i, st):
        @pl.when(i >= SLOTS)
        def _():
            for h in self.hops(k, i - SLOTS, st):
                h.wait_send()
            if k == 5:
                self.keep(i - SLOTS, st).wait()

    def send(self, i):
        self.hop0(i).start()

    def arrive(self, k, i, st):
        for h in self.hops(k, i, st, True):
            h.wait_recv()
        if k == 1:
            self.load(1, i).start()
        else:
            for q in self.lines(k, st):
                self.load(k, i, q).start()

    def process(self, k, i, st):
        a, sl = self.at, i % SLOTS
        nz, ny, nx = a.NZ, a.NY, a.NX
        self.free(k + 1, i, st)
        others = [] if k == 1 else self.lines(k, st)
        if k == 1:
            self.load(1, i).wait()
        for q in others:
            self.load(k, i, q).wait()
        if k == 1:
            @pl.loop(0, nz)
            def _(z):
                for y in range(ny):
                    for x in range(nx):
                        self.a1[sl, z, y, x] = self.p[i % 2, z, y, x, self.half] + self.l0[z, y, x]
        elif k == 2:
            @pl.loop(0, nz)
            def _(z):
                for x in range(nx):
                    own = self.a1[sl, z, a.y, x] if SECOND[st] == "y" else self.a1[sl, z, x, a.x]
                    for q in others:
                        own = own + self.l1[q, z, x]
                    self.a2[sl, z, x] = own
        elif k == 3:
            me = a.x if FIRST[st] == "x" else a.y

            @pl.loop(0, nz)
            def _(z):
                own = self.a2[sl, z, me]
                for q in others:
                    own = own + self.l2[q, z]
                self.a3[sl, z] = own
        else:
            own = self.a3[sl, a.z]
            for q in others:
                own = own + self.l3[q]
            self.a4[sl] = own * self.scale
            self.keep(i, st).start()
        for h in self.hops(k + 1, i, st):
            h.start()

    def step(self, t):
        def at_stage(k, st, f):
            i = t - LAG[k]

            @pl.when((i >= 0) & (i < NI) & (i % 2 == st))
            def _():
                f(k, i, st)
        for k in (4, 3, 2, 1):
            for st in range(2):
                at_stage(k, st, self.arrive)
        for k in (4, 3, 2, 1):
            for st in range(2):
                at_stage(k, st, self.process)

    def finish(self):
        for i in (NI - 2, NI - 1):
            self.hop0(i).wait_send()

        @pl.loop(NI - SLOTS, NI, step=2)
        def _(j):
            for st in range(2):
                for k in (2, 3, 4, 5):
                    for h in self.hops(k, j + st, st):
                        h.wait_send()
                self.keep(j + st, st).wait()

        @pl.loop(0, NI, step=2)
        def _(j):
            for st in range(2):
                self.hop4(j + st, st, True).wait_recv()

    def vhop(self, k, q, recv=False):
        a = self.at
        if k == 0:
            return remote(self.v0, self.w0, self.vs.at[0, 0], self.vr.at[0, 0], a.dev(c=1 - a.c))
        me, src, dst, dev = {1: (a.y, self.v1.at[:, q], self.w1, a.dev(y=q)), 2: (a.x, self.v2.at[:, q], self.w2, a.dev(x=q)),
                             3: (a.z, self.v3.at[q], self.w3, a.dev(z=q))}[k]
        o = q if recv else me
        return remote(src, dst.at[o], self.vs.at[k, q], self.vr.at[k, o], dev)

    def vlines(self, k):
        return [0] if k == 0 else self.at.others({1: "y", 2: "x", 3: "z"}[k])

    def small(self, k):
        a = self.at
        if k:
            for q in self.vlines(k - 1):
                self.vhop(k - 1, q, True).wait_recv()
        if k == 1:
            self.v1[...] = self.v0[...] + self.w0[...]
        if k == 2:
            own = self.v1[:, a.y]
            for q in self.vlines(1):
                own = own + self.w1[q]
            self.v2[...] = own
        if k == 3:
            own = self.v2[:, a.x]
            for q in self.vlines(2):
                own = own + self.w2[q]
            self.v3[...] = own
        if k == 4:
            own = self.v3[a.z]
            for q in self.vlines(3):
                own = own + self.w3[q]
            self.ov[...] = own * self.scale
        else:
            for q in self.vlines(k):
                self.vhop(k, q).start()

    def small_finish(self):
        for k in range(4):
            for q in self.vlines(k):
                self.vhop(k, q).wait_send()


BF = jnp.bfloat16
NN = ((1,), (0,))
NT = ((1,), (1,))
TN = ((0,), (0,))
ROW_P, ROW_G1, ROW_S1, ROW_U, ROW_D, ROW_G2, ROW_S2 = 3, 4, 5, 6, 10, 11, 12
X_, C_, N_, A_ = 0, 1, 2, 3


def mx(a, b, dims=NN):
    return lax.dot_general(a, b, (dims, ((), ())), preferred_element_type=F32)


def split(v):
    hi = v.astype(BF)
    return hi, (v - hi.astype(F32)).astype(BF)


def split32(v):
    hi = v.astype(BF).astype(F32)
    return hi, v - hi


def three(ah, al, bh, bl, dims=NN):
    return mx(ah, bh, dims) + mx(ah, bl, dims) + mx(al, bh, dims)


def left_half(shape):
    return lax.broadcasted_iota(jnp.int32, shape, 1) < HD


def pack_hl0(v):
    m = left_half(v.shape)
    h, l = split32(v)
    hr, lr = pltpu.roll(h, HD, 1), pltpu.roll(l, HD, 1)
    zero = jnp.zeros_like(v)
    one = jnp.concatenate([jnp.where(m, h, lr), jnp.where(m, h, zero)], axis=1).astype(BF)
    two = jnp.concatenate([jnp.where(m, lr, h), jnp.where(m, zero, h)], axis=1).astype(BF)
    return one, two


def pack_hhl(v):
    m = left_half(v.shape)
    h, l = split32(v)
    hr = pltpu.roll(h, HD, 1)
    one = jnp.concatenate([jnp.where(m, h, hr), l], axis=1).astype(BF)
    two = jnp.concatenate([jnp.where(m, hr, h), l], axis=1).astype(BF)
    return one, two


def pack_hl(v):
    m = left_half(v.shape)
    h, l = split32(v)
    lr = pltpu.roll(l, HD, 1)
    return jnp.where(m, h, lr).astype(BF), jnp.where(m, lr, h).astype(BF)


def fold(one, two):
    m = left_half(one.shape)
    return jnp.where(m, one, two) + pltpu.roll(jnp.where(m, two, one), HD, 1)


def stack_t(v):
    t = v.T
    out = []
    for k in range(2):
        h, l = split32(t[k * HD:(k + 1) * HD])
        out.append(jnp.concatenate([h, l], axis=0).astype(BF))
    return out


def fold_t(one, two):
    return jnp.concatenate([one[:HD] + one[HD:], two[:HD] + two[HD:]], axis=0).T


def cols(start, size):
    return pl.ds(pl.multiple_of(start, 128), size)


def forward_kernel(n, x_ref, w_ref, v_ref, segr, segc, okc,
                   out_ref, g_ref, gv_ref, lh_out, ws_out, qkv_out, p_out, sl_out, hat1_out, hat2_out, inv_out, vec_out,
                   lh, wf, ws, qkv, acc, n1, r2, slope, pst, bias, gvv, vec, ld_sem, ws_sem, out_sem, p_sem, sl_sem, *sems):
    at = Where(n)
    L, D = x_ref.shape
    HB = D // 2
    ga = Gather(at, w_ref, g_ref, v_ref, gv_ref, sems)
    ga.begin_local()
    at.barrier()
    ga.begin()

    def lh_copy(s):
        return pltpu.make_async_copy(lh.at[s], lh_out.at[s], out_sem.at[s])

    RB = 128

    @pl.loop(0, L // RB)
    def _(r):
        rows = pl.ds(pl.multiple_of(r * RB, RB), RB)
        h, l = split(x_ref[rows])
        lh[X_, 0, rows] = h
        lh[X_, 1, rows] = l
        kpos = lax.broadcasted_iota(jnp.int32, (RB, L), 0) + r * RB
        qpos = lax.broadcasted_iota(jnp.int32, (RB, L), 1)
        allowed = (segc[rows] == segr[...]) & ((okc[rows] > 0) | (kpos == qpos))
        bias[rows] = jnp.where(allowed, 0.0, MASKED)
    lh_copy(X_).start()
    ga.smalls()
    cp = pltpu.make_async_copy(gv_ref, gvv, ld_sem.at[0])
    cp.start()
    cp.wait()
    R = 2 * ga.RH
    q = 128 // R
    for k in range(D // 128):
        s = None
        for j in range(q):
            c = k * q + j
            blk = gvv[c // (at.NY * at.NX), (c // at.NX) % at.NY, c % at.NX]
            s = blk if s is None else s + blk
        vec[:, k * 128:(k + 1) * 128] = s
    vcp = pltpu.make_async_copy(vec, vec_out, out_sem.at[7])
    vcp.start()

    def load(w, st):
        return pltpu.make_async_copy(g_ref.at[w, st], wf.at[st], ld_sem.at[st])

    def ws_copy(w, st):
        return pltpu.make_async_copy(ws.at[st], ws_out.at[w, st], ws_sem.at[st])

    def weights(w):
        for st in range(2):
            ga.ready(w, st)
            load(w, st).start()

    def half(w, st, s):
        load(w, st).wait()

        @pl.when(w > 0)
        def _():
            ws_copy(w - 1, st).wait()

        @pl.loop(0, at.NZ)
        def _(z):
            for y in range(at.NY):
                for x in range(at.NX):
                    r0 = pl.multiple_of(((z * at.NY + y) * at.NX + x) * R, R)
                    h, l = split(wf[st, z, y, x])
                    ws[st, 0, pl.ds(r0, R)] = h
                    ws[st, 1, pl.ds(r0, R)] = l
        ws_copy(w, st).start()
        acc[...] = three(lh[s, 0], lh[s, 1], ws[st, 0], ws[st, 1])

    @pl.loop(0, 3)
    def _(t):
        ga.step(t)

    def qkv_copy(w):
        return pltpu.make_async_copy(qkv.at[w], qkv_out.at[w], out_sem.at[8 + w])

    @pl.loop(0, 3)
    def _(w):
        ga.step(w + 3)
        weights(w)
        f = jnp.where(w == 0, 1.0 / math.sqrt(HD), 1.0).astype(F32)
        for st in range(2):
            half(w, st, X_)
            b = vec[pl.ds(w, 1), st * HB:(st + 1) * HB]
            qkv[w, :, st * HB:(st + 1) * HB] = (acc[...] + b) * f
        qkv_copy(w).start()

    def p_copy(p):
        return pltpu.make_async_copy(pst.at[p % 2], p_out.at[p], p_sem.at[p % 2])

    def attend(p):
        c = cols(p * 128, 128)
        qp, kp, vp = qkv[0, :, c], qkv[1, :, c], qkv[2, :, c]
        qs, ks, vt = pack_hhl(qp), pack_hl0(kp), stack_t(vp)

        @pl.when(p >= 2)
        def _():
            p_copy(p - 2).wait()
        res = []
        for k in range(2):
            s = mx(ks[k], qs[k], NT) + bias[...]
            e = jnp.exp(s - jnp.max(s, axis=0, keepdims=True))
            e = e * (1.0 / jnp.sum(e, axis=0, keepdims=True))
            ph, pll = split(e)
            pst[p % 2, k, 0] = ph
            pst[p % 2, k, 1] = pll
            res.append(mx(vt[k], ph) + mx(vt[k], pll))
        p_copy(p).start()
        h, l = split(fold_t(*res))
        lh[C_, 0, :, c] = h
        lh[C_, 1, :, c] = l

    @pl.loop(0, 2)
    def _(a):
        ga.step(a + 6)

        @pl.loop(0, H // 4)
        def _(j):
            attend(a * (H // 4) + j)
    lh_copy(C_).start()

    ga.step(8)
    weights(3)
    for st in range(2):
        half(3, st, C_)
        c = slice(st * HB, (st + 1) * HB)
        n1[:, c] = x_ref[:, c] + acc[...] + vec[ROW_P:ROW_P + 1, c]

    def norm_rows(ref, k, hat_ref, rows):
        v = ref[rows]
        center = v - jnp.mean(v, axis=-1, keepdims=True)
        inverse = lax.rsqrt(jnp.mean(center * center, axis=-1, keepdims=True) + EPSILON)
        hat = center * inverse
        return hat, inverse

    @pl.loop(0, L // RB)
    def _(r):
        rows = pl.ds(pl.multiple_of(r * RB, RB), RB)
        hat, inverse = norm_rows(n1, 0, None, rows)
        r2[rows] = hat
        inv_out[rows, 0:128] = jnp.broadcast_to(inverse, (RB, 128))
        v = hat * vec[ROW_G1:ROW_G1 + 1] + vec[ROW_S1:ROW_S1 + 1]
        n1[rows] = v
        h, l = split(v)
        lh[N_, 0, rows] = h
        lh[N_, 1, rows] = l
    lh_copy(N_).start()
    hcp = pltpu.make_async_copy(r2, hat1_out, out_sem.at[11])
    hcp.start()

    def sl_copy(j, st):
        return pltpu.make_async_copy(slope.at[st], sl_out.at[j, st], sl_sem.at[st])

    @pl.loop(0, 4)
    def _(j):
        @pl.when(j % 2 == 1)
        def _():
            ga.step(8 + (j + 1) // 2)
        weights(4 + j)
        for st in range(2):
            half(4 + j, st, N_)
            c = slice(st * HB, (st + 1) * HB)

            @pl.when(j > 0)
            def _():
                sl_copy(j - 1, st).wait()
            b = vec[pl.ds(ROW_U + j, 1), c]

            @pl.loop(0, L // 64)
            def _(r):
                rows = pl.ds(pl.multiple_of(r * 64, 64), 64)
                u = acc[rows] + b
                phi = 0.5 * (1.0 + lax.erf(u * math.sqrt(0.5)))
                h, l = split(u * phi)
                lh[A_ + j, 0, rows, c] = h
                lh[A_ + j, 1, rows, c] = l
                slope[st, rows] = phi + u * jnp.exp(-0.5 * u * u) * (1.0 / math.sqrt(2.0 * math.pi))
            sl_copy(j, st).start()
        lh_copy(A_ + j).start()

    hcp.wait()
    r2[...] = n1[...] + vec[ROW_D:ROW_D + 1]

    @pl.loop(0, 4)
    def _(j):
        ga.step(11 + j)
        weights(8 + j)
        for st in range(2):
            half(8 + j, st, A_ + j)
            r2[:, st * HB:(st + 1) * HB] += acc[...]

    @pl.loop(0, L // RB)
    def _(r):
        rows = pl.ds(pl.multiple_of(r * RB, RB), RB)
        hat, inverse = norm_rows(r2, 1, None, rows)
        r2[rows] = hat
        inv_out[rows, 128:256] = jnp.broadcast_to(inverse, (RB, 128))
        out_ref[rows] = hat * vec[ROW_G2:ROW_G2 + 1] + vec[ROW_S2:ROW_S2 + 1]
    hcp2 = pltpu.make_async_copy(r2, hat2_out, out_sem.at[11])
    hcp2.start()
    vcp.wait()
    for s in range(7):
        lh_copy(s).wait()
    for w in range(3):
        qkv_copy(w).wait()
    for p in (H // 2 - 2, H // 2 - 1):
        p_copy(p).wait()
    for st in range(2):
        sl_copy(3, st).wait()
        ws_copy(NW - 1, st).wait()
    hcp2.wait()
    ga.finish()


def forward(n, x, w, v, segr, segc, okc):
    nz, ny, nx = torus(n)
    _, _, R, HB = w.shape
    L, D = x.shape
    S = lambda shape, t=F32: jax.ShapeDtypeStruct(shape, t)
    V = pltpu.VMEM
    ANY = pl.BlockSpec(memory_space=pl.ANY)
    VM = pl.BlockSpec(memory_space=pltpu.VMEM)
    return pl.pallas_call(
        functools.partial(forward_kernel, n),
        out_shape=[S((L, D)), S((NW, 2, nz, ny, nx, R, HB)), S((nz, ny, nx) + v.shape), S((7, 2, L, D), BF),
                   S((NW, 2, 2, D, HB), BF), S((3, L, D)), S((H // 2, 2, 2, L, L), BF), S((4, 2, L, HB)),
                   S((L, D)), S((L, D)), S((L, 256)), S((v.shape[0], D))],
        in_specs=[VM] * 6,
        out_specs=[VM] + [ANY] * 9 + [VM, ANY],
        scratch_shapes=[V((7, 2, L, D), BF), V((2, nz, ny, nx, R, HB), F32), V((2, 2, D, HB), BF), V((3, L, D), F32),
                        V((L, HB), F32), V((L, D), F32), V((L, D), F32), V((2, L, HB), F32), V((2, 2, 2, L, L), BF),
                        V((L, L), F32), V((nz, ny, nx) + v.shape, F32), V((v.shape[0], D), F32),
                        DMA((2,)), DMA((2,)), DMA((12,)), DMA((2,)), DMA((2,))] + Gather.sems(n),
        compiler_params=pltpu.CompilerParams(collective_id=0, has_side_effects=True, vmem_limit_bytes=63 * 2**20),
        name="forward",
    )(x, w, v, segr, segc, okc)


E_U, E_P, E_Q = 8, 16, 18
E_PAIR = 9
R_R2, R_U, R_R1, R_Q = 0, 1, 5, 6


def backward_kernel(n, scale, ct_ref, hat2_ref, hat1_ref, inv_ref, lh_ref, ws_ref, qkv_ref, p_ref, sl_ref, vec,
                    dx_ref, o_ref, ov_ref, rhs_ref, h0, h1, h2, h3,
                    lbuf, rbuf, wbuf, sbuf, pbuf, qbuf, dr2, du, dn1, fb, dst, small,
                    l_sem, r_sem, w_sem, s_sem, p_sem, q_sem, f_sem, o_sem, d_sem, *rest):
    at = Where(n)
    bufs, sems = rest[:17], rest[17:]
    rd = Reduce(at, o_ref, ov_ref, (h0, h1, h2, h3), bufs, sems, scale)
    L, D = ct_ref.shape
    HB = D // 2
    RB = 128
    FB = D // at.NZ
    copy = pltpu.make_async_copy

    def f_load(src, k):
        return copy(src, fb.at[k], f_sem.at[k])

    def lhs_slot(e):
        return jnp.where(e < E_U, A_ + e // 2, jnp.where(e < E_P, N_, jnp.where(e < E_Q, C_, X_)))

    def rhs_slot(e):
        return jnp.where(e < E_U, R_R2, jnp.where(e < E_P, R_U + (e - E_U) // 2, jnp.where(e < E_Q, R_R1, R_Q + (e - E_Q) % 3)))

    def rhs_half(e):
        return jnp.where(e < E_Q, e % 2, (e - E_Q) // 3)

    def l_load(e):
        return copy(lh_ref.at[lhs_slot(e)], lbuf.at[e % 2], l_sem.at[e % 2])

    def r_load(e):
        return copy(rhs_ref.at[rhs_slot(e), :, :, cols(rhs_half(e) * HB, HB)], rbuf.at[e % 2], r_sem.at[e % 2])

    def w_load(e, k):
        pairs = jnp.where(e < E_U, jnp.where(e % 2 == 0, 8, 4) + e // 2, 3)
        w = jnp.where(e < E_Q, pairs, (e - E_Q) % 3)
        h = jnp.where(e < E_Q, k, (e - E_Q) // 3)
        return copy(ws_ref.at[w, h], wbuf.at[e % 2, k], w_sem.at[e % 2, k])

    def s_load(j):
        return copy(sl_ref.at[j], sbuf, s_sem)

    def p_load(p):
        return copy(p_ref.at[p], pbuf.at[p % 2], p_sem.at[p % 2])

    def q_load(p):
        return copy(qkv_ref.at[:, :, cols(p * 128, 128)], qbuf.at[p % 2], q_sem.at[p % 2])

    def rhs_store(src, slot, k):
        return copy(src, rhs_ref.at[slot], o_sem.at[k])

    f_load(ct_ref, 0).start()
    f_load(hat2_ref, 1).start()
    l_load(0).start()
    for k in range(2):
        w_load(0, k).start()
    s_load(0).start()
    at.barrier()
    small[...] = jnp.zeros_like(small)
    f_load(ct_ref, 0).wait()
    f_load(hat2_ref, 1).wait()

    def norm_back(r, g, hat, inverse, gain, row_shift, row_gain):
        gg = g * gain
        small[row_shift:row_shift + 1] += jnp.sum(g, axis=0, keepdims=True)
        small[row_gain:row_gain + 1] += jnp.sum(g * hat, axis=0, keepdims=True)
        return inverse * (gg - jnp.mean(gg, -1, keepdims=True) - hat * jnp.mean(gg * hat, -1, keepdims=True))

    @pl.loop(0, L // RB)
    def _(r):
        rows = pl.ds(pl.multiple_of(r * RB, RB), RB)
        d = norm_back(r, fb[0, rows], fb[1, rows], inv_ref[rows, 128:129], vec[ROW_G2:ROW_G2 + 1], ROW_S2, ROW_G2)
        small[ROW_D:ROW_D + 1] += jnp.sum(d, axis=0, keepdims=True)
        dn1[rows] = d
        h, l = split(d)
        dr2[0, rows] = h
        dr2[1, rows] = l
    rhs_store(dr2, R_R2, 0).start()
    f_load(hat1_ref, 0).start()
    rhs_store(dr2, R_R2, 0).wait()
    r_load(0).start()

    def chunk_da(j, e):
        for k in range(2):
            w_load(e, k).wait()
        s_load(j).wait()

        @pl.when(j > 0)
        def _():
            rhs_store(du, R_U + j - 1, 1).wait()
        for k in range(4):
            b = slice(k * FB, (k + 1) * FB)
            v = three(dr2[0, :, :HB], dr2[1, :, :HB], wbuf[e % 2, 0, 0, b], wbuf[e % 2, 0, 1, b], NT) \
                + three(dr2[0, :, HB:], dr2[1, :, HB:], wbuf[e % 2, 1, 0, b], wbuf[e % 2, 1, 1, b], NT)
            half, off = (k * FB) // HB, (k * FB) % HB
            v = v * sbuf[half, :, off:off + FB]
            small[pl.ds(ROW_U + j, 1), b] = jnp.sum(v, axis=0, keepdims=True)
            h, l = split(v)
            du[0, :, b] = h
            du[1, :, b] = l
        rhs_store(du, R_U + j, 1).start()

        @pl.when(j < 3)
        def _():
            s_load(j + 1).start()

    def nt_into(ref, a, e, b):
        return ref[:, b] + three(a[0, :, :HB], a[1, :, :HB], wbuf[e % 2, 0, 0, b], wbuf[e % 2, 0, 1, b], NT) \
            + three(a[0, :, HB:], a[1, :, HB:], wbuf[e % 2, 1, 0, b], wbuf[e % 2, 1, 1, b], NT)

    def chunk_dn(e):
        for k in range(2):
            w_load(e, k).wait()
        for k in range(4):
            b = slice(k * FB, (k + 1) * FB)
            dn1[:, b] = nt_into(dn1, du, e, b)

    def chunk_norm():
        f_load(hat1_ref, 0).wait()

        @pl.loop(0, L // RB)
        def _(r):
            rows = pl.ds(pl.multiple_of(r * RB, RB), RB)
            d = norm_back(r, dn1[rows], fb[0, rows], inv_ref[rows, 0:1], vec[ROW_G1:ROW_G1 + 1], ROW_S1, ROW_G1)
            small[ROW_P:ROW_P + 1] += jnp.sum(d, axis=0, keepdims=True)
            dn1[rows] = d
            h, l = split(d)
            dr2[0, rows] = h
            dr2[1, rows] = l
        rhs_store(du, R_U + 3, 1).wait()
        rhs_store(dr2, R_R1, 0).start()

    def chunk_dc(e):
        for k in range(2):
            w_load(e, k).wait()
        for k in range(4):
            b = slice(k * FB, (k + 1) * FB)
            fb[1, :, b] = three(dr2[0, :, :HB], dr2[1, :, :HB], wbuf[e % 2, 0, 0, b], wbuf[e % 2, 0, 1, b], NT) \
                + three(dr2[0, :, HB:], dr2[1, :, HB:], wbuf[e % 2, 1, 0, b], wbuf[e % 2, 1, 1, b], NT)
        rhs_store(dr2, R_R1, 0).wait()

    def d_store(p, k):
        return copy(dst.at[p % 2, k], rhs_ref.at[R_Q + k, :, :, cols(p * 128, 128)], d_sem.at[p % 2, k])

    def chunk_pair(p):
        c = cols(p * 128, 128)
        s = p % 2
        p_load(p).wait()
        q_load(p).wait()

        @pl.when(p < H // 2 - 1)
        def _():
            p_load(p + 1).start()
            q_load(p + 1).start()
        qp, kp, vp, dc = qbuf[s, 0], qbuf[s, 1], qbuf[s, 2], fb[1, :, c]
        va, da, kt, qx, dx = pack_hl0(vp), pack_hhl(dc), stack_t(kp), pack_hl(qp), pack_hl(dc)
        dq, dk, dv = [], [], []
        for k in range(2):
            dp = mx(va[k], da[k], NT)
            ph, pll = pbuf[s, k, 0], pbuf[s, k, 1]
            pf = ph.astype(F32) + pll.astype(F32)
            t = pf * dp
            t = t - pf * jnp.sum(t, axis=0, keepdims=True)
            sh, sll = split(t)
            dk.append(mx(sh, qx[k]) + mx(sll, qx[k]))
            dv.append(mx(ph, dx[k]) + mx(pll, dx[k]))
            dq.append(mx(kt[k], sh) + mx(kt[k], sll))
        out = (fold_t(*dq) * (1.0 / math.sqrt(HD)), fold(*dk), fold(*dv))

        @pl.when(p >= 2)
        def _():
            for k in range(3):
                d_store(p - 2, k).wait()
        for k in range(3):
            small[k:k + 1, c] = jnp.sum(out[k], axis=0, keepdims=True)
            h, l = split(out[k])
            dst[s, k, 0] = h
            dst[s, k, 1] = l
            d_store(p, k).start()

    def chunk_dx(e):
        w_load(e, 0).wait()
        for k in range(4):
            b = slice(k * FB, (k + 1) * FB)
            dn1[:, b] += three(rbuf[e % 2, 0], rbuf[e % 2, 1], wbuf[e % 2, 0, 0, b], wbuf[e % 2, 0, 1, b], NT)

    @pl.loop(0, NI + LAG[4])
    def _(e):
        @pl.when(e < NI)
        def _():
            l_load(e).wait()
            r_load(e).wait()

            @pl.when(e >= 2)
            def _():
                rd.hop0(e - 2).wait_send()

            @pl.loop(0, at.NZ)
            def _(z):
                b = cols(z * FB, FB)
                v = three(lbuf[e % 2, 0, :, b], lbuf[e % 2, 1, :, b], rbuf[e % 2, 0], rbuf[e % 2, 1], TN)
                rd.p[e % 2, z] = v.reshape(rd.p.shape[2:])
            rd.send(e)

            @pl.when(e < NI - 1)
            def _():
                l_load(e + 1).start()
                r_load(e + 1).start()

            @pl.when((e < E_U) | ((e >= E_Q - 1) & (e < NI - 1)))
            def _():
                w_load(e + 1, 0).start()

            @pl.when(e < E_U)
            def _():
                w_load(e + 1, 1).start()

        @pl.when((e < E_U) & (e % 2 == 0))
        def _():
            chunk_da(e // 2, e)

        @pl.when((e < E_U) & (e % 2 == 1))
        def _():
            chunk_dn(e)

        @pl.when(e == E_U - 1)
        def _():
            chunk_norm()

        @pl.when(e == E_U)
        def _():
            p_load(0).start()
            q_load(0).start()
            chunk_dc(e)

        @pl.when((e >= E_PAIR) & (e < E_PAIR + H // 2))
        def _():
            chunk_pair(e - E_PAIR)

        @pl.when(e == E_PAIR + H // 2)
        def _():
            for p in (H // 2 - 2, H // 2 - 1):
                for k in range(3):
                    d_store(p, k).wait()
            for z in range(at.NZ):
                for y in range(at.NY):
                    for x in range(at.NX):
                        g = ((z * at.NY + y) * at.NX + x) * 2 * rd.RH // 128
                        rd.v0[z, y, x] = small[:, g * 128:(g + 1) * 128]

        for k in range(5):
            @pl.when(e == E_PAIR + H // 2 + k)
            def _():
                rd.small(k)

        @pl.when((e >= E_Q) & (e < NI))
        def _():
            chunk_dx(e)

        @pl.when(e == NI - 1)
        def _():
            copy(dn1, dx_ref, o_sem.at[0]).start()
        rd.step(e)
    copy(dn1, dx_ref, o_sem.at[0]).wait()
    rd.finish()
    rd.small_finish()


def backward(n, R, scale, ct, hat2, hat1, inv, lh, ws, qkv, p, sl, vec):
    L, D = ct.shape
    HB = D // 2
    VR = vec.shape[0]
    S = lambda shape, t=F32: jax.ShapeDtypeStruct(shape, t)
    V = pltpu.VMEM
    ANY = pl.BlockSpec(memory_space=pl.ANY)
    VM = pl.BlockSpec(memory_space=pltpu.VMEM)
    return pl.pallas_call(
        functools.partial(backward_kernel, n, scale),
        out_shape=[S((L, D)), S((NI, R, HB)), S((VR, 128)), S((9, 2, L, D), BF)] + Reduce.recv_shapes(n, R, HB),
        in_specs=[ANY, ANY, ANY, VM, ANY, ANY, ANY, ANY, ANY, VM],
        out_specs=[ANY, ANY, VM, ANY, ANY, ANY, ANY, ANY],
        scratch_shapes=[V((2, 2, L, D), BF), V((2, 2, L, HB), BF), V((2, 2, 2, D, HB), BF), V((2, L, HB), F32),
                        V((2, 2, 2, L, L), BF), V((2, 3, L, 128), F32), V((2, L, D), BF), V((2, L, D), BF), V((L, D), F32),
                        V((2, L, D), F32), V((2, 3, 2, L, 128), BF), V((VR, D), F32),
                        DMA((2,)), DMA((2,)), DMA((2, 2)), DMA(()), DMA((2,)), DMA((2,)), DMA((2,)), DMA((2,)), DMA((2, 3))]
        + Reduce.bufs(n, R, HB, VR) + Reduce.sems(n),
        compiler_params=pltpu.CompilerParams(collective_id=1, has_side_effects=True, vmem_limit_bytes=63 * 2**20),
        name="backward",
    )(ct, hat2, hat1, inv, lh, ws, qkv, p, sl, vec)[:3]


def pack_weights(n, qkv, proj, up, down):
    R, D = proj.shape
    J = up.shape[1] // D
    q3 = qkv.reshape(R, 3, D).transpose(1, 0, 2)
    u4 = up.reshape(R, n, J, R).transpose(2, 0, 1, 3).reshape(J, R, D)
    d4 = down.reshape(J, R, D)
    w = jnp.concatenate([q3, proj[None], u4, d4], axis=0)
    return w.reshape(NW, R, 2, D // 2).transpose(0, 2, 1, 3)


def unpack_grads(n, o):
    _, R, HB = o.shape
    D, J = 2 * HB, 4
    down = o[:E_U].reshape(J, 2, R, HB).transpose(0, 2, 1, 3).reshape(J * R, D)
    up = o[E_U:E_P].reshape(J, 2, R, n // 2, R).transpose(2, 1, 3, 0, 4).reshape(R, n * J * R)
    proj = o[E_P:E_Q].transpose(1, 0, 2).reshape(R, D)
    qkv = o[E_Q:].reshape(2, 3, R, HB).transpose(2, 1, 0, 3).reshape(R, 3 * D)
    return qkv, proj, up, down


VROWS = 16


def lane(R):
    return (lax.axis_index("shard") * R) % 128


def pack_small(before, up_bias, after):
    R = before[0].shape[0]
    rows = jnp.concatenate([jnp.stack(before), up_bias.reshape(4, R), jnp.stack(after)])
    wide = jnp.zeros((VROWS, 128), F32)
    return lax.dynamic_update_slice(wide, jnp.pad(rows, ((0, VROWS - rows.shape[0]), (0, 0))), (0, lane(R)))


def shards(n, tokens, segment_ids, valid_lengths, qkv_weight, query_bias, value_bias, proj_weight, proj_bias, first_gain,
           first_shift, up_weight, up_bias, down_weight, down_bias, second_gain, second_shift, cotangent):
    amount, length, D = tokens.shape
    R = proj_weight.shape[0]
    x = tokens.reshape(amount * length, D)
    seg = segment_ids.reshape(1, length)
    ok = (jnp.arange(length, dtype=jnp.int32) < valid_lengths[0]).astype(jnp.int32)
    wsh = pack_weights(n, qkv_weight, proj_weight, up_weight, down_weight)
    vsh = pack_small([query_bias, jnp.zeros_like(query_bias), value_bias, proj_bias, first_gain, first_shift], up_bias,
                     [down_bias, second_gain, second_shift])
    out, g, gv, lh, ws, qkv, pr, sl, hat1, hat2, inv, v = forward(n, x, wsh, vsh, seg, seg.reshape(length, 1), ok.reshape(length, 1))
    scale = 1.0 / math.sqrt(amount * length * n * lax.axis_size("rep"))
    dx, o, ov = backward(n, R, scale, cotangent.reshape(amount * length, D), hat2, hat1, inv, lh, ws, qkv, pr, sl, v)
    gqkv, gproj, gup, gdown = unpack_grads(n, o)
    s = lax.dynamic_slice(ov, (0, lane(R)), (VROWS, R))
    return (out.reshape(amount, length, D), dx.reshape(amount, length, D), gqkv, s[0], s[2], gproj, s[3], s[4], s[5], gup,
            s[6:10].reshape(4 * R), gdown, s[10], s[11], s[12])


def solution(mesh):
    n = mesh.shape["shard"]
    one, two, seq = P("shard"), P("shard", None), P(("shard", "rep"), None, None)
    return jax.shard_map(
        functools.partial(shards, n),
        mesh=mesh,
        in_specs=(seq, P(("shard", "rep"), None), P(("shard", "rep")), two, one, one, two, one, one, one, two, one, two, one, one, one, seq),
        out_specs=(seq, seq, two, one, one, two, one, one, one, two, one, two, one, one, one),
        check_vma=False,
    )
```

```python
import functools
import math

import jax
import jax.numpy as jnp
from jax import lax
from jax.experimental import pallas as pl
from jax.experimental.pallas import tpu as pltpu
from jax.sharding import PartitionSpec as P

H = 16
HD = 64
HIGH = lax.Precision.HIGH
EPSILON = 1e-05
MASKED = -1000000000.0
MESH = pl.DeviceIdType.MESH
DMA = pltpu.SemaphoreType.DMA
F32 = jnp.float32
VMEM_LIMIT = 60 * 2**20
NW = 12


def torus(n):
    side = math.isqrt(n // 4)
    assert side * side * 4 == n
    return 4, side, side


def ds(start, size, align=8):
    return pl.ds(pl.multiple_of(start, align), size)


class Where:
    def __init__(self, n):
        self.NZ, self.NY, self.NX = torus(n)
        s = lax.axis_index("shard")
        self.s = s
        self.c = lax.axis_index("rep")
        self.z = s // (self.NY * self.NX)
        self.y = (s // self.NX) % self.NY
        self.x = s % self.NX

    def dev(self, z=None, y=None, x=None, c=None):
        z = self.z if z is None else z
        y = self.y if y is None else y
        x = self.x if x is None else x
        c = self.c if c is None else c
        return (z * (self.NY * self.NX) + y * self.NX + x, c)

    def partners(self):
        out = [self.dev(c=1 - self.c)]
        out += [self.dev(z=p) for p in self.others("z")]
        out += [self.dev(y=p) for p in self.others("y")]
        out += [self.dev(x=p) for p in self.others("x")]
        return out

    def others(self, axis):
        me, n = self.line(axis)
        return [(me + d) % n for d in range(1, n)]

    def line(self, axis):
        return {"z": (self.z, self.NZ), "y": (self.y, self.NY), "x": (self.x, self.NX)}[axis]

    def barrier(self):
        sem = pltpu.get_barrier_semaphore()
        ps = self.partners()
        for p in ps:
            pl.semaphore_signal(sem, inc=1, device_id=p, device_id_type=MESH)
        pl.semaphore_wait(sem, len(ps))


def remote(src, dst, ssem, rsem, dev):
    return pltpu.make_async_remote_copy(
        src_ref=src, dst_ref=dst, send_sem=ssem, recv_sem=rsem, device_id=dev, device_id_type=MESH
    )


NI = 2 * NW


def z_first(i):
    w = i // 2
    return (w % 2 == 1) & (w < NW - 1)


class Item:
    def __init__(self, at, i):
        swap = i % 2 == 1
        self.i, self.at, self.n = i, at, at.NX
        self.a = jnp.where(swap, at.x, at.y)
        self.b = jnp.where(swap, at.y, at.x)
        self.swap = swap

    def chip(self, z, a, b):
        return (z * self.n + jnp.where(self.swap, b, a)) * self.n + jnp.where(self.swap, a, b)

    def along_a(self, q):
        return (self.chip(self.at.z, q, self.b), self.at.c)

    def along_b(self, q):
        return (self.chip(self.at.z, self.a, q), self.at.c)

    def others_a(self):
        return [(self.a + d) % self.n for d in range(1, self.n)]

    def others_b(self):
        return [(self.b + d) % self.n for d in range(1, self.n)]


class Line:
    def __init__(self, at):
        assert at.NZ == 4
        self.z = at.z
        self.others = at.others("z")
        self.middle = (at.z == 1) | (at.z == 2)
        self.far = jnp.where(at.z == 2, 0, 3)
        self.near = jnp.where(at.z == 2, 3, 0)
        self.end = jnp.where(at.z == 0, 3, 0)
        self.relay = jnp.where(at.z == 0, 1, 2)

    def direct(self, p):
        return jnp.abs(p - self.z) != 3


G_LAG = {1: 0, 2: 2, 3: 4, 4: 7}
G_AHEAD = 3


class Gather:
    def __init__(self, at, w_ref, g_ref, v_ref, gv_ref, sems):
        self.at, self.w, self.g, self.v, self.gv = at, w_ref, g_ref, v_ref, gv_ref
        (self.l, self.zs, self.zr, self.zx, self.s_a, self.r_a, self.s_b, self.r_b, self.ss, self.rs, self.vs, self.vr) = sems
        R = w_ref.shape[1]
        self.RH = R // 2
        self.half = ds(at.c * self.RH, self.RH)
        self.other = ds((1 - at.c) * self.RH, self.RH)
        self.line = Line(at)

    @staticmethod
    def sems(n):
        nz, ny, nx = torus(n)
        return [DMA((NI + 1,)), DMA((NI, nz)), DMA((NI, nz)), DMA((NI,)), DMA((NI, nx)), DMA((NI, nx)),
                DMA((NI, nx)), DMA((NI, nx)), DMA((NI,)), DMA((NI,)), DMA((3, nz)), DMA((3, nz))]

    def local(self, i):
        t = Item(self.at, i)
        return pltpu.make_async_copy(self.w.at[i, self.half], self.g.at[i, self.at.z, t.a, t.b, self.half], self.l.at[i])

    def local_v(self):
        a = self.at
        return pltpu.make_async_copy(self.v, self.gv.at[a.z, a.y, a.x], self.l.at[NI])

    def own(self, i, z):
        pass

    def zhop(self, i, first, p, recv=False):
        t, z = Item(self.at, i), self.at.z
        o = p if recv else z
        sems = (self.zs.at[i, p], self.zr.at[i, o], self.at.dev(z=p))
        if first:
            return remote(self.w.at[i, self.half], self.g.at[i, o, t.a, t.b, self.half], *sems)
        return remote(self.g.at[i, o, :, t.b, self.half], self.g.at[i, o, :, t.b, self.half], *sems)

    def zrelay(self, i, first):
        t, o, p = Item(self.at, i), self.line.far, self.line.near
        ref = self.g.at[i, o, t.a, t.b, self.half] if first else self.g.at[i, o, :, t.b, self.half]
        return remote(ref, ref, self.zx.at[i], self.zr.at[i, o], self.at.dev(z=p))

    def ahop(self, i, first, q, recv=False):
        t, z = Item(self.at, i), self.at.z
        o = q if recv else t.a
        sems = (self.s_a.at[i, q], self.r_a.at[i, o], t.along_a(q))
        if first:
            return remote(self.g.at[i, :, o, t.b, self.half], self.g.at[i, :, o, t.b, self.half], *sems)
        return remote(self.w.at[i, self.half], self.g.at[i, z, o, t.b, self.half], *sems)

    def bhop(self, i, q, recv=False):
        t = Item(self.at, i)
        o = q if recv else t.b
        ref = self.g.at[i, :, :, o, self.half]
        return remote(ref, ref, self.s_b.at[i, q], self.r_b.at[i, o], t.along_b(q))

    def pair(self, i, recv=False):
        ref = self.g.at[i, :, :, :, self.other if recv else self.half]
        return remote(ref, ref, self.ss.at[i], self.rs.at[i], self.at.dev(c=1 - self.at.c))

    def small(self, hop, p, recv=False):
        a, g = self.at, self.gv
        if hop == 0:
            o = p if recv else a.z
            return remote(self.v, g.at[o, a.y, a.x], self.vs.at[0, p], self.vr.at[0, o], a.dev(z=p))
        if hop == 1:
            o = p if recv else a.x
            return remote(g.at[:, a.y, a.x], g.at[:, a.y, o], self.vs.at[1, p], self.vr.at[1, o], a.dev(x=p))
        o = p if recv else a.y
        return remote(g.at[:, a.y], g.at[:, o], self.vs.at[2, p], self.vr.at[2, o], a.dev(y=p))

    def z_send(self, i, first):
        for p in self.line.others:
            @pl.when(self.line.direct(p))
            def _():
                self.zhop(i, first, p).start()

    def z_pass(self, i, first):
        @pl.when(self.line.middle)
        def _():
            self.zhop(i, first, self.line.far, True).wait_recv()
            self.zrelay(i, first).start()

    def z_wait(self, i, first):
        for p in self.line.others:
            @pl.when(~(self.line.middle & (p == self.line.far)))
            def _():
                self.zhop(i, first, p, True).wait_recv()

    def a_send(self, i, first):
        for q in Item(self.at, i).others_a():
            self.ahop(i, first, q).start()

    def a_wait(self, i, first):
        for q in Item(self.at, i).others_a():
            self.ahop(i, first, q, True).wait_recv()

    def begin_local(self):
        self.local_v().start()

        @pl.loop(0, NI)
        def _(i):
            self.local(i).start()

    def begin(self):
        for p in self.at.others("z"):
            self.small(0, p).start()

        @pl.loop(0, NI)
        def _(i):
            @pl.when((i < G_AHEAD) | ~z_first(i))
            def _():
                self.stage(0, i)

    def small_step(self, hop):
        a = self.at
        here, nxt = (("z", "x"), ("x", "y"), ("y", None))[hop]
        if hop == 0:
            self.local_v().wait()
        for p in a.others(here):
            self.small(hop, p, True).wait_recv()
        if nxt:
            for p in a.others(nxt):
                self.small(hop + 1, p).start()

    def stage(self, k, i):
        if k == 4:
            for q in Item(self.at, i).others_b():
                self.bhop(i, q, True).wait_recv()
            self.pair(i).start()
            return
        first = z_first(i)

        @pl.when(first)
        def _():
            if k == 0:
                self.z_send(i, True)
            elif k == 1:
                self.z_pass(i, True)
            elif k == 2:
                self.z_wait(i, True)
                self.local(i).wait()
                self.a_send(i, True)
            else:
                self.a_wait(i, True)

        @pl.when(~first)
        def _():
            if k == 0:
                self.a_send(i, False)
            elif k == 1:
                self.a_wait(i, False)
                self.local(i).wait()
                self.z_send(i, False)
            elif k == 2:
                self.z_pass(i, False)
            else:
                self.z_wait(i, False)
        if k == 3:
            for q in Item(self.at, i).others_b():
                self.bhop(i, q).start()

    def ready(self, i):
        self.pair(i, True).wait_recv()

    def step(self, t):
        @pl.when((t + G_AHEAD < NI) & z_first(t + G_AHEAD))
        def _():
            self.z_send(t + G_AHEAD, True)
        for k in (1, 2, 3, 4):
            @pl.when((t >= G_LAG[k]) & (t < NI + G_LAG[k]))
            def _():
                self.stage(k, t - G_LAG[k])
        for hop in range(3):
            @pl.when(t == hop + 1)
            def _():
                self.small_step(hop)

    def finish(self):
        a = self.at
        for hop, here in ((0, "z"), (1, "x"), (2, "y")):
            for p in a.others(here):
                self.small(hop, p).wait_send()

        @pl.loop(0, NI)
        def _(i):
            self.pair(i).wait_send()
            t = Item(a, i)
            for q in t.others_b():
                self.bhop(i, q).wait_send()
            first = z_first(i)
            for f in (True, False):
                @pl.when(first if f else ~first)
                def _():
                    for q in t.others_a():
                        self.ahop(i, f, q).wait_send()
                    for p in self.line.others:
                        @pl.when(self.line.direct(p))
                        def _():
                            self.zhop(i, f, p).wait_send()

                    @pl.when(self.line.middle)
                    def _():
                        self.zrelay(i, f).wait_send()


SLOTS = 8
PS = 3
LAG = {1: 1, 2: 4, 3: 7, 4: 9, 5: 11}


class Reduce:
    def __init__(self, at, o_ref, ov_ref, r_refs, bufs, sems, scale):
        self.at, self.o, self.ov, self.scale = at, o_ref, ov_ref, scale
        self.h0, self.hb, self.ha, self.hz, self.hx = r_refs
        (self.p, self.a1, self.a2, self.a3, self.a4, self.l0, self.lb, self.la, self.lz, self.lx,
         self.v0, self.v1, self.v2, self.v3, self.w0, self.w1, self.w2, self.w3) = bufs
        (self.s0, self.r0, self.s_b, self.r_b, self.s_a, self.r_a, self.s_z, self.r_z, self.s_x, self.r_x, self.s4, self.r4,
         self.ls, self.os, self.vs, self.vr) = sems
        self.RH = o_ref.shape[1] // 2
        self.half = ds(at.c * self.RH, self.RH)
        self.other = ds((1 - at.c) * self.RH, self.RH)
        self.line = Line(at)

    @staticmethod
    def recv_shapes(n, R, CB):
        nz, m, nx = torus(n)
        RH = R // 2
        S = lambda *s: jax.ShapeDtypeStruct(s, F32)
        return [S(NI, nz, m, m, RH, CB), S(NI, m, nz, m, RH, CB), S(NI, m, nz, RH, CB), S(NI, nz, m, RH, CB), S(NI, m, RH, CB)]

    @staticmethod
    def bufs(n, R, CB, VR):
        nz, m, nx = torus(n)
        assert nx == m
        RH = R // 2
        V = lambda *s: pltpu.VMEM(s, F32)
        return [V(PS, nz, m, m, R, CB), V(4, nz, m, m, RH, CB), V(SLOTS, nz, m, RH, CB), V(SLOTS, nz, RH, CB), V(SLOTS, RH, CB),
                V(nz, m, m, RH, CB), V(m, nz, m, RH, CB), V(m, nz + 1, RH, CB), V(nz, m + 1, RH, CB), V(m + 1, RH, CB),
                V(nz, m, m, VR, 128), V(nz, m, m, VR, 128), V(nz, m, VR, 128), V(nz, VR, 128),
                V(nz, m, m, VR, 128), V(m, nz, m, VR, 128), V(m, nz, VR, 128), V(nz, VR, 128)]

    @staticmethod
    def sems(n):
        nz, m, nx = torus(n)
        return [DMA((NI,)), DMA((NI,)), DMA((NI, m)), DMA((NI, m)), DMA((NI, m)), DMA((NI, m)),
                DMA((NI, nz)), DMA((NI, nz)), DMA((NI,)), DMA((NI,)), DMA((NI,)), DMA((NI,)),
                DMA((8, nz)), DMA((NI,)), DMA((4, nz)), DMA((4, nz))]

    def hop0(self, i):
        return remote(self.p.at[i % PS, :, :, :, self.other], self.h0.at[i], self.s0.at[i], self.r0.at[i], self.at.dev(c=1 - self.at.c))

    def bhop(self, i, q, recv=False):
        t = Item(self.at, i)
        o = q if recv else t.b
        return remote(self.a1.at[i % 4, :, :, q], self.hb.at[i, o], self.s_b.at[i, q], self.r_b.at[i, o], t.along_b(q))

    def ahop(self, i, last, q, recv=False):
        t, sl = Item(self.at, i), i % SLOTS
        o = q if recv else t.a
        sems = (self.s_a.at[i, q], self.r_a.at[i, o], t.along_a(q))
        if last:
            return remote(self.a2.at[sl, :, q], self.ha.at[i, o], *sems)
        return remote(self.a3.at[sl, q], self.ha.at[i, o, 0], *sems)

    def zhop(self, i, last, p, recv=False):
        sl = i % SLOTS
        o = p if recv else self.at.z
        sems = (self.s_z.at[i, p], self.r_z.at[i, o], self.at.dev(z=p))
        if last:
            return remote(self.a3.at[sl, p], self.hz.at[i, o, 0], *sems)
        return remote(self.a2.at[sl, p], self.hz.at[i, o], *sems)

    def zrelay(self, i, last):
        sl, e = i % SLOTS, self.line.end
        sems = (self.s_x.at[i], self.r_x.at[i], self.at.dev(z=self.line.relay))
        if last:
            return remote(self.a3.at[sl, e], self.hx.at[i, 0], *sems)
        return remote(self.a2.at[sl, e], self.hx.at[i], *sems)

    def hop4(self, i, recv=False):
        return remote(self.a4.at[i % SLOTS], self.o.at[i, self.other if recv else self.half], self.s4.at[i], self.r4.at[i], self.at.dev(c=1 - self.at.c))

    def keep(self, i):
        return pltpu.make_async_copy(self.a4.at[i % SLOTS], self.o.at[i, self.half], self.os.at[i])

    def copy(self, src, dst, k, q=0):
        return pltpu.make_async_copy(src, dst, self.ls.at[k, q])

    def load_a(self, i, last, q):
        nz = self.at.NZ
        return self.copy(self.ha.at[i, q], self.la.at[q, 0:nz], 2, q) if last else self.copy(self.ha.at[i, q, 0], self.la.at[q, nz], 5, q)

    def load_z(self, i, last, p):
        m = self.at.NX
        return self.copy(self.hz.at[i, p, 0], self.lz.at[p, m], 3, p) if last else self.copy(self.hz.at[i, p], self.lz.at[p, 0:m], 6, p)

    def load_x(self, i, last):
        m = self.at.NX
        return self.copy(self.hx.at[i, 0], self.lx.at[m], 4) if last else self.copy(self.hx.at[i], self.lx.at[0:m], 7)

    def from_z(self, f):
        for p in self.line.others:
            @pl.when(self.line.direct(p))
            def _():
                f(p)

    def z_send(self, i, last):
        for p in self.line.others:
            @pl.when(self.line.direct(p) & ~(self.line.middle & (p == self.line.far)))
            def _():
                self.zhop(i, last, p).start()

        @pl.when(~self.line.middle)
        def _():
            self.zrelay(i, last).start()

    def z_sent(self, i, last):
        for p in self.line.others:
            @pl.when(self.line.direct(p))
            def _():
                self.zhop(i, last, p).wait_send()

        @pl.when(~self.line.middle)
        def _():
            self.zrelay(i, last).wait_send()

    def a_sent(self, i, last):
        for q in Item(self.at, i).others_a():
            self.ahop(i, last, q).wait_send()

    def by_type(self, i, f):
        last = z_first(i)
        for v in (True, False):
            @pl.when(last if v else ~last)
            def _():
                f(v)

    def send(self, i):
        self.hop0(i).start()

    def sends_done(self, k, i):
        if k == 1:
            for q in Item(self.at, i).others_b():
                self.bhop(i, q).wait_send()
        elif k == 2:
            self.by_type(i, lambda last: self.a_sent(i, True) if last else self.z_sent(i, False))
        elif k == 3:
            self.by_type(i, lambda last: self.z_sent(i, True) if last else self.a_sent(i, False))
        else:
            self.hop4(i).wait_send()
            self.keep(i).wait()

    def free(self, k, i):
        n = 4 if k == 1 else SLOTS

        @pl.when(i >= n)
        def _():
            self.sends_done(k, i - n)

    def arrive(self, k, i):
        t = Item(self.at, i)
        if k == 1:
            self.hop0(i).wait_recv()
            self.copy(self.h0.at[i], self.l0, 0).start()
        elif k == 2:
            for q in t.others_b():
                self.bhop(i, q, True).wait_recv()
                self.copy(self.hb.at[i, q], self.lb.at[q], 1, q).start()
        else:
            def f(last):
                step = {3: "a", 4: "x", 5: "z"}[k] if last else {3: "x", 4: "z", 5: "a"}[k]
                if step == "a":
                    for q in t.others_a():
                        self.ahop(i, last, q, True).wait_recv()
                        self.load_a(i, last, q).start()
                elif step == "x":
                    @pl.when(self.line.middle)
                    def _():
                        self.zrelay(i, last).wait_recv()
                        self.load_x(i, last).start()
                else:
                    def g(p):
                        self.zhop(i, last, p, True).wait_recv()
                        self.load_z(i, last, p).start()
                    self.from_z(g)
            self.by_type(i, f)

    def done(self, i, value):
        self.free(5, i)
        self.a4[i % SLOTS] = value * self.scale
        self.keep(i).start()
        self.hop4(i).start()

    def process(self, k, i):
        at, sl, t = self.at, i % SLOTS, Item(self.at, i)
        nz, m = at.NZ, at.NX
        if k == 1:
            self.free(1, i)
            self.copy(self.h0.at[i], self.l0, 0).wait()

            @pl.loop(0, nz)
            def _(z):
                for y in range(m):
                    for x in range(m):
                        self.a1[i % 4, z, y, x] = self.p[i % PS, z, y, x, self.half] + self.l0[z, y, x]
            for q in t.others_b():
                self.bhop(i, q).start()
        elif k == 2:
            self.free(2, i)
            for q in t.others_b():
                self.copy(self.hb.at[i, q], self.lb.at[q], 1, q).wait()

            @pl.loop(0, nz)
            def _(z):
                for a in range(m):
                    own = self.a1[i % 4, z, a, t.b]
                    for q in t.others_b():
                        own = own + self.lb[q, z, a]
                    self.a2[sl, z, a] = own

            def f(last):
                if last:
                    for q in t.others_a():
                        self.ahop(i, True, q).start()
                else:
                    self.z_send(i, False)
            self.by_type(i, f)
        else:
            if k == 3:
                pass

            def f(last):
                step = {3: "a", 4: "x", 5: "z"}[k] if last else {3: "x", 4: "z", 5: "a"}[k]
                if step == "a":
                    for q in t.others_a():
                        self.load_a(i, last, q).wait()
                    if last:
                        self.free(3, i)

                        @pl.loop(0, nz)
                        def _(z):
                            own = self.a2[sl, z, t.a]
                            for q in t.others_a():
                                own = own + self.la[q, z]
                            self.a3[sl, z] = own
                        self.z_send(i, True)
                    else:
                        own = self.a3[sl, t.a]
                        for q in t.others_a():
                            own = own + self.la[q, nz]
                        self.done(i, own)
                elif step == "x":
                    @pl.when(self.line.middle)
                    def _():
                        self.load_x(i, last).wait()
                        far = self.line.far
                        if last:
                            self.a3[sl, far] += self.lx[m]
                        else:
                            for a in range(m):
                                self.a2[sl, far, a] += self.lx[a]
                        self.zhop(i, last, far).start()
                else:
                    self.from_z(lambda p: self.load_z(i, last, p).wait())
                    if not last:
                        self.free(3, i)
                    tmp = []
                    for a in range(1 if last else m):
                        own = self.a3[sl, at.z] if last else self.a2[sl, at.z, a]
                        for p in self.line.others:
                            own = own + jnp.where(self.line.direct(p), self.lz[p, m if last else a], 0.0)
                        tmp.append(own)
                    if last:
                        self.done(i, tmp[0])
                    else:
                        for a in range(m):
                            self.a3[sl, a] = tmp[a]
                        for q in t.others_a():
                            self.ahop(i, False, q).start()
            self.by_type(i, f)

    def step(self, t, f):
        for k in (5, 4, 3, 2, 1):
            i = t - LAG[k]

            @pl.when((i >= 0) & (i < NI))
            def _():
                f(k, i)

    def finish(self):
        for i in range(NI - PS, NI):
            self.hop0(i).wait_send()
        for k, n in ((1, 4), (2, SLOTS), (3, SLOTS), (5, SLOTS)):
            @pl.loop(NI - n, NI)
            def _(i):
                self.sends_done(k, i)

        @pl.loop(0, NI)
        def _(i):
            self.hop4(i, True).wait_recv()

    def vhop(self, k, q, recv=False):
        a = self.at
        if k == 0:
            return remote(self.v0, self.w0, self.vs.at[0, 0], self.vr.at[0, 0], a.dev(c=1 - a.c))
        me, src, dst, dev = {1: (a.y, self.v1.at[:, q], self.w1, a.dev(y=q)), 2: (a.x, self.v2.at[:, q], self.w2, a.dev(x=q)),
                             3: (a.z, self.v3.at[q], self.w3, a.dev(z=q))}[k]
        o = q if recv else me
        return remote(src, dst.at[o], self.vs.at[k, q], self.vr.at[k, o], dev)

    def vlines(self, k):
        return [0] if k == 0 else self.at.others({1: "y", 2: "x", 3: "z"}[k])

    def small(self, k):
        a = self.at
        if k:
            for q in self.vlines(k - 1):
                self.vhop(k - 1, q, True).wait_recv()
        if k == 1:
            self.v1[...] = self.v0[...] + self.w0[...]
        if k == 2:
            own = self.v1[:, a.y]
            for q in self.vlines(1):
                own = own + self.w1[q]
            self.v2[...] = own
        if k == 3:
            own = self.v2[:, a.x]
            for q in self.vlines(2):
                own = own + self.w2[q]
            self.v3[...] = own
        if k == 4:
            own = self.v3[a.z]
            for q in self.vlines(3):
                own = own + self.w3[q]
            self.ov[...] = own * self.scale
        else:
            for q in self.vlines(k):
                self.vhop(k, q).start()

    def small_finish(self):
        for k in range(4):
            for q in self.vlines(k):
                self.vhop(k, q).wait_send()


BF = jnp.bfloat16
NN = ((1,), (0,))
NT = ((1,), (1,))
TN = ((0,), (0,))
ROW_P, ROW_G1, ROW_S1, ROW_U, ROW_D, ROW_G2, ROW_S2 = 3, 4, 5, 6, 10, 11, 12
X_, C_, N_, A_ = 0, 1, 2, 3


def mx(a, b, dims=NN):
    return lax.dot_general(a, b, (dims, ((), ())), preferred_element_type=F32)


def split(v):
    hi = v.astype(BF)
    return hi, (v - hi.astype(F32)).astype(BF)


def split32(v):
    hi = v.astype(BF).astype(F32)
    return hi, v - hi


def three(ah, al, bh, bl, dims=NN):
    return mx(ah, bh, dims) + mx(ah, bl, dims) + mx(al, bh, dims)


def left_half(shape):
    return lax.broadcasted_iota(jnp.int32, shape, 1) < HD


def pack_hl0(v):
    m = left_half(v.shape)
    h, l = split32(v)
    hr, lr = pltpu.roll(h, HD, 1), pltpu.roll(l, HD, 1)
    zero = jnp.zeros_like(v)
    one = jnp.concatenate([jnp.where(m, h, lr), jnp.where(m, h, zero)], axis=1).astype(BF)
    two = jnp.concatenate([jnp.where(m, lr, h), jnp.where(m, zero, h)], axis=1).astype(BF)
    return one, two


def pack_hhl(v):
    m = left_half(v.shape)
    h, l = split32(v)
    hr = pltpu.roll(h, HD, 1)
    one = jnp.concatenate([jnp.where(m, h, hr), l], axis=1).astype(BF)
    two = jnp.concatenate([jnp.where(m, hr, h), l], axis=1).astype(BF)
    return one, two


def pack_hl(v):
    m = left_half(v.shape)
    h, l = split32(v)
    lr = pltpu.roll(l, HD, 1)
    return jnp.where(m, h, lr).astype(BF), jnp.where(m, lr, h).astype(BF)


def fold(one, two):
    m = left_half(one.shape)
    return jnp.where(m, one, two) + pltpu.roll(jnp.where(m, two, one), HD, 1)


def stack_t(v):
    t = v.T
    out = []
    for k in range(2):
        h, l = split32(t[k * HD:(k + 1) * HD])
        out.append(jnp.concatenate([h, l], axis=0).astype(BF))
    return out


def fold_t(one, two):
    return jnp.concatenate([one[:HD] + one[HD:], two[:HD] + two[HD:]], axis=0).T


def cols(start, size):
    return pl.ds(pl.multiple_of(start, 128), size)


def forward_kernel(n, x_ref, w_ref, v_ref, segr, segc, okc,
                   out_ref, g_ref, gv_ref, lh_out, ws_out, qkv_out, p_out, sl_out, hat1_out, hat2_out, inv_out, vec_out,
                   lh, wf, ws, qkv, acc, n1, r2, slope, pst, bias, gvv, vec, ld_sem, ws_sem, out_sem, p_sem, sl_sem, *sems):
    at = Where(n)
    L, D = x_ref.shape
    HB = D // 2
    ga = Gather(at, w_ref, g_ref, v_ref, gv_ref, sems)
    ga.begin_local()
    at.barrier()
    ga.begin()

    def lh_copy(s):
        return pltpu.make_async_copy(lh.at[s], lh_out.at[s], out_sem.at[s])

    RB = 128

    @pl.loop(0, L // RB)
    def _(r):
        rows = pl.ds(pl.multiple_of(r * RB, RB), RB)
        h, l = split(x_ref[rows])
        lh[X_, 0, rows] = h
        lh[X_, 1, rows] = l
        kpos = lax.broadcasted_iota(jnp.int32, (RB, L), 0) + r * RB
        qpos = lax.broadcasted_iota(jnp.int32, (RB, L), 1)
        allowed = (segc[rows] == segr[...]) & ((okc[rows] > 0) | (kpos == qpos))
        bias[rows] = jnp.where(allowed, 0.0, MASKED)
    lh_copy(X_).start()
    @pl.loop(0, 2 + G_LAG[4])
    def _(t):
        ga.step(t)
    cp = pltpu.make_async_copy(gv_ref, gvv, ld_sem.at[0])
    cp.start()
    cp.wait()
    R = 2 * ga.RH
    q = 128 // R
    for k in range(D // 128):
        s = None
        for j in range(q):
            c = k * q + j
            blk = gvv[c // (at.NY * at.NX), (c // at.NX) % at.NY, c % at.NX]
            s = blk if s is None else s + blk
        vec[:, k * 128:(k + 1) * 128] = s
    vcp = pltpu.make_async_copy(vec, vec_out, out_sem.at[7])
    vcp.start()

    def load(w, st):
        return pltpu.make_async_copy(g_ref.at[2 * w + st], wf.at[st], ld_sem.at[st])

    def ws_copy(w, st):
        return pltpu.make_async_copy(ws.at[st], ws_out.at[w, st], ws_sem.at[st])

    def weights(w):
        for st in range(2):
            ga.ready(2 * w + st)
            load(w, st).start()

    def half(w, st, s):
        load(w, st).wait()

        @pl.when(w > 0)
        def _():
            ws_copy(w - 1, st).wait()

        @pl.loop(0, at.NZ)
        def _(z):
            for a in range(at.NY):
                for b in range(at.NX):
                    y, x = (a, b) if st == 0 else (b, a)
                    r0 = pl.multiple_of(((z * at.NY + y) * at.NX + x) * R, R)
                    h, l = split(wf[st, z, a, b])
                    ws[st, 0, pl.ds(r0, R)] = h
                    ws[st, 1, pl.ds(r0, R)] = l
        ws_copy(w, st).start()
        acc[...] = three(lh[s, 0], lh[s, 1], ws[st, 0], ws[st, 1])

    T0 = 2 + G_LAG[4]

    def qkv_copy(w):
        return pltpu.make_async_copy(qkv.at[w], qkv_out.at[w], out_sem.at[8 + w])

    @pl.loop(0, 3)
    def _(w):
        weights(w)
        f = jnp.where(w == 0, 1.0 / math.sqrt(HD), 1.0).astype(F32)
        for st in range(2):
            half(w, st, X_)
            b = vec[pl.ds(w, 1), st * HB:(st + 1) * HB]
            qkv[w, :, st * HB:(st + 1) * HB] = (acc[...] + b) * f
            ga.step(T0 + 2 * w + st)
        qkv_copy(w).start()

    def p_copy(p):
        return pltpu.make_async_copy(pst.at[p % 2], p_out.at[p], p_sem.at[p % 2])

    def attend(p):
        c = cols(p * 128, 128)
        qp, kp, vp = qkv[0, :, c], qkv[1, :, c], qkv[2, :, c]
        qs, ks, vt = pack_hhl(qp), pack_hl0(kp), stack_t(vp)

        @pl.when(p >= 2)
        def _():
            p_copy(p - 2).wait()
        res = []
        for k in range(2):
            s = mx(ks[k], qs[k], NT) + bias[...]
            e = jnp.exp(s - jnp.max(s, axis=0, keepdims=True))
            e = e * (1.0 / jnp.sum(e, axis=0, keepdims=True))
            ph, pll = split(e)
            pst[p % 2, k, 0] = ph
            pst[p % 2, k, 1] = pll
            res.append(mx(vt[k], ph) + mx(vt[k], pll))
        p_copy(p).start()
        h, l = split(fold_t(*res))
        lh[C_, 0, :, c] = h
        lh[C_, 1, :, c] = l

    @pl.loop(0, H // 2)
    def _(p):
        attend(p)

        @pl.when(p % 4 != 3)
        def _():
            ga.step(T0 + 6 + p - p // 4)
    lh_copy(C_).start()

    weights(3)
    for st in range(2):
        half(3, st, C_)
        c = slice(st * HB, (st + 1) * HB)
        n1[:, c] = x_ref[:, c] + acc[...] + vec[ROW_P:ROW_P + 1, c]
    @pl.loop(T0 + 12, T0 + 13)
    def _(t):
        ga.step(t)

    def norm_rows(ref, k, hat_ref, rows):
        v = ref[rows]
        center = v - jnp.mean(v, axis=-1, keepdims=True)
        inverse = lax.rsqrt(jnp.mean(center * center, axis=-1, keepdims=True) + EPSILON)
        hat = center * inverse
        return hat, inverse

    @pl.loop(0, L // RB)
    def _(r):
        rows = pl.ds(pl.multiple_of(r * RB, RB), RB)
        hat, inverse = norm_rows(n1, 0, None, rows)
        r2[rows] = hat
        inv_out[rows, 0:128] = jnp.broadcast_to(inverse, (RB, 128))
        v = hat * vec[ROW_G1:ROW_G1 + 1] + vec[ROW_S1:ROW_S1 + 1]
        n1[rows] = v
        h, l = split(v)
        lh[N_, 0, rows] = h
        lh[N_, 1, rows] = l
    lh_copy(N_).start()
    hcp = pltpu.make_async_copy(r2, hat1_out, out_sem.at[11])
    hcp.start()

    def sl_copy(j, st):
        return pltpu.make_async_copy(slope.at[st], sl_out.at[j, st], sl_sem.at[st])

    @pl.loop(0, 4)
    def _(j):
        weights(4 + j)
        for st in range(2):
            half(4 + j, st, N_)
            c = slice(st * HB, (st + 1) * HB)

            @pl.when(j > 0)
            def _():
                sl_copy(j - 1, st).wait()
            b = vec[pl.ds(ROW_U + j, 1), c]

            @pl.loop(0, L // 64)
            def _(r):
                rows = pl.ds(pl.multiple_of(r * 64, 64), 64)
                u = acc[rows] + b
                phi = 0.5 * (1.0 + lax.erf(u * math.sqrt(0.5)))
                h, l = split(u * phi)
                lh[A_ + j, 0, rows, c] = h
                lh[A_ + j, 1, rows, c] = l
                slope[st, rows] = phi + u * jnp.exp(-0.5 * u * u) * (1.0 / math.sqrt(2.0 * math.pi))
            sl_copy(j, st).start()
            if st == 0:
                ga.step(T0 + 13 + j)
        lh_copy(A_ + j).start()

    hcp.wait()
    r2[...] = n1[...] + vec[ROW_D:ROW_D + 1]

    @pl.loop(0, 4)
    def _(j):
        weights(8 + j)
        for st in range(2):
            half(8 + j, st, A_ + j)
            r2[:, st * HB:(st + 1) * HB] += acc[...]

            @pl.when((j < 3) if st == 0 else (j == 1) | (j == 2))
            def _():
                ga.step(T0 + 17 + j + (j == 2).astype(jnp.int32) if st == 0 else T0 + 17 + 2 * j)

    @pl.loop(0, L // RB)
    def _(r):
        rows = pl.ds(pl.multiple_of(r * RB, RB), RB)
        hat, inverse = norm_rows(r2, 1, None, rows)
        r2[rows] = hat
        inv_out[rows, 128:256] = jnp.broadcast_to(inverse, (RB, 128))
        out_ref[rows] = hat * vec[ROW_G2:ROW_G2 + 1] + vec[ROW_S2:ROW_S2 + 1]
    hcp2 = pltpu.make_async_copy(r2, hat2_out, out_sem.at[11])
    hcp2.start()
    vcp.wait()
    for s in range(7):
        lh_copy(s).wait()
    for w in range(3):
        qkv_copy(w).wait()
    for p in (H // 2 - 2, H // 2 - 1):
        p_copy(p).wait()
    for st in range(2):
        sl_copy(3, st).wait()
        ws_copy(NW - 1, st).wait()
    hcp2.wait()
    ga.finish()


def forward(n, x, w, v, segr, segc, okc):
    nz, ny, nx = torus(n)
    _, R, HB = w.shape
    L, D = x.shape
    S = lambda shape, t=F32: jax.ShapeDtypeStruct(shape, t)
    V = pltpu.VMEM
    ANY = pl.BlockSpec(memory_space=pl.ANY)
    VM = pl.BlockSpec(memory_space=pltpu.VMEM)
    return pl.pallas_call(
        functools.partial(forward_kernel, n),
        out_shape=[S((L, D)), S((NI, nz, ny, nx, R, HB)), S((nz, ny, nx) + v.shape), S((7, 2, L, D), BF),
                   S((NW, 2, 2, D, HB), BF), S((3, L, D)), S((H // 2, 2, 2, L, L), BF), S((4, 2, L, HB)),
                   S((L, D)), S((L, D)), S((L, 256)), S((v.shape[0], D))],
        in_specs=[VM] * 6,
        out_specs=[VM] + [ANY] * 9 + [VM, ANY],
        scratch_shapes=[V((7, 2, L, D), BF), V((2, nz, ny, nx, R, HB), F32), V((2, 2, D, HB), BF), V((3, L, D), F32),
                        V((L, HB), F32), V((L, D), F32), V((L, D), F32), V((2, L, HB), F32), V((2, 2, 2, L, L), BF),
                        V((L, L), F32), V((nz, ny, nx) + v.shape, F32), V((v.shape[0], D), F32),
                        DMA((2,)), DMA((2,)), DMA((12,)), DMA((2,)), DMA((2,))] + Gather.sems(n),
        compiler_params=pltpu.CompilerParams(collective_id=0, has_side_effects=True, vmem_limit_bytes=63 * 2**20),
        name="forward",
    )(x, w, v, segr, segc, okc)


E_U, E_P, E_Q = 8, 16, 18
E_PAIR = 9
R_R2, R_U, R_R1, R_Q = 0, 1, 5, 6


def backward_kernel(n, scale, ct_ref, hat2_ref, hat1_ref, inv_ref, lh_ref, ws_ref, qkv_ref, p_ref, sl_ref, vec,
                    dx_ref, o_ref, ov_ref, rhs_ref, h0, h1, h2, h3, h4,
                    lbuf, rbuf, wbuf, sbuf, pbuf, qbuf, dr2, du, dn1, fb, dst, small,
                    l_sem, r_sem, w_sem, s_sem, p_sem, q_sem, f_sem, o_sem, d_sem, *rest):
    at = Where(n)
    bufs, sems = rest[:18], rest[18:]
    rd = Reduce(at, o_ref, ov_ref, (h0, h1, h2, h3, h4), bufs, sems, scale)
    L, D = ct_ref.shape
    HB = D // 2
    RB = 128
    FB = D // at.NZ
    R = 2 * rd.RH
    copy = pltpu.make_async_copy

    def f_load(src, k):
        return copy(src, fb.at[k], f_sem.at[k])

    def lhs_slot(e):
        return jnp.where(e < E_U, A_ + e // 2, jnp.where(e < E_P, N_, jnp.where(e < E_Q, C_, X_)))

    def rhs_slot(e):
        return jnp.where(e < E_U, R_R2, jnp.where(e < E_P, R_U + (e - E_U) // 2, jnp.where(e < E_Q, R_R1, R_Q + (e - E_Q) % 3)))

    def rhs_half(e):
        return jnp.where(e < E_Q, e % 2, (e - E_Q) // 3)

    def l_load(e):
        return copy(lh_ref.at[lhs_slot(e)], lbuf.at[e % 2], l_sem.at[e % 2])

    def r_load(e):
        return copy(rhs_ref.at[rhs_slot(e), :, :, cols(rhs_half(e) * HB, HB)], rbuf.at[e % 2], r_sem.at[e % 2])

    def w_load(e, k):
        pairs = jnp.where(e < E_U, jnp.where(e % 2 == 0, 8, 4) + e // 2, 3)
        w = jnp.where(e < E_Q, pairs, (e - E_Q) % 3)
        h = jnp.where(e < E_Q, k, (e - E_Q) // 3)
        return copy(ws_ref.at[w, h], wbuf.at[e % 2, k], w_sem.at[e % 2, k])

    def s_load(j):
        return copy(sl_ref.at[j], sbuf, s_sem)

    def p_load(p):
        return copy(p_ref.at[p], pbuf.at[p % 2], p_sem.at[p % 2])

    def q_load(p):
        return copy(qkv_ref.at[:, :, cols(p * 128, 128)], qbuf.at[p % 2], q_sem.at[p % 2])

    def rhs_store(src, slot, k):
        return copy(src, rhs_ref.at[slot], o_sem.at[k])

    f_load(ct_ref, 0).start()
    f_load(hat2_ref, 1).start()
    l_load(0).start()
    for k in range(2):
        w_load(0, k).start()
    s_load(0).start()
    at.barrier()
    small[...] = jnp.zeros_like(small)
    f_load(ct_ref, 0).wait()
    f_load(hat2_ref, 1).wait()

    def norm_back(r, g, hat, inverse, gain, row_shift, row_gain):
        gg = g * gain
        small[row_shift:row_shift + 1] += jnp.sum(g, axis=0, keepdims=True)
        small[row_gain:row_gain + 1] += jnp.sum(g * hat, axis=0, keepdims=True)
        return inverse * (gg - jnp.mean(gg, -1, keepdims=True) - hat * jnp.mean(gg * hat, -1, keepdims=True))

    @pl.loop(0, L // RB)
    def _(r):
        rows = pl.ds(pl.multiple_of(r * RB, RB), RB)
        d = norm_back(r, fb[0, rows], fb[1, rows], inv_ref[rows, 128:129], vec[ROW_G2:ROW_G2 + 1], ROW_S2, ROW_G2)
        small[ROW_D:ROW_D + 1] += jnp.sum(d, axis=0, keepdims=True)
        dn1[rows] = d
        h, l = split(d)
        dr2[0, rows] = h
        dr2[1, rows] = l
    rhs_store(dr2, R_R2, 0).start()
    f_load(hat1_ref, 0).start()
    rhs_store(dr2, R_R2, 0).wait()
    r_load(0).start()

    def chunk_da(j, e):
        for k in range(2):
            w_load(e, k).wait()
        s_load(j).wait()

        @pl.when(j > 0)
        def _():
            rhs_store(du, R_U + j - 1, 1).wait()
        for k in range(4):
            b = slice(k * FB, (k + 1) * FB)
            v = three(dr2[0, :, :HB], dr2[1, :, :HB], wbuf[e % 2, 0, 0, b], wbuf[e % 2, 0, 1, b], NT) \
                + three(dr2[0, :, HB:], dr2[1, :, HB:], wbuf[e % 2, 1, 0, b], wbuf[e % 2, 1, 1, b], NT)
            half, off = (k * FB) // HB, (k * FB) % HB
            v = v * sbuf[half, :, off:off + FB]
            small[pl.ds(ROW_U + j, 1), b] = jnp.sum(v, axis=0, keepdims=True)
            h, l = split(v)
            du[0, :, b] = h
            du[1, :, b] = l
        rhs_store(du, R_U + j, 1).start()

        @pl.when(j < 3)
        def _():
            s_load(j + 1).start()

    def nt_into(ref, a, e, b):
        return ref[:, b] + three(a[0, :, :HB], a[1, :, :HB], wbuf[e % 2, 0, 0, b], wbuf[e % 2, 0, 1, b], NT) \
            + three(a[0, :, HB:], a[1, :, HB:], wbuf[e % 2, 1, 0, b], wbuf[e % 2, 1, 1, b], NT)

    def chunk_dn(e):
        for k in range(2):
            w_load(e, k).wait()
        for k in range(4):
            b = slice(k * FB, (k + 1) * FB)
            dn1[:, b] = nt_into(dn1, du, e, b)

    def chunk_norm():
        f_load(hat1_ref, 0).wait()

        @pl.loop(0, L // RB)
        def _(r):
            rows = pl.ds(pl.multiple_of(r * RB, RB), RB)
            d = norm_back(r, dn1[rows], fb[0, rows], inv_ref[rows, 0:1], vec[ROW_G1:ROW_G1 + 1], ROW_S1, ROW_G1)
            small[ROW_P:ROW_P + 1] += jnp.sum(d, axis=0, keepdims=True)
            dn1[rows] = d
            h, l = split(d)
            dr2[0, rows] = h
            dr2[1, rows] = l
        rhs_store(du, R_U + 3, 1).wait()
        rhs_store(dr2, R_R1, 0).start()

    def chunk_dc(e):
        for k in range(2):
            w_load(e, k).wait()
        for k in range(4):
            b = slice(k * FB, (k + 1) * FB)
            fb[1, :, b] = three(dr2[0, :, :HB], dr2[1, :, :HB], wbuf[e % 2, 0, 0, b], wbuf[e % 2, 0, 1, b], NT) \
                + three(dr2[0, :, HB:], dr2[1, :, HB:], wbuf[e % 2, 1, 0, b], wbuf[e % 2, 1, 1, b], NT)
        rhs_store(dr2, R_R1, 0).wait()

    def d_store(p, k):
        return copy(dst.at[p % 2, k], rhs_ref.at[R_Q + k, :, :, cols(p * 128, 128)], d_sem.at[p % 2, k])

    def chunk_pair(p):
        c = cols(p * 128, 128)
        s = p % 2
        p_load(p).wait()
        q_load(p).wait()

        @pl.when(p < H // 2 - 1)
        def _():
            p_load(p + 1).start()
            q_load(p + 1).start()
        qp, kp, vp, dc = qbuf[s, 0], qbuf[s, 1], qbuf[s, 2], fb[1, :, c]
        va, da, kt, qx, dx = pack_hl0(vp), pack_hhl(dc), stack_t(kp), pack_hl(qp), pack_hl(dc)
        dq, dk, dv = [], [], []
        for k in range(2):
            dp = mx(va[k], da[k], NT)
            ph, pll = pbuf[s, k, 0], pbuf[s, k, 1]
            pf = ph.astype(F32) + pll.astype(F32)
            t = pf * dp
            t = t - pf * jnp.sum(t, axis=0, keepdims=True)
            sh, sll = split(t)
            dk.append(mx(sh, qx[k]) + mx(sll, qx[k]))
            dv.append(mx(ph, dx[k]) + mx(pll, dx[k]))
            dq.append(mx(kt[k], sh) + mx(kt[k], sll))
        out = (fold_t(*dq) * (1.0 / math.sqrt(HD)), fold(*dk), fold(*dv))

        @pl.when(p >= 2)
        def _():
            for k in range(3):
                d_store(p - 2, k).wait()
        for k in range(3):
            small[k:k + 1, c] = jnp.sum(out[k], axis=0, keepdims=True)
            h, l = split(out[k])
            dst[s, k, 0] = h
            dst[s, k, 1] = l
            d_store(p, k).start()

    def chunk_dx(e):
        w_load(e, 0).wait()
        for k in range(4):
            b = slice(k * FB, (k + 1) * FB)
            dn1[:, b] += three(rbuf[e % 2, 0], rbuf[e % 2, 1], wbuf[e % 2, 0, 0, b], wbuf[e % 2, 0, 1, b], NT)

    @pl.loop(0, NI + LAG[5])
    def _(e):
        @pl.when(e < NI)
        def _():
            l_load(e).wait()
            r_load(e).wait()

            @pl.when(e >= PS)
            def _():
                rd.hop0(e - PS).wait_send()

            @pl.loop(0, at.NZ)
            def _(z):
                b = cols(z * FB, FB)
                v = three(lbuf[e % 2, 0, :, b], lbuf[e % 2, 1, :, b], rbuf[e % 2, 0], rbuf[e % 2, 1], TN)
                odd = e % 2 == 1
                for y in range(at.NY):
                    for x in range(at.NX):
                        k = (y * at.NX + x) * R
                        rd.p[e % PS, z, jnp.where(odd, x, y), jnp.where(odd, y, x)] = v[k:k + R]
            rd.send(e)

            @pl.when(e < NI - 1)
            def _():
                l_load(e + 1).start()
                r_load(e + 1).start()

            @pl.when((e < E_U) | ((e >= E_Q - 1) & (e < NI - 1)))
            def _():
                w_load(e + 1, 0).start()

            @pl.when(e < E_U)
            def _():
                w_load(e + 1, 1).start()
        rd.step(e, rd.arrive)

        @pl.when((e < E_U) & (e % 2 == 0))
        def _():
            chunk_da(e // 2, e)

        @pl.when((e < E_U) & (e % 2 == 1))
        def _():
            chunk_dn(e)

        @pl.when(e == E_U - 1)
        def _():
            chunk_norm()

        @pl.when(e == E_U)
        def _():
            p_load(0).start()
            q_load(0).start()
            chunk_dc(e)

        @pl.when((e >= E_PAIR) & (e < E_PAIR + H // 2))
        def _():
            chunk_pair(e - E_PAIR)

        @pl.when(e == E_PAIR + H // 2)
        def _():
            for p in (H // 2 - 2, H // 2 - 1):
                for k in range(3):
                    d_store(p, k).wait()
            for z in range(at.NZ):
                for y in range(at.NY):
                    for x in range(at.NX):
                        g = ((z * at.NY + y) * at.NX + x) * 2 * rd.RH // 128
                        rd.v0[z, y, x] = small[:, g * 128:(g + 1) * 128]

        for k in range(5):
            @pl.when(e == E_PAIR + H // 2 + k)
            def _():
                rd.small(k)

        @pl.when((e >= E_Q) & (e < NI))
        def _():
            chunk_dx(e)

        @pl.when(e == NI - 1)
        def _():
            copy(dn1, dx_ref, o_sem.at[0]).start()
        rd.step(e, rd.process)
    copy(dn1, dx_ref, o_sem.at[0]).wait()
    rd.finish()
    rd.small_finish()


def backward(n, R, scale, ct, hat2, hat1, inv, lh, ws, qkv, p, sl, vec):
    L, D = ct.shape
    HB = D // 2
    VR = vec.shape[0]
    S = lambda shape, t=F32: jax.ShapeDtypeStruct(shape, t)
    V = pltpu.VMEM
    ANY = pl.BlockSpec(memory_space=pl.ANY)
    VM = pl.BlockSpec(memory_space=pltpu.VMEM)
    return pl.pallas_call(
        functools.partial(backward_kernel, n, scale),
        out_shape=[S((L, D)), S((NI, R, HB)), S((VR, 128)), S((9, 2, L, D), BF)] + Reduce.recv_shapes(n, R, HB),
        in_specs=[ANY, ANY, ANY, VM, ANY, ANY, ANY, ANY, ANY, VM],
        out_specs=[ANY, ANY, VM] + [ANY] * 6,
        scratch_shapes=[V((2, 2, L, D), BF), V((2, 2, L, HB), BF), V((2, 2, 2, D, HB), BF), V((2, L, HB), F32),
                        V((2, 2, 2, L, L), BF), V((2, 3, L, 128), F32), V((2, L, D), BF), V((2, L, D), BF), V((L, D), F32),
                        V((2, L, D), F32), V((2, 3, 2, L, 128), BF), V((VR, D), F32),
                        DMA((2,)), DMA((2,)), DMA((2, 2)), DMA(()), DMA((2,)), DMA((2,)), DMA((2,)), DMA((2,)), DMA((2, 3))]
        + Reduce.bufs(n, R, HB, VR) + Reduce.sems(n),
        compiler_params=pltpu.CompilerParams(collective_id=1, has_side_effects=True, vmem_limit_bytes=63 * 2**20),
        name="backward",
    )(ct, hat2, hat1, inv, lh, ws, qkv, p, sl, vec)[:3]


def pack_weights(n, qkv, proj, up, down):
    R, D = proj.shape
    J = up.shape[1] // D
    q3 = qkv.reshape(R, 3, D).transpose(1, 0, 2)
    u4 = up.reshape(R, n, J, R).transpose(2, 0, 1, 3).reshape(J, R, D)
    d4 = down.reshape(J, R, D)
    w = jnp.concatenate([q3, proj[None], u4, d4], axis=0)
    return w.reshape(NW, R, 2, D // 2).transpose(0, 2, 1, 3).reshape(NI, R, D // 2)


def unpack_grads(n, o):
    _, R, HB = o.shape
    D, J = 2 * HB, 4
    down = o[:E_U].reshape(J, 2, R, HB).transpose(0, 2, 1, 3).reshape(J * R, D)
    up = o[E_U:E_P].reshape(J, 2, R, n // 2, R).transpose(2, 1, 3, 0, 4).reshape(R, n * J * R)
    proj = o[E_P:E_Q].transpose(1, 0, 2).reshape(R, D)
    qkv = o[E_Q:].reshape(2, 3, R, HB).transpose(2, 1, 0, 3).reshape(R, 3 * D)
    return qkv, proj, up, down


VROWS = 16


def lane(R):
    return (lax.axis_index("shard") * R) % 128


def pack_small(before, up_bias, after):
    R = before[0].shape[0]
    rows = jnp.concatenate([jnp.stack(before), up_bias.reshape(4, R), jnp.stack(after)])
    wide = jnp.zeros((VROWS, 128), F32)
    return lax.dynamic_update_slice(wide, jnp.pad(rows, ((0, VROWS - rows.shape[0]), (0, 0))), (0, lane(R)))


def shards(n, tokens, segment_ids, valid_lengths, qkv_weight, query_bias, value_bias, proj_weight, proj_bias, first_gain,
           first_shift, up_weight, up_bias, down_weight, down_bias, second_gain, second_shift, cotangent):
    amount, length, D = tokens.shape
    R = proj_weight.shape[0]
    x = tokens.reshape(amount * length, D)
    seg = segment_ids.reshape(1, length)
    ok = (jnp.arange(length, dtype=jnp.int32) < valid_lengths[0]).astype(jnp.int32)
    wsh = pack_weights(n, qkv_weight, proj_weight, up_weight, down_weight)
    vsh = pack_small([query_bias, jnp.zeros_like(query_bias), value_bias, proj_bias, first_gain, first_shift], up_bias,
                     [down_bias, second_gain, second_shift])
    out, g, gv, lh, ws, qkv, pr, sl, hat1, hat2, inv, v = forward(n, x, wsh, vsh, seg, seg.reshape(length, 1), ok.reshape(length, 1))
    scale = 1.0 / math.sqrt(amount * length * n * lax.axis_size("rep"))
    dx, o, ov = backward(n, R, scale, cotangent.reshape(amount * length, D), hat2, hat1, inv, lh, ws, qkv, pr, sl, v)
    gqkv, gproj, gup, gdown = unpack_grads(n, o)
    s = lax.dynamic_slice(ov, (0, lane(R)), (VROWS, R))
    return (out.reshape(amount, length, D), dx.reshape(amount, length, D), gqkv, s[0], s[2], gproj, s[3], s[4], s[5], gup,
            s[6:10].reshape(4 * R), gdown, s[10], s[11], s[12])


def solution(mesh):
    n = mesh.shape["shard"]
    one, two, seq = P("shard"), P("shard", None), P(("shard", "rep"), None, None)
    return jax.shard_map(
        functools.partial(shards, n),
        mesh=mesh,
        in_specs=(seq, P(("shard", "rep"), None), P(("shard", "rep")), two, one, one, two, one, one, one, two, one, two, one, one, one, seq),
        out_specs=(seq, seq, two, one, one, two, one, one, one, two, one, two, one, one, one),
        check_vma=False,
    )
```

```python
import functools
import math

import jax
import jax.numpy as jnp
from jax import lax
from jax.experimental import pallas as pl
from jax.experimental.pallas import tpu as pltpu
from jax.sharding import PartitionSpec as P

H = 16
HD = 64
HIGH = lax.Precision.HIGH
EPSILON = 1e-05
MASKED = -1000000000.0
MESH = pl.DeviceIdType.MESH
DMA = pltpu.SemaphoreType.DMA
F32 = jnp.float32
VMEM_LIMIT = 60 * 2**20
NW = 12


def torus(n):
    side = math.isqrt(n // 4)
    assert side * side * 4 == n
    return 4, side, side


def ds(start, size, align=8):
    return pl.ds(pl.multiple_of(start, align), size)


class Where:
    def __init__(self, n):
        self.NZ, self.NY, self.NX = torus(n)
        s = lax.axis_index("shard")
        self.s = s
        self.c = lax.axis_index("rep")
        self.z = s // (self.NY * self.NX)
        self.y = (s // self.NX) % self.NY
        self.x = s % self.NX

    def dev(self, z=None, y=None, x=None, c=None):
        z = self.z if z is None else z
        y = self.y if y is None else y
        x = self.x if x is None else x
        c = self.c if c is None else c
        return (z * (self.NY * self.NX) + y * self.NX + x, c)

    def partners(self):
        out = [self.dev(c=1 - self.c)]
        out += [self.dev(z=p) for p in self.others("z")]
        out += [self.dev(y=p) for p in self.others("y")]
        out += [self.dev(x=p) for p in self.others("x")]
        return out

    def others(self, axis):
        me, n = self.line(axis)
        return [(me + d) % n for d in range(1, n)]

    def line(self, axis):
        return {"z": (self.z, self.NZ), "y": (self.y, self.NY), "x": (self.x, self.NX)}[axis]

    def barrier(self):
        sem = pltpu.get_barrier_semaphore()
        ps = self.partners()
        for p in ps:
            pl.semaphore_signal(sem, inc=1, device_id=p, device_id_type=MESH)
        pl.semaphore_wait(sem, len(ps))


def remote(src, dst, ssem, rsem, dev):
    return pltpu.make_async_remote_copy(
        src_ref=src, dst_ref=dst, send_sem=ssem, recv_sem=rsem, device_id=dev, device_id_type=MESH
    )


NI = 2 * NW


def z_first(i):
    w = i // 2
    return (w % 2 == 0) & (w < NW - 2)


def z_last(i):
    w = i // 2
    return w % 2 == 1


class Item:
    def __init__(self, at, i):
        swap = i % 2 == 1
        self.i, self.at, self.n = i, at, at.NX
        self.a = jnp.where(swap, at.x, at.y)
        self.b = jnp.where(swap, at.y, at.x)
        self.swap = swap

    def chip(self, z, a, b):
        return (z * self.n + jnp.where(self.swap, b, a)) * self.n + jnp.where(self.swap, a, b)

    def along_a(self, q):
        return (self.chip(self.at.z, q, self.b), self.at.c)

    def along_b(self, q):
        return (self.chip(self.at.z, self.a, q), self.at.c)

    def others_a(self):
        return [(self.a + d) % self.n for d in range(1, self.n)]

    def others_b(self):
        return [(self.b + d) % self.n for d in range(1, self.n)]


class Line:
    def __init__(self, at):
        assert at.NZ == 4
        self.z = at.z
        self.others = at.others("z")
        self.middle = (at.z == 1) | (at.z == 2)
        self.far = jnp.where(at.z == 2, 0, 3)
        self.near = jnp.where(at.z == 2, 3, 0)
        self.end = jnp.where(at.z == 0, 3, 0)
        self.relay = jnp.where(at.z == 0, 1, 2)

    def direct(self, p):
        return jnp.abs(p - self.z) != 3


G_LAG = {1: 0, 2: 1, 3: 3, 4: 6}
G_AHEAD = 3


class Gather:
    def __init__(self, at, w_ref, g_ref, v_ref, gv_ref, sems):
        self.at, self.w, self.g, self.v, self.gv = at, w_ref, g_ref, v_ref, gv_ref
        (self.l, self.zs, self.zr, self.zx, self.s_a, self.r_a, self.s_b, self.r_b, self.ss, self.rs, self.vs, self.vr) = sems
        R = w_ref.shape[1]
        self.RH = R // 2
        self.half = ds(at.c * self.RH, self.RH)
        self.other = ds((1 - at.c) * self.RH, self.RH)
        self.line = Line(at)

    @staticmethod
    def sems(n):
        nz, ny, nx = torus(n)
        return [DMA((NI + 1,)), DMA((NI, nz)), DMA((NI, nz)), DMA((NI,)), DMA((NI, nx)), DMA((NI, nx)),
                DMA((NI, nx)), DMA((NI, nx)), DMA((NI,)), DMA((NI,)), DMA((3, nz)), DMA((3, nz))]

    def local(self, i):
        t = Item(self.at, i)
        return pltpu.make_async_copy(self.w.at[i, self.half], self.g.at[i, self.at.z, t.a, t.b, self.half], self.l.at[i])

    def local_v(self):
        a = self.at
        return pltpu.make_async_copy(self.v, self.gv.at[a.z, a.y, a.x], self.l.at[NI])

    def own(self, i, z):
        pass

    def zhop(self, i, first, p, recv=False):
        t, z = Item(self.at, i), self.at.z
        o = p if recv else z
        sems = (self.zs.at[i, p], self.zr.at[i, o], self.at.dev(z=p))
        if first:
            return remote(self.w.at[i, self.half], self.g.at[i, o, t.a, t.b, self.half], *sems)
        return remote(self.g.at[i, o, :, t.b, self.half], self.g.at[i, o, :, t.b, self.half], *sems)

    def zrelay(self, i, first):
        t, o, p = Item(self.at, i), self.line.far, self.line.near
        ref = self.g.at[i, o, t.a, t.b, self.half] if first else self.g.at[i, o, :, t.b, self.half]
        return remote(ref, ref, self.zx.at[i], self.zr.at[i, o], self.at.dev(z=p))

    def ahop(self, i, first, q, recv=False):
        t, z = Item(self.at, i), self.at.z
        o = q if recv else t.a
        sems = (self.s_a.at[i, q], self.r_a.at[i, o], t.along_a(q))
        if first:
            return remote(self.g.at[i, :, o, t.b, self.half], self.g.at[i, :, o, t.b, self.half], *sems)
        return remote(self.w.at[i, self.half], self.g.at[i, z, o, t.b, self.half], *sems)

    def bhop(self, i, q, recv=False):
        t = Item(self.at, i)
        o = q if recv else t.b
        ref = self.g.at[i, :, :, o, self.half]
        return remote(ref, ref, self.s_b.at[i, q], self.r_b.at[i, o], t.along_b(q))

    def pair(self, i, recv=False):
        ref = self.g.at[i, :, :, :, self.other if recv else self.half]
        return remote(ref, ref, self.ss.at[i], self.rs.at[i], self.at.dev(c=1 - self.at.c))

    def small(self, hop, p, recv=False):
        a, g = self.at, self.gv
        if hop == 0:
            o = p if recv else a.z
            return remote(self.v, g.at[o, a.y, a.x], self.vs.at[0, p], self.vr.at[0, o], a.dev(z=p))
        if hop == 1:
            o = p if recv else a.x
            return remote(g.at[:, a.y, a.x], g.at[:, a.y, o], self.vs.at[1, p], self.vr.at[1, o], a.dev(x=p))
        o = p if recv else a.y
        return remote(g.at[:, a.y], g.at[:, o], self.vs.at[2, p], self.vr.at[2, o], a.dev(y=p))

    def z_send(self, i, first):
        for p in self.line.others:
            @pl.when(self.line.direct(p))
            def _():
                self.zhop(i, first, p).start()

    def z_pass(self, i, first):
        @pl.when(self.line.middle)
        def _():
            self.zhop(i, first, self.line.far, True).wait_recv()
            self.zrelay(i, first).start()

    def z_wait(self, i, first):
        for p in self.line.others:
            @pl.when(~(self.line.middle & (p == self.line.far)))
            def _():
                self.zhop(i, first, p, True).wait_recv()

    def a_send(self, i, first):
        for q in Item(self.at, i).others_a():
            self.ahop(i, first, q).start()

    def a_wait(self, i, first):
        for q in Item(self.at, i).others_a():
            self.ahop(i, first, q, True).wait_recv()

    def begin_local(self):
        self.local_v().start()

        @pl.loop(0, NI)
        def _(i):
            self.local(i).start()

    def begin(self):
        for p in self.at.others("z"):
            self.small(0, p).start()

        @pl.loop(0, NI)
        def _(i):
            @pl.when((i < G_AHEAD) | ~z_first(i))
            def _():
                self.stage(0, i)

    def small_step(self, hop):
        a = self.at
        here, nxt = (("z", "x"), ("x", "y"), ("y", None))[hop]
        if hop == 0:
            self.local_v().wait()
        for p in a.others(here):
            self.small(hop, p, True).wait_recv()
        if nxt:
            for p in a.others(nxt):
                self.small(hop + 1, p).start()

    def stage(self, k, i):
        if k == 4:
            for q in Item(self.at, i).others_b():
                self.bhop(i, q, True).wait_recv()
            self.pair(i).start()
            return
        first = z_first(i)

        @pl.when(first)
        def _():
            if k == 0:
                self.z_send(i, True)
            elif k == 1:
                self.z_pass(i, True)
            elif k == 2:
                self.z_wait(i, True)
                self.local(i).wait()
                self.a_send(i, True)
            else:
                self.a_wait(i, True)

        @pl.when(~first)
        def _():
            if k == 0:
                self.a_send(i, False)
            elif k == 1:
                self.a_wait(i, False)
                self.local(i).wait()
                self.z_send(i, False)
            elif k == 2:
                self.z_pass(i, False)
            else:
                self.z_wait(i, False)
        if k == 3:
            for q in Item(self.at, i).others_b():
                self.bhop(i, q).start()

    def ready(self, i):
        self.pair(i, True).wait_recv()

    def step(self, t):
        @pl.when((t + G_AHEAD < NI) & z_first(t + G_AHEAD))
        def _():
            self.z_send(t + G_AHEAD, True)
        for k in (1, 2, 3, 4):
            @pl.when((t >= G_LAG[k]) & (t < NI + G_LAG[k]))
            def _():
                self.stage(k, t - G_LAG[k])
        for hop in range(3):
            @pl.when(t == hop + 1)
            def _():
                self.small_step(hop)

    def finish(self):
        a = self.at
        for hop, here in ((0, "z"), (1, "x"), (2, "y")):
            for p in a.others(here):
                self.small(hop, p).wait_send()

        @pl.loop(0, NI)
        def _(i):
            self.pair(i).wait_send()
            t = Item(a, i)
            for q in t.others_b():
                self.bhop(i, q).wait_send()
            first = z_first(i)
            for f in (True, False):
                @pl.when(first if f else ~first)
                def _():
                    for q in t.others_a():
                        self.ahop(i, f, q).wait_send()
                    for p in self.line.others:
                        @pl.when(self.line.direct(p))
                        def _():
                            self.zhop(i, f, p).wait_send()

                    @pl.when(self.line.middle)
                    def _():
                        self.zrelay(i, f).wait_send()


E_U, E_P, E_Q = 8, 16, 18
SLOTS = 8
PS = 3
LAG = {1: 1, 2: 4, 3: 7, 4: 10, 5: 12}


class Reduce:
    def __init__(self, at, o_ref, ov_ref, r_refs, bufs, sems, scale):
        self.at, self.out, self.ov, self.scale = at, o_ref, ov_ref, scale
        self.h0, self.hb, self.ha, self.hz, self.hx = r_refs
        (self.p, self.a1, self.a2, self.a3, self.a4, self.l0, self.lb, self.la, self.lz, self.lx,
         self.v0, self.v1, self.v2, self.v3, self.w0, self.w1, self.w2, self.w3) = bufs
        (self.s0, self.r0, self.s_b, self.r_b, self.s_a, self.r_a, self.s_z, self.r_z, self.s_x, self.r_x, self.s4, self.r4,
         self.ls, self.os, self.vs, self.vr) = sems
        self.RH = self.a4.shape[1]
        self.half = ds(at.c * self.RH, self.RH)
        self.other = ds((1 - at.c) * self.RH, self.RH)
        self.line = Line(at)

    @staticmethod
    def recv_shapes(n, R, CB):
        nz, m, nx = torus(n)
        RH = R // 2
        S = lambda *s: jax.ShapeDtypeStruct(s, F32)
        return [S(NI, nz, m, m, RH, CB), S(NI, m, nz, m, RH, CB), S(NI, m, nz, RH, CB), S(NI, nz, m, RH, CB), S(NI, m, RH, CB)]

    @staticmethod
    def bufs(n, R, CB, VR):
        nz, m, nx = torus(n)
        assert nx == m
        RH = R // 2
        V = lambda *s: pltpu.VMEM(s, F32)
        return [V(PS, nz, m, m, R, CB), V(4, nz, m, m, RH, CB), V(SLOTS, nz, m, RH, CB), V(SLOTS, nz, RH, CB), V(SLOTS, RH, CB),
                V(nz, m, m, RH, CB), V(m, nz, m, RH, CB), V(m, nz + 1, RH, CB), V(nz, m + 1, RH, CB), V(m + 1, RH, CB),
                V(nz, m, m, VR, 128), V(nz, m, m, VR, 128), V(nz, m, VR, 128), V(nz, VR, 128),
                V(nz, m, m, VR, 128), V(m, nz, m, VR, 128), V(m, nz, VR, 128), V(nz, VR, 128)]

    @staticmethod
    def sems(n):
        nz, m, nx = torus(n)
        return [DMA((NI,)), DMA((NI,)), DMA((NI, m)), DMA((NI, m)), DMA((NI, m)), DMA((NI, m)),
                DMA((NI, nz)), DMA((NI, nz)), DMA((NI,)), DMA((NI,)), DMA((NI,)), DMA((NI,)),
                DMA((8, nz)), DMA((NI,)), DMA((4, nz)), DMA((4, nz))]

    def hop0(self, i):
        return remote(self.p.at[i % PS, :, :, :, self.other], self.h0.at[i], self.s0.at[i], self.r0.at[i], self.at.dev(c=1 - self.at.c))

    def bhop(self, i, q, recv=False):
        t = Item(self.at, i)
        o = q if recv else t.b
        return remote(self.a1.at[i % 4, :, :, q], self.hb.at[i, o], self.s_b.at[i, q], self.r_b.at[i, o], t.along_b(q))

    def ahop(self, i, last, q, recv=False):
        t, sl = Item(self.at, i), i % SLOTS
        o = q if recv else t.a
        sems = (self.s_a.at[i, q], self.r_a.at[i, o], t.along_a(q))
        if last:
            return remote(self.a2.at[sl, :, q], self.ha.at[i, o], *sems)
        return remote(self.a3.at[sl, q], self.ha.at[i, o, 0], *sems)

    def zhop(self, i, last, p, recv=False):
        sl = i % SLOTS
        o = p if recv else self.at.z
        sems = (self.s_z.at[i, p], self.r_z.at[i, o], self.at.dev(z=p))
        if last:
            return remote(self.a3.at[sl, p], self.hz.at[i, o, 0], *sems)
        return remote(self.a2.at[sl, p], self.hz.at[i, o], *sems)

    def zrelay(self, i, last):
        sl, e = i % SLOTS, self.line.end
        sems = (self.s_x.at[i], self.r_x.at[i], self.at.dev(z=self.line.relay))
        if last:
            return remote(self.a3.at[sl, e], self.hx.at[i, 0], *sems)
        return remote(self.a2.at[sl, e], self.hx.at[i], *sems)

    def last(self, i, f):
        src, rows, other = self.a4.at[i % SLOTS], self.at.c * self.RH, (1 - self.at.c) * self.RH
        for here, place in self.out(i):
            @pl.when(here)
            def _():
                s, r, dev = self.s4.at[i], self.r4.at[i], self.at.dev(c=1 - self.at.c)
                f(lambda: remote(src, place(rows), s, r, dev), lambda: remote(src, place(other), s, r, dev),
                  lambda: pltpu.make_async_copy(src, place(rows), self.os.at[i]))

    def copy(self, src, dst, k, q=0):
        return pltpu.make_async_copy(src, dst, self.ls.at[k, q])

    def load_a(self, i, last, q):
        nz = self.at.NZ
        return self.copy(self.ha.at[i, q], self.la.at[q, 0:nz], 2, q) if last else self.copy(self.ha.at[i, q, 0], self.la.at[q, nz], 5, q)

    def load_z(self, i, last, p):
        m = self.at.NX
        return self.copy(self.hz.at[i, p, 0], self.lz.at[p, m], 3, p) if last else self.copy(self.hz.at[i, p], self.lz.at[p, 0:m], 6, p)

    def load_x(self, i, last):
        m = self.at.NX
        return self.copy(self.hx.at[i, 0], self.lx.at[m], 4) if last else self.copy(self.hx.at[i], self.lx.at[0:m], 7)

    def from_z(self, f):
        for p in self.line.others:
            @pl.when(self.line.direct(p))
            def _():
                f(p)

    def z_send(self, i, last):
        for p in self.line.others:
            @pl.when(self.line.direct(p) & ~(self.line.middle & (p == self.line.far)))
            def _():
                self.zhop(i, last, p).start()

        @pl.when(~self.line.middle)
        def _():
            self.zrelay(i, last).start()

    def z_sent(self, i, last):
        for p in self.line.others:
            @pl.when(self.line.direct(p))
            def _():
                self.zhop(i, last, p).wait_send()

        @pl.when(~self.line.middle)
        def _():
            self.zrelay(i, last).wait_send()

    def a_sent(self, i, last):
        for q in Item(self.at, i).others_a():
            self.ahop(i, last, q).wait_send()

    def by_type(self, i, f):
        last = z_last(i)
        for v in (True, False):
            @pl.when(last if v else ~last)
            def _():
                f(v)

    def send(self, i):
        self.hop0(i).start()

    def sends_done(self, k, i):
        if k == 1:
            for q in Item(self.at, i).others_b():
                self.bhop(i, q).wait_send()
        elif k == 2:
            self.by_type(i, lambda last: self.a_sent(i, True) if last else self.z_sent(i, False))
        elif k == 3:
            self.by_type(i, lambda last: self.z_sent(i, True) if last else self.a_sent(i, False))
        else:
            def f(to, back, own):
                to().wait_send()
                own().wait()
            self.last(i, f)

    def free(self, k, i):
        n = 4 if k == 1 else SLOTS

        @pl.when(i >= n)
        def _():
            self.sends_done(k, i - n)

    def arrive(self, k, i):
        t = Item(self.at, i)
        if k == 1:
            self.hop0(i).wait_recv()
            self.copy(self.h0.at[i], self.l0, 0).start()
        elif k == 2:
            for q in t.others_b():
                self.bhop(i, q, True).wait_recv()
                self.copy(self.hb.at[i, q], self.lb.at[q], 1, q).start()
        else:
            def f(last):
                step = {3: "a", 4: "x", 5: "z"}[k] if last else {3: "x", 4: "z", 5: "a"}[k]
                if step == "a":
                    for q in t.others_a():
                        self.ahop(i, last, q, True).wait_recv()
                        self.load_a(i, last, q).start()
                elif step == "x":
                    @pl.when(self.line.middle)
                    def _():
                        self.zrelay(i, last).wait_recv()
                        self.load_x(i, last).start()
                else:
                    def g(p):
                        self.zhop(i, last, p, True).wait_recv()
                        self.load_z(i, last, p).start()
                    self.from_z(g)
            self.by_type(i, f)

    def done(self, i, value):
        self.free(5, i)
        self.a4[i % SLOTS] = value * self.scale

        def f(to, back, own):
            to().start()
            own().start()
        self.last(i, f)

    def process(self, k, i):
        at, sl, t = self.at, i % SLOTS, Item(self.at, i)
        nz, m = at.NZ, at.NX
        if k == 1:
            self.free(1, i)
            self.copy(self.h0.at[i], self.l0, 0).wait()

            @pl.loop(0, nz)
            def _(z):
                for y in range(m):
                    for x in range(m):
                        self.a1[i % 4, z, y, x] = self.p[i % PS, z, y, x, self.half] + self.l0[z, y, x]
            for q in t.others_b():
                self.bhop(i, q).start()
        elif k == 2:
            self.free(2, i)
            for q in t.others_b():
                self.copy(self.hb.at[i, q], self.lb.at[q], 1, q).wait()

            @pl.loop(0, nz)
            def _(z):
                for a in range(m):
                    own = self.a1[i % 4, z, a, t.b]
                    for q in t.others_b():
                        own = own + self.lb[q, z, a]
                    self.a2[sl, z, a] = own

            def f(last):
                if last:
                    for q in t.others_a():
                        self.ahop(i, True, q).start()
                else:
                    self.z_send(i, False)
            self.by_type(i, f)
        else:
            if k == 3:
                pass

            def f(last):
                step = {3: "a", 4: "x", 5: "z"}[k] if last else {3: "x", 4: "z", 5: "a"}[k]
                if step == "a":
                    for q in t.others_a():
                        self.load_a(i, last, q).wait()
                    if last:
                        self.free(3, i)

                        @pl.loop(0, nz)
                        def _(z):
                            own = self.a2[sl, z, t.a]
                            for q in t.others_a():
                                own = own + self.la[q, z]
                            self.a3[sl, z] = own
                        self.z_send(i, True)
                    else:
                        own = self.a3[sl, t.a]
                        for q in t.others_a():
                            own = own + self.la[q, nz]
                        self.done(i, own)
                elif step == "x":
                    @pl.when(self.line.middle)
                    def _():
                        self.load_x(i, last).wait()
                        far = self.line.far
                        if last:
                            self.a3[sl, far] += self.lx[m]
                        else:
                            for a in range(m):
                                self.a2[sl, far, a] += self.lx[a]
                        self.zhop(i, last, far).start()
                else:
                    self.from_z(lambda p: self.load_z(i, last, p).wait())
                    if not last:
                        self.free(3, i)
                    tmp = []
                    for a in range(1 if last else m):
                        own = self.a3[sl, at.z] if last else self.a2[sl, at.z, a]
                        for p in self.line.others:
                            own = own + jnp.where(self.line.direct(p), self.lz[p, m if last else a], 0.0)
                        tmp.append(own)
                    if last:
                        self.done(i, tmp[0])
                    else:
                        for a in range(m):
                            self.a3[sl, a] = tmp[a]
                        for q in t.others_a():
                            self.ahop(i, False, q).start()
            self.by_type(i, f)

    def step(self, t, f):
        for k in (5, 4, 3, 2, 1):
            i = t - LAG[k]

            @pl.when((i >= 0) & (i < NI))
            def _():
                f(k, i)

    def finish(self):
        for i in range(NI - PS, NI):
            self.hop0(i).wait_send()
        for k, n in ((1, 4), (2, SLOTS), (3, SLOTS), (5, SLOTS)):
            @pl.loop(NI - n, NI)
            def _(i):
                self.sends_done(k, i)

        for lo, hi in ((0, E_U), (E_P, NI)):
            @pl.loop(lo, hi)
            def _(i):
                self.last(i, lambda to, back, own: back().wait_recv())

    def vhop(self, k, q, recv=False):
        a = self.at
        if k == 0:
            return remote(self.v0, self.w0, self.vs.at[0, 0], self.vr.at[0, 0], a.dev(c=1 - a.c))
        me, src, dst, dev = {1: (a.y, self.v1.at[:, q], self.w1, a.dev(y=q)), 2: (a.x, self.v2.at[:, q], self.w2, a.dev(x=q)),
                             3: (a.z, self.v3.at[q], self.w3, a.dev(z=q))}[k]
        o = q if recv else me
        return remote(src, dst.at[o], self.vs.at[k, q], self.vr.at[k, o], dev)

    def vlines(self, k):
        return [0] if k == 0 else self.at.others({1: "y", 2: "x", 3: "z"}[k])

    def small(self, k):
        a = self.at
        if k:
            for q in self.vlines(k - 1):
                self.vhop(k - 1, q, True).wait_recv()
        if k == 1:
            self.v1[...] = self.v0[...] + self.w0[...]
        if k == 2:
            own = self.v1[:, a.y]
            for q in self.vlines(1):
                own = own + self.w1[q]
            self.v2[...] = own
        if k == 3:
            own = self.v2[:, a.x]
            for q in self.vlines(2):
                own = own + self.w2[q]
            self.v3[...] = own
        if k == 4:
            own = self.v3[a.z]
            for q in self.vlines(3):
                own = own + self.w3[q]
            self.ov[...] = own * self.scale
        else:
            for q in self.vlines(k):
                self.vhop(k, q).start()

    def small_finish(self):
        for k in range(4):
            for q in self.vlines(k):
                self.vhop(k, q).wait_send()


BF = jnp.bfloat16
NN = ((1,), (0,))
NT = ((1,), (1,))
TN = ((0,), (0,))
ROW_P, ROW_G1, ROW_S1, ROW_U, ROW_D, ROW_G2, ROW_S2 = 3, 4, 5, 6, 10, 11, 12
X_, C_, N_, A_ = 0, 1, 2, 3


def mx(a, b, dims=NN):
    return lax.dot_general(a, b, (dims, ((), ())), preferred_element_type=F32)


def split(v):
    hi = v.astype(BF)
    return hi, (v - hi.astype(F32)).astype(BF)


def split32(v):
    hi = v.astype(BF).astype(F32)
    return hi, v - hi


def three(ah, al, bh, bl, dims=NN):
    return mx(ah, bh, dims) + mx(ah, bl, dims) + mx(al, bh, dims)


def left_half(shape):
    return lax.broadcasted_iota(jnp.int32, shape, 1) < HD


def pack_hl0(v):
    m = left_half(v.shape)
    h, l = split32(v)
    hr, lr = pltpu.roll(h, HD, 1), pltpu.roll(l, HD, 1)
    zero = jnp.zeros_like(v)
    one = jnp.concatenate([jnp.where(m, h, lr), jnp.where(m, h, zero)], axis=1).astype(BF)
    two = jnp.concatenate([jnp.where(m, lr, h), jnp.where(m, zero, h)], axis=1).astype(BF)
    return one, two


def pack_hhl(v):
    m = left_half(v.shape)
    h, l = split32(v)
    hr = pltpu.roll(h, HD, 1)
    one = jnp.concatenate([jnp.where(m, h, hr), l], axis=1).astype(BF)
    two = jnp.concatenate([jnp.where(m, hr, h), l], axis=1).astype(BF)
    return one, two


def pack_hl(v):
    m = left_half(v.shape)
    h, l = split32(v)
    lr = pltpu.roll(l, HD, 1)
    return jnp.where(m, h, lr).astype(BF), jnp.where(m, lr, h).astype(BF)


def fold(one, two):
    m = left_half(one.shape)
    return jnp.where(m, one, two) + pltpu.roll(jnp.where(m, two, one), HD, 1)


def stack_t(v):
    t = v.T
    out = []
    for k in range(2):
        h, l = split32(t[k * HD:(k + 1) * HD])
        out.append(jnp.concatenate([h, l], axis=0).astype(BF))
    return out


def fold_t(one, two):
    return jnp.concatenate([one[:HD] + one[HD:], two[:HD] + two[HD:]], axis=0).T


def lanes(lane, R, pieces):
    out = None
    for i, (ref, c0) in enumerate(pieces):
        t = ref[:, c0 // 128 * 128:c0 // 128 * 128 + 128]
        shift = (i * R - c0) % 128
        t = pltpu.roll(t, shift, 1) if shift else t
        out = t if out is None else jnp.where(lane == i, t, out)
    return out


def cols(start, size):
    return pl.ds(pl.multiple_of(start, 128), size)


def forward_kernel(n, x_ref, qkv_w, proj_w, up_w, down_w, v_ref, seg_ref, len_ref,
                   out_ref, g_ref, gv_ref, lh_out, ws_out, qkv_out, p_out, sl_out, hat1_out, hat2_out, inv_out, vec_out,
                   lh, wf, ws, qkv, acc, n1, r2, slope, pst, bias, gvv, vec, w_ref, ld_sem, ws_sem, out_sem, p_sem, sl_sem, in_sem, *sems):
    at = Where(n)
    L, D = x_ref.shape
    HB = D // 2
    ga = Gather(at, w_ref, g_ref, v_ref, gv_ref, sems)
    R = w_ref.shape[1]
    q = 128 // R
    parts = []
    for w in range(3):
        parts += [(2 * w + st, qkv_w.at[:, w * D + st * HB:w * D + (st + 1) * HB]) for st in range(2)]
    parts += [(6 + st, proj_w.at[:, st * HB:(st + 1) * HB]) for st in range(2)]
    parts += [(16 + 2 * j + st, down_w.at[j * R:(j + 1) * R, st * HB:(st + 1) * HB]) for j in range(4) for st in range(2)]
    parts = [pltpu.make_async_copy(src, w_ref.at[i], in_sem.at[k]) for k, (i, src) in enumerate(parts)]
    for part in parts:
        part.start()
    lane = lax.broadcasted_iota(jnp.int32, (R, 128), 1) // R
    for j in range(4):
        for k in range(D // 128):
            t = lanes(lane, R, [(up_w, (k * q + i) * 4 * R + j * R) for i in range(q)])
            w_ref[8 + 2 * j + k * 128 // HB, :, k * 128 % HB:k * 128 % HB + 128] = t
    at.barrier()
    for part in parts:
        part.wait()
    ga.begin()
    ga.begin_local()

    def lh_copy(s):
        return pltpu.make_async_copy(lh.at[s], lh_out.at[s], out_sem.at[s])

    RB = 128

    @pl.loop(0, L // RB)
    def _(r):
        rows = pl.ds(pl.multiple_of(r * RB, RB), RB)
        h, l = split(x_ref[rows])
        lh[X_, 0, rows] = h
        lh[X_, 1, rows] = l
        kpos = lax.broadcasted_iota(jnp.int32, (RB, L), 0) + r * RB
        qpos = lax.broadcasted_iota(jnp.int32, (RB, L), 1)
        own = seg_ref[:, rows].astype(F32)
        own = jnp.broadcast_to(own, (RB, RB)).T[:, :1]
        allowed = (own == seg_ref[...].astype(F32)) & ((kpos < len_ref[0]) | (kpos == qpos))
        bias[rows] = jnp.where(allowed, 0.0, MASKED)
    lh_copy(X_).start()
    @pl.loop(0, 2 + G_LAG[4])
    def _(t):
        ga.step(t)
    cp = pltpu.make_async_copy(gv_ref, gvv, ld_sem.at[0])
    cp.start()
    cp.wait()
    for k in range(D // 128):
        s = None
        for j in range(q):
            c = k * q + j
            blk = gvv[c // (at.NY * at.NX), (c // at.NX) % at.NY, c % at.NX]
            s = blk if s is None else s + blk
        vec[:, k * 128:(k + 1) * 128] = s
    vcp = pltpu.make_async_copy(vec, vec_out, out_sem.at[7])
    vcp.start()

    def load(w, st):
        return pltpu.make_async_copy(g_ref.at[2 * w + st], wf.at[st], ld_sem.at[st])

    def ws_copy(w, st):
        return pltpu.make_async_copy(ws.at[st], ws_out.at[w, st], ws_sem.at[st])

    def weights(w):
        for st in range(2):
            ga.ready(2 * w + st)
            load(w, st).start()

    def half(w, st, s):
        load(w, st).wait()

        @pl.when(w > 0)
        def _():
            ws_copy(w - 1, st).wait()

        @pl.loop(0, at.NZ)
        def _(z):
            for a in range(at.NY):
                for b in range(at.NX):
                    y, x = (a, b) if st == 0 else (b, a)
                    r0 = pl.multiple_of(((z * at.NY + y) * at.NX + x) * R, R)
                    h, l = split(wf[st, z, a, b])
                    ws[st, 0, pl.ds(r0, R)] = h
                    ws[st, 1, pl.ds(r0, R)] = l
        ws_copy(w, st).start()
        acc[...] = three(lh[s, 0], lh[s, 1], ws[st, 0], ws[st, 1])

    T0 = 2 + G_LAG[4]

    def qkv_copy(w):
        return pltpu.make_async_copy(qkv.at[w], qkv_out.at[w], out_sem.at[8 + w])

    @pl.loop(0, 3)
    def _(w):
        weights(w)
        f = jnp.where(w == 0, 1.0 / math.sqrt(HD), 1.0).astype(F32)
        for st in range(2):
            half(w, st, X_)
            b = vec[pl.ds(w, 1), st * HB:(st + 1) * HB]
            qkv[w, :, st * HB:(st + 1) * HB] = (acc[...] + b) * f
            ga.step(T0 + 2 * w + st)
        qkv_copy(w).start()

    def p_copy(p):
        return pltpu.make_async_copy(pst.at[p % 2], p_out.at[p], p_sem.at[p % 2])

    def attend(p):
        c = cols(p * 128, 128)
        qp, kp, vp = qkv[0, :, c], qkv[1, :, c], qkv[2, :, c]
        qs, ks, vt = pack_hhl(qp), pack_hl0(kp), stack_t(vp)

        @pl.when(p >= 2)
        def _():
            p_copy(p - 2).wait()
        res = []
        for k in range(2):
            s = mx(ks[k], qs[k], NT) + bias[...]
            e = jnp.exp(s - jnp.max(s, axis=0, keepdims=True))
            e = e * (1.0 / jnp.sum(e, axis=0, keepdims=True))
            ph, pll = split(e)
            pst[p % 2, k, 0] = ph
            pst[p % 2, k, 1] = pll
            res.append(mx(vt[k], ph) + mx(vt[k], pll))
        p_copy(p).start()
        h, l = split(fold_t(*res))
        lh[C_, 0, :, c] = h
        lh[C_, 1, :, c] = l

    @pl.loop(0, H // 2)
    def _(p):
        attend(p)

        @pl.when(p % 4 != 3)
        def _():
            ga.step(T0 + 6 + p - p // 4)
    lh_copy(C_).start()

    weights(3)
    for st in range(2):
        half(3, st, C_)
        c = slice(st * HB, (st + 1) * HB)
        n1[:, c] = x_ref[:, c] + acc[...] + vec[ROW_P:ROW_P + 1, c]
    @pl.loop(T0 + 12, T0 + 13)
    def _(t):
        ga.step(t)

    def norm_rows(ref, k, hat_ref, rows):
        v = ref[rows]
        center = v - jnp.mean(v, axis=-1, keepdims=True)
        inverse = lax.rsqrt(jnp.mean(center * center, axis=-1, keepdims=True) + EPSILON)
        hat = center * inverse
        return hat, inverse

    @pl.loop(0, L // RB)
    def _(r):
        rows = pl.ds(pl.multiple_of(r * RB, RB), RB)
        hat, inverse = norm_rows(n1, 0, None, rows)
        r2[rows] = hat
        inv_out[rows, 0:128] = jnp.broadcast_to(inverse, (RB, 128))
        v = hat * vec[ROW_G1:ROW_G1 + 1] + vec[ROW_S1:ROW_S1 + 1]
        n1[rows] = v
        h, l = split(v)
        lh[N_, 0, rows] = h
        lh[N_, 1, rows] = l
    lh_copy(N_).start()
    hcp = pltpu.make_async_copy(r2, hat1_out, out_sem.at[11])
    hcp.start()

    def sl_copy(j, st):
        return pltpu.make_async_copy(slope.at[st], sl_out.at[j, st], sl_sem.at[st])

    @pl.loop(0, 4)
    def _(j):
        weights(4 + j)
        for st in range(2):
            half(4 + j, st, N_)
            c = slice(st * HB, (st + 1) * HB)

            @pl.when(j > 0)
            def _():
                sl_copy(j - 1, st).wait()
            b = vec[pl.ds(ROW_U + j, 1), c]

            @pl.loop(0, L // 64)
            def _(r):
                rows = pl.ds(pl.multiple_of(r * 64, 64), 64)
                u = acc[rows] + b
                phi = 0.5 * (1.0 + lax.erf(u * math.sqrt(0.5)))
                h, l = split(u * phi)
                lh[A_ + j, 0, rows, c] = h
                lh[A_ + j, 1, rows, c] = l
                slope[st, rows] = phi + u * jnp.exp(-0.5 * u * u) * (1.0 / math.sqrt(2.0 * math.pi))
            sl_copy(j, st).start()
            if st == 0:
                ga.step(T0 + 13 + j)
        lh_copy(A_ + j).start()

    hcp.wait()
    r2[...] = n1[...] + vec[ROW_D:ROW_D + 1]

    @pl.loop(0, 4)
    def _(j):
        weights(8 + j)
        for st in range(2):
            half(8 + j, st, A_ + j)
            r2[:, st * HB:(st + 1) * HB] += acc[...]

            @pl.when((j < 3) if st == 0 else (j == 1) | (j == 2))
            def _():
                ga.step(T0 + 17 + j + (j == 2).astype(jnp.int32) if st == 0 else T0 + 17 + 2 * j)

    @pl.loop(0, L // RB)
    def _(r):
        rows = pl.ds(pl.multiple_of(r * RB, RB), RB)
        hat, inverse = norm_rows(r2, 1, None, rows)
        r2[rows] = hat
        inv_out[rows, 128:256] = jnp.broadcast_to(inverse, (RB, 128))
        out_ref[rows] = hat * vec[ROW_G2:ROW_G2 + 1] + vec[ROW_S2:ROW_S2 + 1]
    hcp2 = pltpu.make_async_copy(r2, hat2_out, out_sem.at[11])
    hcp2.start()
    vcp.wait()
    for s in range(7):
        lh_copy(s).wait()
    for w in range(3):
        qkv_copy(w).wait()
    for p in (H // 2 - 2, H // 2 - 1):
        p_copy(p).wait()
    for st in range(2):
        sl_copy(3, st).wait()
        ws_copy(NW - 1, st).wait()
    hcp2.wait()
    ga.finish()


def forward(n, x, qkv, proj, up, down, v, seg, length):
    nz, ny, nx = torus(n)
    R, HB = proj.shape[0], proj.shape[1] // 2
    L, D = x.shape
    S = lambda shape, t=F32: jax.ShapeDtypeStruct(shape, t)
    V = pltpu.VMEM
    ANY = pl.BlockSpec(memory_space=pl.ANY)
    VM = pl.BlockSpec(memory_space=pltpu.VMEM)
    return pl.pallas_call(
        functools.partial(forward_kernel, n),
        out_shape=[S((L, D)), S((NI, nz, ny, nx, R, HB)), S((nz, ny, nx) + v.shape), S((7, 2, L, D), BF),
                   S((NW, 2, 2, D, HB), BF), S((3, L, D)), S((H // 2, 2, 2, L, L), BF), S((4, 2, L, HB)),
                   S((L, D)), S((L, D)), S((L, 256)), S((v.shape[0], D))],
        in_specs=[VM, ANY, ANY, VM, ANY, VM, VM, pl.BlockSpec(memory_space=pltpu.SMEM)],
        out_specs=[VM] + [ANY] * 9 + [VM, ANY],
        scratch_shapes=[V((7, 2, L, D), BF), V((2, nz, ny, nx, R, HB), F32), V((2, 2, D, HB), BF), V((3, L, D), F32),
                        V((L, HB), F32), V((L, D), F32), V((L, D), F32), V((2, L, HB), F32), V((2, 2, 2, L, L), BF),
                        V((L, L), F32), V((nz, ny, nx) + v.shape, F32), V((v.shape[0], D), F32), V((NI, R, HB), F32),
                        DMA((2,)), DMA((2,)), DMA((12,)), DMA((2,)), DMA((2,)), DMA((16,))] + Gather.sems(n),
        compiler_params=pltpu.CompilerParams(collective_id=0, has_side_effects=True, vmem_limit_bytes=63 * 2**20),
        name="forward",
    )(x, qkv, proj, up, down, v, seg, length)


E_PAIR = 9
R_R2, R_U, R_R1, R_Q = 0, 1, 5, 6


def backward_kernel(n, scale, ct_ref, hat2_ref, hat1_ref, inv_ref, lh_ref, ws_ref, qkv_ref, p_ref, sl_ref, vec,
                    dx_ref, qkv_o, proj_o, up_o, down_o, ov_ref, rhs_ref, h0, h1, h2, h3, h4,
                    lbuf, rbuf, wbuf, sbuf, pbuf, qbuf, dr2, du, dn1, fb, dst, small, uo,
                    l_sem, r_sem, w_sem, s_sem, p_sem, q_sem, f_sem, o_sem, d_sem, *rest):
    at = Where(n)
    bufs, sems = rest[:18], rest[18:]
    L, D = dx_ref.shape
    HB = D // 2
    R = up_o.shape[0]
    RH = R // 2

    def places(e):
        block = lambda ref, r, c: ref.at[pl.ds(pl.multiple_of(r, 8), RH), cols(c, HB)]
        return [(e < E_U, lambda r: block(down_o, e // 2 * R + r, e % 2 * HB)),
                ((e >= E_U) & (e < E_P), lambda r: uo.at[jnp.clip(e - E_U, 0, 7), pl.ds(pl.multiple_of(r, 8), RH)]),
                ((e >= E_P) & (e < E_Q), lambda r: block(proj_o, r, e % 2 * HB)),
                (e >= E_Q, lambda r: block(qkv_o, r, (e - E_Q) % 3 * D + (e - E_Q) // 3 * HB))]

    rd = Reduce(at, places, ov_ref, (h0, h1, h2, h3, h4), bufs, sems, scale)
    RB = 128
    FB = D // at.NZ
    copy = pltpu.make_async_copy

    def f_load(src, k):
        return copy(src, fb.at[k], f_sem.at[k])

    def lhs_slot(e):
        return jnp.where(e < E_U, A_ + e // 2, jnp.where(e < E_P, N_, jnp.where(e < E_Q, C_, X_)))

    def rhs_slot(e):
        return jnp.where(e < E_U, R_R2, jnp.where(e < E_P, R_U + (e - E_U) // 2, jnp.where(e < E_Q, R_R1, R_Q + (e - E_Q) % 3)))

    def rhs_half(e):
        return jnp.where(e < E_Q, e % 2, (e - E_Q) // 3)

    def l_load(e):
        return copy(lh_ref.at[lhs_slot(e)], lbuf.at[e % 2], l_sem.at[e % 2])

    def r_load(e):
        return copy(rhs_ref.at[rhs_slot(e), :, :, cols(rhs_half(e) * HB, HB)], rbuf.at[e % 2], r_sem.at[e % 2])

    def w_load(e, k):
        pairs = jnp.where(e < E_U, jnp.where(e % 2 == 0, 8, 4) + e // 2, 3)
        w = jnp.where(e < E_Q, pairs, (e - E_Q) % 3)
        h = jnp.where(e < E_Q, k, (e - E_Q) // 3)
        return copy(ws_ref.at[w, h], wbuf.at[e % 2, k], w_sem.at[e % 2, k])

    def s_load(j):
        return copy(sl_ref.at[j], sbuf, s_sem)

    def p_load(p):
        return copy(p_ref.at[p], pbuf.at[p % 2], p_sem.at[p % 2])

    def q_load(p):
        return copy(qkv_ref.at[:, :, cols(p * 128, 128)], qbuf.at[p % 2], q_sem.at[p % 2])

    def rhs_store(src, slot, k):
        return copy(src, rhs_ref.at[slot], o_sem.at[k])

    f_load(ct_ref, 0).start()
    f_load(hat2_ref, 1).start()
    l_load(0).start()
    for k in range(2):
        w_load(0, k).start()
    s_load(0).start()
    at.barrier()
    small[...] = jnp.zeros_like(small)
    f_load(ct_ref, 0).wait()
    f_load(hat2_ref, 1).wait()

    def norm_back(r, g, hat, inverse, gain, row_shift, row_gain):
        gg = g * gain
        small[row_shift:row_shift + 1] += jnp.sum(g, axis=0, keepdims=True)
        small[row_gain:row_gain + 1] += jnp.sum(g * hat, axis=0, keepdims=True)
        return inverse * (gg - jnp.mean(gg, -1, keepdims=True) - hat * jnp.mean(gg * hat, -1, keepdims=True))

    @pl.loop(0, L // RB)
    def _(r):
        rows = pl.ds(pl.multiple_of(r * RB, RB), RB)
        d = norm_back(r, fb[0, rows], fb[1, rows], inv_ref[rows, 128:129], vec[ROW_G2:ROW_G2 + 1], ROW_S2, ROW_G2)
        small[ROW_D:ROW_D + 1] += jnp.sum(d, axis=0, keepdims=True)
        dn1[rows] = d
        h, l = split(d)
        dr2[0, rows] = h
        dr2[1, rows] = l
    rhs_store(dr2, R_R2, 0).start()
    f_load(hat1_ref, 0).start()
    rhs_store(dr2, R_R2, 0).wait()
    r_load(0).start()

    def chunk_da(j, e):
        for k in range(2):
            w_load(e, k).wait()
        s_load(j).wait()

        @pl.when(j > 0)
        def _():
            rhs_store(du, R_U + j - 1, 1).wait()
        for k in range(4):
            b = slice(k * FB, (k + 1) * FB)
            v = three(dr2[0, :, :HB], dr2[1, :, :HB], wbuf[e % 2, 0, 0, b], wbuf[e % 2, 0, 1, b], NT) \
                + three(dr2[0, :, HB:], dr2[1, :, HB:], wbuf[e % 2, 1, 0, b], wbuf[e % 2, 1, 1, b], NT)
            half, off = (k * FB) // HB, (k * FB) % HB
            v = v * sbuf[half, :, off:off + FB]
            small[pl.ds(ROW_U + j, 1), b] = jnp.sum(v, axis=0, keepdims=True)
            h, l = split(v)
            du[0, :, b] = h
            du[1, :, b] = l
        rhs_store(du, R_U + j, 1).start()

        @pl.when(j < 3)
        def _():
            s_load(j + 1).start()

    def nt_into(ref, a, e, b):
        return ref[:, b] + three(a[0, :, :HB], a[1, :, :HB], wbuf[e % 2, 0, 0, b], wbuf[e % 2, 0, 1, b], NT) \
            + three(a[0, :, HB:], a[1, :, HB:], wbuf[e % 2, 1, 0, b], wbuf[e % 2, 1, 1, b], NT)

    def chunk_dn(e):
        for k in range(2):
            w_load(e, k).wait()
        for k in range(4):
            b = slice(k * FB, (k + 1) * FB)
            dn1[:, b] = nt_into(dn1, du, e, b)

    def chunk_norm():
        f_load(hat1_ref, 0).wait()

        @pl.loop(0, L // RB)
        def _(r):
            rows = pl.ds(pl.multiple_of(r * RB, RB), RB)
            d = norm_back(r, dn1[rows], fb[0, rows], inv_ref[rows, 0:1], vec[ROW_G1:ROW_G1 + 1], ROW_S1, ROW_G1)
            small[ROW_P:ROW_P + 1] += jnp.sum(d, axis=0, keepdims=True)
            dn1[rows] = d
            h, l = split(d)
            dr2[0, rows] = h
            dr2[1, rows] = l
        rhs_store(du, R_U + 3, 1).wait()
        rhs_store(dr2, R_R1, 0).start()

    def chunk_dc(e):
        for k in range(2):
            w_load(e, k).wait()
        for k in range(4):
            b = slice(k * FB, (k + 1) * FB)
            fb[1, :, b] = three(dr2[0, :, :HB], dr2[1, :, :HB], wbuf[e % 2, 0, 0, b], wbuf[e % 2, 0, 1, b], NT) \
                + three(dr2[0, :, HB:], dr2[1, :, HB:], wbuf[e % 2, 1, 0, b], wbuf[e % 2, 1, 1, b], NT)
        rhs_store(dr2, R_R1, 0).wait()

    def d_store(p, k):
        return copy(dst.at[p % 2, k], rhs_ref.at[R_Q + k, :, :, cols(p * 128, 128)], d_sem.at[p % 2, k])

    def chunk_pair(p):
        c = cols(p * 128, 128)
        s = p % 2
        p_load(p).wait()
        q_load(p).wait()

        @pl.when(p < H // 2 - 1)
        def _():
            p_load(p + 1).start()
            q_load(p + 1).start()
        qp, kp, vp, dc = qbuf[s, 0], qbuf[s, 1], qbuf[s, 2], fb[1, :, c]
        va, da, kt, qx, dx = pack_hl0(vp), pack_hhl(dc), stack_t(kp), pack_hl(qp), pack_hl(dc)
        dq, dk, dv = [], [], []
        for k in range(2):
            dp = mx(va[k], da[k], NT)
            ph, pll = pbuf[s, k, 0], pbuf[s, k, 1]
            pf = ph.astype(F32) + pll.astype(F32)
            t = pf * dp
            t = t - pf * jnp.sum(t, axis=0, keepdims=True)
            sh, sll = split(t)
            dk.append(mx(sh, qx[k]) + mx(sll, qx[k]))
            dv.append(mx(ph, dx[k]) + mx(pll, dx[k]))
            dq.append(mx(kt[k], sh) + mx(kt[k], sll))
        out = (fold_t(*dq) * (1.0 / math.sqrt(HD)), fold(*dk), fold(*dv))

        @pl.when(p >= 2)
        def _():
            for k in range(3):
                d_store(p - 2, k).wait()
        for k in range(3):
            small[k:k + 1, c] = jnp.sum(out[k], axis=0, keepdims=True)
            h, l = split(out[k])
            dst[s, k, 0] = h
            dst[s, k, 1] = l
            d_store(p, k).start()

    def chunk_dx(e):
        w_load(e, 0).wait()
        for k in range(4):
            b = slice(k * FB, (k + 1) * FB)
            dn1[:, b] += three(rbuf[e % 2, 0], rbuf[e % 2, 1], wbuf[e % 2, 0, 0, b], wbuf[e % 2, 0, 1, b], NT)

    @pl.loop(0, NI + LAG[5])
    def _(e):
        @pl.when(e < NI)
        def _():
            l_load(e).wait()
            r_load(e).wait()

            @pl.when(e >= PS)
            def _():
                rd.hop0(e - PS).wait_send()

            @pl.loop(0, at.NZ)
            def _(z):
                b = cols(z * FB, FB)
                v = three(lbuf[e % 2, 0, :, b], lbuf[e % 2, 1, :, b], rbuf[e % 2, 0], rbuf[e % 2, 1], TN)
                odd = e % 2 == 1
                for y in range(at.NY):
                    for x in range(at.NX):
                        k = (y * at.NX + x) * R
                        rd.p[e % PS, z, jnp.where(odd, x, y), jnp.where(odd, y, x)] = v[k:k + R]
            rd.send(e)

            @pl.when(e < NI - 1)
            def _():
                l_load(e + 1).start()
                r_load(e + 1).start()

            @pl.when((e < E_U) | ((e >= E_Q - 1) & (e < NI - 1)))
            def _():
                w_load(e + 1, 0).start()

            @pl.when(e < E_U)
            def _():
                w_load(e + 1, 1).start()
        rd.step(e, rd.arrive)

        @pl.when((e < E_U) & (e % 2 == 0))
        def _():
            chunk_da(e // 2, e)

        @pl.when((e < E_U) & (e % 2 == 1))
        def _():
            chunk_dn(e)

        @pl.when(e == E_U - 1)
        def _():
            chunk_norm()

        @pl.when(e == E_U)
        def _():
            p_load(0).start()
            q_load(0).start()
            chunk_dc(e)

        @pl.when((e >= E_PAIR) & (e < E_PAIR + H // 2))
        def _():
            chunk_pair(e - E_PAIR)

        @pl.when(e == E_PAIR + H // 2)
        def _():
            for p in (H // 2 - 2, H // 2 - 1):
                for k in range(3):
                    d_store(p, k).wait()
            for z in range(at.NZ):
                for y in range(at.NY):
                    for x in range(at.NX):
                        g = ((z * at.NY + y) * at.NX + x) * 2 * rd.RH // 128
                        rd.v0[z, y, x] = small[:, g * 128:(g + 1) * 128]

        for k in range(5):
            @pl.when(e == E_PAIR + H // 2 + k)
            def _():
                rd.small(k)

        @pl.when((e >= E_Q) & (e < NI))
        def _():
            chunk_dx(e)

        @pl.when(e == NI - 1)
        def _():
            copy(dn1, dx_ref, o_sem.at[0]).start()
        rd.step(e, rd.process)

        @pl.when(e == E_P + LAG[5] + 1)
        def _():
            @pl.loop(E_U, E_P)
            def _(i):
                def f(to, back, own):
                    back().wait_recv()
                rd.last(i, f)
    copy(dn1, dx_ref, o_sem.at[0]).wait()
    rd.finish()
    lane = lax.broadcasted_iota(jnp.int32, (R, 128), 1) // R
    for t in range(4 * D // 128):
        pieces = []
        for i in range(128 // R):
            f0 = t * 128 + i * R
            chip, j = f0 // (4 * R), f0 % (4 * R) // R
            pieces.append((uo.at[2 * j + chip * R // HB], chip * R % HB))
        up_o[:, t * 128:(t + 1) * 128] = lanes(lane, R, pieces)
    rd.small_finish()


def backward(n, R, scale, ct, hat2, hat1, inv, lh, ws, qkv, p, sl, vec):
    L, D = ct.shape
    HB = D // 2
    VR = vec.shape[0]
    S = lambda shape, t=F32: jax.ShapeDtypeStruct(shape, t)
    V = pltpu.VMEM
    ANY = pl.BlockSpec(memory_space=pl.ANY)
    VM = pl.BlockSpec(memory_space=pltpu.VMEM)
    return pl.pallas_call(
        functools.partial(backward_kernel, n, scale),
        out_shape=[S((L, D)), S((R, 3 * D)), S((R, D)), S((R, 4 * D)), S((4 * R, D)), S((VR, 128)), S((9, 2, L, D), BF)] + Reduce.recv_shapes(n, R, HB),
        in_specs=[ANY, ANY, ANY, VM, ANY, ANY, ANY, ANY, ANY, VM],
        out_specs=[ANY, ANY, ANY, VM, ANY, VM] + [ANY] * 6,
        scratch_shapes=[V((2, 2, L, D), BF), V((2, 2, L, HB), BF), V((2, 2, 2, D, HB), BF), V((2, L, HB), F32),
                        V((2, 2, 2, L, L), BF), V((2, 3, L, 128), F32), V((2, L, D), BF), V((2, L, D), BF), V((L, D), F32),
                        V((2, L, D), F32), V((2, 3, 2, L, 128), BF), V((VR, D), F32), V((8, R, HB), F32),
                        DMA((2,)), DMA((2,)), DMA((2, 2)), DMA(()), DMA((2,)), DMA((2,)), DMA((2,)), DMA((2,)), DMA((2, 3))]
        + Reduce.bufs(n, R, HB, VR) + Reduce.sems(n),
        compiler_params=pltpu.CompilerParams(collective_id=1, has_side_effects=True, vmem_limit_bytes=63 * 2**20),
        name="backward",
    )(ct, hat2, hat1, inv, lh, ws, qkv, p, sl, vec)[:6]


VROWS = 16


def lane(R):
    return (lax.axis_index("shard") * R) % 128


def pack_small(before, up_bias, after):
    R = before[0].shape[0]
    rows = jnp.concatenate(before + [up_bias] + after + [jnp.zeros((3 * R,), F32)]).reshape(VROWS, R)
    here = lax.broadcasted_iota(jnp.int32, (VROWS, 128), 1) // R == lax.axis_index("shard") % (128 // R)
    return jnp.where(here, jnp.concatenate([rows] * (128 // R), axis=1), 0.0)


def shards(n, tokens, segment_ids, valid_lengths, qkv_weight, query_bias, value_bias, proj_weight, proj_bias, first_gain,
           first_shift, up_weight, up_bias, down_weight, down_bias, second_gain, second_shift, cotangent):
    amount, length, D = tokens.shape
    R = proj_weight.shape[0]
    x = tokens.reshape(amount * length, D)
    vsh = pack_small([query_bias, jnp.zeros_like(query_bias), value_bias, proj_bias, first_gain, first_shift], up_bias,
                     [down_bias, second_gain, second_shift])
    out, g, gv, lh, ws, qkv, pr, sl, hat1, hat2, inv, v = forward(
        n, x, qkv_weight, proj_weight, up_weight, down_weight, vsh, segment_ids, valid_lengths)
    scale = 1.0 / math.sqrt(amount * length * n * lax.axis_size("rep"))
    dx, gqkv, gproj, gup, gdown, ov = backward(n, R, scale, cotangent.reshape(amount * length, D), hat2, hat1, inv, lh, ws, qkv, pr, sl, v)
    s = lax.dynamic_slice(ov, (0, lane(R)), (VROWS, R))
    return (out.reshape(amount, length, D), dx.reshape(amount, length, D), gqkv, s[0], s[2], gproj, s[3], s[4], s[5], gup,
            s[6:10].reshape(4 * R), gdown, s[10], s[11], s[12])


def solution(mesh):
    n = mesh.shape["shard"]
    one, two, seq = P("shard"), P("shard", None), P(("shard", "rep"), None, None)
    return jax.shard_map(
        functools.partial(shards, n),
        mesh=mesh,
        in_specs=(seq, P(("shard", "rep"), None), P(("shard", "rep")), two, one, one, two, one, one, one, two, one, two, one, one, one, seq),
        out_specs=(seq, seq, two, one, one, two, one, one, one, two, one, two, one, one, one),
        check_vma=False,
    )
```

```python
import functools
import math

import jax
import jax.numpy as jnp
from jax import lax
from jax.experimental import pallas as pl
from jax.experimental.pallas import tpu as pltpu
from jax.sharding import PartitionSpec as P

H = 16
HD = 64
HIGH = lax.Precision.HIGH
EPSILON = 1e-05
MASKED = -1000000000.0
MESH = pl.DeviceIdType.MESH
DMA = pltpu.SemaphoreType.DMA
F32 = jnp.float32
VMEM_LIMIT = 60 * 2**20
NW = 12


def torus(n):
    side = math.isqrt(n // 4)
    assert side * side * 4 == n
    return 4, side, side


def ds(start, size, align=8):
    return pl.ds(pl.multiple_of(start, align), size)


class Where:
    def __init__(self, n):
        self.NZ, self.NY, self.NX = torus(n)
        s = lax.axis_index("shard")
        self.s = s
        self.c = lax.axis_index("rep")
        self.z = s // (self.NY * self.NX)
        self.y = (s // self.NX) % self.NY
        self.x = s % self.NX

    def dev(self, z=None, y=None, x=None, c=None):
        z = self.z if z is None else z
        y = self.y if y is None else y
        x = self.x if x is None else x
        c = self.c if c is None else c
        return (z * (self.NY * self.NX) + y * self.NX + x, c)

    def partners(self):
        out = [self.dev(c=1 - self.c)]
        out += [self.dev(z=p) for p in self.others("z")]
        out += [self.dev(y=p) for p in self.others("y")]
        out += [self.dev(x=p) for p in self.others("x")]
        return out

    def others(self, axis):
        me, n = self.line(axis)
        return [(me + d) % n for d in range(1, n)]

    def line(self, axis):
        return {"z": (self.z, self.NZ), "y": (self.y, self.NY), "x": (self.x, self.NX)}[axis]

    def greet(self):
        for p in self.partners():
            pl.semaphore_signal(pltpu.get_barrier_semaphore(), inc=1, device_id=p, device_id_type=MESH)

    def met(self):
        pl.semaphore_wait(pltpu.get_barrier_semaphore(), len(self.partners()))


def remote(src, dst, ssem, rsem, dev):
    return pltpu.make_async_remote_copy(
        src_ref=src, dst_ref=dst, send_sem=ssem, recv_sem=rsem, device_id=dev, device_id_type=MESH
    )


NI = 2 * NW


def z_first(i):
    w = i // 2
    return (w % 2 == 0) & (w < NW - 2)


def z_last(i):
    w = i // 2
    return w % 2 == 1


class Item:
    def __init__(self, at, i):
        swap = i % 2 == 1
        self.i, self.at, self.n = i, at, at.NX
        self.a = jnp.where(swap, at.x, at.y)
        self.b = jnp.where(swap, at.y, at.x)
        self.swap = swap

    def chip(self, z, a, b):
        return (z * self.n + jnp.where(self.swap, b, a)) * self.n + jnp.where(self.swap, a, b)

    def along_a(self, q):
        return (self.chip(self.at.z, q, self.b), self.at.c)

    def along_b(self, q):
        return (self.chip(self.at.z, self.a, q), self.at.c)

    def others_a(self):
        return [(self.a + d) % self.n for d in range(1, self.n)]

    def others_b(self):
        return [(self.b + d) % self.n for d in range(1, self.n)]


class Line:
    def __init__(self, at):
        assert at.NZ == 4
        self.z = at.z
        self.others = at.others("z")
        self.middle = (at.z == 1) | (at.z == 2)
        self.far = jnp.where(at.z == 2, 0, 3)
        self.near = jnp.where(at.z == 2, 3, 0)
        self.end = jnp.where(at.z == 0, 3, 0)
        self.relay = jnp.where(at.z == 0, 1, 2)

    def direct(self, p):
        return jnp.abs(p - self.z) != 3


G_LAG = {1: 0, 2: 1, 3: 3, 4: 6}
G_AHEAD = 3


class Gather:
    def __init__(self, at, w_ref, g_ref, v_ref, gv_ref, sems):
        self.at, self.w, self.g, self.v, self.gv = at, w_ref, g_ref, v_ref, gv_ref
        (self.l, self.zs, self.zr, self.zx, self.s_a, self.r_a, self.s_b, self.r_b, self.ss, self.rs, self.vs, self.vr) = sems
        R = w_ref.shape[1]
        self.RH = R // 2
        self.half = ds(at.c * self.RH, self.RH)
        self.other = ds((1 - at.c) * self.RH, self.RH)
        self.line = Line(at)

    @staticmethod
    def sems(n):
        nz, ny, nx = torus(n)
        return [DMA((NI + 1,)), DMA((NI, nz)), DMA((NI, nz)), DMA((NI,)), DMA((NI, nx)), DMA((NI, nx)),
                DMA((NI, nx)), DMA((NI, nx)), DMA((NI,)), DMA((NI,)), DMA((3, nz)), DMA((3, nz))]

    def local(self, i):
        t = Item(self.at, i)
        return pltpu.make_async_copy(self.w.at[i, self.half], self.g.at[i, self.at.z, t.a, t.b, self.half], self.l.at[i])

    def local_v(self):
        a = self.at
        return pltpu.make_async_copy(self.v, self.gv.at[a.z, a.y, a.x], self.l.at[NI])

    def own(self, i, z):
        pass

    def zhop(self, i, first, p, recv=False):
        t, z = Item(self.at, i), self.at.z
        o = p if recv else z
        sems = (self.zs.at[i, p], self.zr.at[i, o], self.at.dev(z=p))
        if first:
            return remote(self.w.at[i, self.half], self.g.at[i, o, t.a, t.b, self.half], *sems)
        return remote(self.g.at[i, o, :, t.b, self.half], self.g.at[i, o, :, t.b, self.half], *sems)

    def zrelay(self, i, first):
        t, o, p = Item(self.at, i), self.line.far, self.line.near
        ref = self.g.at[i, o, t.a, t.b, self.half] if first else self.g.at[i, o, :, t.b, self.half]
        return remote(ref, ref, self.zx.at[i], self.zr.at[i, o], self.at.dev(z=p))

    def ahop(self, i, first, q, recv=False):
        t, z = Item(self.at, i), self.at.z
        o = q if recv else t.a
        sems = (self.s_a.at[i, q], self.r_a.at[i, o], t.along_a(q))
        if first:
            return remote(self.g.at[i, :, o, t.b, self.half], self.g.at[i, :, o, t.b, self.half], *sems)
        return remote(self.w.at[i, self.half], self.g.at[i, z, o, t.b, self.half], *sems)

    def bhop(self, i, q, recv=False):
        t = Item(self.at, i)
        o = q if recv else t.b
        ref = self.g.at[i, :, :, o, self.half]
        return remote(ref, ref, self.s_b.at[i, q], self.r_b.at[i, o], t.along_b(q))

    def pair(self, i, recv=False):
        ref = self.g.at[i, :, :, :, self.other if recv else self.half]
        return remote(ref, ref, self.ss.at[i], self.rs.at[i], self.at.dev(c=1 - self.at.c))

    def small(self, hop, p, recv=False):
        a, g = self.at, self.gv
        if hop == 0:
            o = p if recv else a.z
            return remote(self.v, g.at[o, a.y, a.x], self.vs.at[0, p], self.vr.at[0, o], a.dev(z=p))
        if hop == 1:
            o = p if recv else a.x
            return remote(g.at[:, a.y, a.x], g.at[:, a.y, o], self.vs.at[1, p], self.vr.at[1, o], a.dev(x=p))
        o = p if recv else a.y
        return remote(g.at[:, a.y], g.at[:, o], self.vs.at[2, p], self.vr.at[2, o], a.dev(y=p))

    def z_send(self, i, first):
        for p in self.line.others:
            @pl.when(self.line.direct(p))
            def _():
                self.zhop(i, first, p).start()

    def z_pass(self, i, first):
        @pl.when(self.line.middle)
        def _():
            self.zhop(i, first, self.line.far, True).wait_recv()
            self.zrelay(i, first).start()

    def z_wait(self, i, first):
        for p in self.line.others:
            @pl.when(~(self.line.middle & (p == self.line.far)))
            def _():
                self.zhop(i, first, p, True).wait_recv()

    def a_send(self, i, first):
        for q in Item(self.at, i).others_a():
            self.ahop(i, first, q).start()

    def a_wait(self, i, first):
        for q in Item(self.at, i).others_a():
            self.ahop(i, first, q, True).wait_recv()

    def begin_local(self):
        self.local_v().start()

        @pl.loop(0, NI)
        def _(i):
            self.local(i).start()

    def begin(self):
        for p in self.at.others("z"):
            self.small(0, p).start()

        @pl.loop(0, NI)
        def _(i):
            @pl.when((i < G_AHEAD) | ~z_first(i))
            def _():
                self.stage(0, i)

    def small_step(self, hop):
        a = self.at
        here, nxt = (("z", "x"), ("x", "y"), ("y", None))[hop]
        if hop == 0:
            self.local_v().wait()
        for p in a.others(here):
            self.small(hop, p, True).wait_recv()
        if nxt:
            for p in a.others(nxt):
                self.small(hop + 1, p).start()

    def stage(self, k, i):
        if k == 4:
            for q in Item(self.at, i).others_b():
                self.bhop(i, q, True).wait_recv()
            self.pair(i).start()
            return
        first = z_first(i)

        @pl.when(first)
        def _():
            if k == 0:
                self.z_send(i, True)
            elif k == 1:
                self.z_pass(i, True)
            elif k == 2:
                self.z_wait(i, True)
                self.local(i).wait()
                self.a_send(i, True)
            else:
                self.a_wait(i, True)

        @pl.when(~first)
        def _():
            if k == 0:
                self.a_send(i, False)
            elif k == 1:
                self.a_wait(i, False)
                self.local(i).wait()
                self.z_send(i, False)
            elif k == 2:
                self.z_pass(i, False)
            else:
                self.z_wait(i, False)
        if k == 3:
            for q in Item(self.at, i).others_b():
                self.bhop(i, q).start()

    def ready(self, i):
        self.pair(i, True).wait_recv()

    def step(self, t):
        @pl.when((t + G_AHEAD < NI) & z_first(t + G_AHEAD))
        def _():
            self.z_send(t + G_AHEAD, True)
        for k in (1, 2, 3, 4):
            @pl.when((t >= G_LAG[k]) & (t < NI + G_LAG[k]))
            def _():
                self.stage(k, t - G_LAG[k])
        for hop in range(3):
            @pl.when(t == hop + 1)
            def _():
                self.small_step(hop)

    def finish(self):
        a = self.at
        for hop, here in ((0, "z"), (1, "x"), (2, "y")):
            for p in a.others(here):
                self.small(hop, p).wait_send()

        @pl.loop(0, NI)
        def _(i):
            self.pair(i).wait_send()
            t = Item(a, i)
            for q in t.others_b():
                self.bhop(i, q).wait_send()
            first = z_first(i)
            for f in (True, False):
                @pl.when(first if f else ~first)
                def _():
                    for q in t.others_a():
                        self.ahop(i, f, q).wait_send()
                    for p in self.line.others:
                        @pl.when(self.line.direct(p))
                        def _():
                            self.zhop(i, f, p).wait_send()

                    @pl.when(self.line.middle)
                    def _():
                        self.zrelay(i, f).wait_send()


E_U, E_P, E_Q = 8, 16, 18
SLOTS = 8
PS = 3
LAG = {1: 1, 2: 4, 3: 7, 4: 10, 5: 12}


class Reduce:
    def __init__(self, at, o_ref, ov_ref, r_refs, bufs, sems, scale):
        self.at, self.out, self.ov, self.scale = at, o_ref, ov_ref, scale
        self.h0, self.hb, self.ha, self.hz, self.hx = r_refs
        (self.p, self.a1, self.a2, self.a3, self.a4, self.l0, self.lb, self.la, self.lz, self.lx,
         self.v0, self.v1, self.v2, self.v3, self.w0, self.w1, self.w2, self.w3) = bufs
        (self.s0, self.r0, self.s_b, self.r_b, self.s_a, self.r_a, self.s_z, self.r_z, self.s_x, self.r_x, self.s4, self.r4,
         self.ls, self.os, self.vs, self.vr) = sems
        self.RH = self.a4.shape[1]
        self.half = ds(at.c * self.RH, self.RH)
        self.other = ds((1 - at.c) * self.RH, self.RH)
        self.line = Line(at)

    @staticmethod
    def recv_shapes(n, R, CB):
        nz, m, nx = torus(n)
        RH = R // 2
        S = lambda *s: jax.ShapeDtypeStruct(s, F32)
        return [S(NI, nz, m, m, RH, CB), S(NI, m, nz, m, RH, CB), S(NI, m, nz, RH, CB), S(NI, nz, m, RH, CB), S(NI, m, RH, CB)]

    @staticmethod
    def bufs(n, R, CB, VR):
        nz, m, nx = torus(n)
        assert nx == m
        RH = R // 2
        V = lambda *s: pltpu.VMEM(s, F32)
        return [V(PS, nz, m, m, R, CB), V(4, nz, m, m, RH, CB), V(SLOTS, nz, m, RH, CB), V(SLOTS, nz, RH, CB), V(SLOTS, RH, CB),
                V(nz, m, m, RH, CB), V(m, nz, m, RH, CB), V(m, nz + 1, RH, CB), V(nz, m + 1, RH, CB), V(m + 1, RH, CB),
                V(nz, m, m, VR, 128), V(nz, m, m, VR, 128), V(nz, m, VR, 128), V(nz, VR, 128),
                V(nz, m, m, VR, 128), V(m, nz, m, VR, 128), V(m, nz, VR, 128), V(nz, VR, 128)]

    @staticmethod
    def sems(n):
        nz, m, nx = torus(n)
        return [DMA((NI,)), DMA((NI,)), DMA((NI, m)), DMA((NI, m)), DMA((NI, m)), DMA((NI, m)),
                DMA((NI, nz)), DMA((NI, nz)), DMA((NI,)), DMA((NI,)), DMA((NI,)), DMA((NI,)),
                DMA((8, nz)), DMA((NI,)), DMA((4, nz)), DMA((4, nz))]

    def hop0(self, i):
        return remote(self.p.at[i % PS, :, :, :, self.other], self.h0.at[i], self.s0.at[i], self.r0.at[i], self.at.dev(c=1 - self.at.c))

    def bhop(self, i, q, recv=False):
        t = Item(self.at, i)
        o = q if recv else t.b
        return remote(self.a1.at[i % 4, :, :, q], self.hb.at[i, o], self.s_b.at[i, q], self.r_b.at[i, o], t.along_b(q))

    def ahop(self, i, last, q, recv=False):
        t, sl = Item(self.at, i), i % SLOTS
        o = q if recv else t.a
        sems = (self.s_a.at[i, q], self.r_a.at[i, o], t.along_a(q))
        if last:
            return remote(self.a2.at[sl, :, q], self.ha.at[i, o], *sems)
        return remote(self.a3.at[sl, q], self.ha.at[i, o, 0], *sems)

    def zhop(self, i, last, p, recv=False):
        sl = i % SLOTS
        o = p if recv else self.at.z
        sems = (self.s_z.at[i, p], self.r_z.at[i, o], self.at.dev(z=p))
        if last:
            return remote(self.a3.at[sl, p], self.hz.at[i, o, 0], *sems)
        return remote(self.a2.at[sl, p], self.hz.at[i, o], *sems)

    def zrelay(self, i, last):
        sl, e = i % SLOTS, self.line.end
        sems = (self.s_x.at[i], self.r_x.at[i], self.at.dev(z=self.line.relay))
        if last:
            return remote(self.a3.at[sl, e], self.hx.at[i, 0], *sems)
        return remote(self.a2.at[sl, e], self.hx.at[i], *sems)

    def last(self, i, f):
        src, rows, other = self.a4.at[i % SLOTS], self.at.c * self.RH, (1 - self.at.c) * self.RH
        for here, place in self.out(i):
            @pl.when(here)
            def _():
                s, r, dev = self.s4.at[i], self.r4.at[i], self.at.dev(c=1 - self.at.c)
                f(lambda: remote(src, place(rows), s, r, dev), lambda: remote(src, place(other), s, r, dev),
                  lambda: pltpu.make_async_copy(src, place(rows), self.os.at[i]))

    def copy(self, src, dst, k, q=0):
        return pltpu.make_async_copy(src, dst, self.ls.at[k, q])

    def load_a(self, i, last, q):
        nz = self.at.NZ
        return self.copy(self.ha.at[i, q], self.la.at[q, 0:nz], 2, q) if last else self.copy(self.ha.at[i, q, 0], self.la.at[q, nz], 5, q)

    def load_z(self, i, last, p):
        m = self.at.NX
        return self.copy(self.hz.at[i, p, 0], self.lz.at[p, m], 3, p) if last else self.copy(self.hz.at[i, p], self.lz.at[p, 0:m], 6, p)

    def load_x(self, i, last):
        m = self.at.NX
        return self.copy(self.hx.at[i, 0], self.lx.at[m], 4) if last else self.copy(self.hx.at[i], self.lx.at[0:m], 7)

    def from_z(self, f):
        for p in self.line.others:
            @pl.when(self.line.direct(p))
            def _():
                f(p)

    def z_send(self, i, last):
        for p in self.line.others:
            @pl.when(self.line.direct(p) & ~(self.line.middle & (p == self.line.far)))
            def _():
                self.zhop(i, last, p).start()

        @pl.when(~self.line.middle)
        def _():
            self.zrelay(i, last).start()

    def z_sent(self, i, last):
        for p in self.line.others:
            @pl.when(self.line.direct(p))
            def _():
                self.zhop(i, last, p).wait_send()

        @pl.when(~self.line.middle)
        def _():
            self.zrelay(i, last).wait_send()

    def a_sent(self, i, last):
        for q in Item(self.at, i).others_a():
            self.ahop(i, last, q).wait_send()

    def by_type(self, i, f):
        last = z_last(i)
        for v in (True, False):
            @pl.when(last if v else ~last)
            def _():
                f(v)

    def send(self, i):
        self.hop0(i).start()

    def sends_done(self, k, i):
        if k == 1:
            for q in Item(self.at, i).others_b():
                self.bhop(i, q).wait_send()
        elif k == 2:
            self.by_type(i, lambda last: self.a_sent(i, True) if last else self.z_sent(i, False))
        elif k == 3:
            self.by_type(i, lambda last: self.z_sent(i, True) if last else self.a_sent(i, False))
        else:
            def f(to, back, own):
                to().wait_send()
                own().wait()
            self.last(i, f)

    def free(self, k, i):
        n = 4 if k == 1 else SLOTS

        @pl.when(i >= n)
        def _():
            self.sends_done(k, i - n)

    def arrive(self, k, i):
        t = Item(self.at, i)
        if k == 1:
            self.hop0(i).wait_recv()
            self.copy(self.h0.at[i], self.l0, 0).start()
        elif k == 2:
            for q in t.others_b():
                self.bhop(i, q, True).wait_recv()
                self.copy(self.hb.at[i, q], self.lb.at[q], 1, q).start()
        else:
            def f(last):
                step = {3: "a", 4: "x", 5: "z"}[k] if last else {3: "x", 4: "z", 5: "a"}[k]
                if step == "a":
                    for q in t.others_a():
                        self.ahop(i, last, q, True).wait_recv()
                        self.load_a(i, last, q).start()
                elif step == "x":
                    @pl.when(self.line.middle)
                    def _():
                        self.zrelay(i, last).wait_recv()
                        self.load_x(i, last).start()
                else:
                    def g(p):
                        self.zhop(i, last, p, True).wait_recv()
                        self.load_z(i, last, p).start()
                    self.from_z(g)
            self.by_type(i, f)

    def done(self, i, value):
        self.free(5, i)
        self.a4[i % SLOTS] = value * self.scale

        def f(to, back, own):
            to().start()
            own().start()
        self.last(i, f)

    def process(self, k, i):
        at, sl, t = self.at, i % SLOTS, Item(self.at, i)
        nz, m = at.NZ, at.NX
        if k == 1:
            self.free(1, i)
            self.copy(self.h0.at[i], self.l0, 0).wait()

            @pl.loop(0, nz)
            def _(z):
                for y in range(m):
                    for x in range(m):
                        self.a1[i % 4, z, y, x] = self.p[i % PS, z, y, x, self.half] + self.l0[z, y, x]
            for q in t.others_b():
                self.bhop(i, q).start()
        elif k == 2:
            self.free(2, i)
            for q in t.others_b():
                self.copy(self.hb.at[i, q], self.lb.at[q], 1, q).wait()

            @pl.loop(0, nz)
            def _(z):
                for a in range(m):
                    own = self.a1[i % 4, z, a, t.b]
                    for q in t.others_b():
                        own = own + self.lb[q, z, a]
                    self.a2[sl, z, a] = own

            def f(last):
                if last:
                    for q in t.others_a():
                        self.ahop(i, True, q).start()
                else:
                    self.z_send(i, False)
            self.by_type(i, f)
        else:
            if k == 3:
                pass

            def f(last):
                step = {3: "a", 4: "x", 5: "z"}[k] if last else {3: "x", 4: "z", 5: "a"}[k]
                if step == "a":
                    for q in t.others_a():
                        self.load_a(i, last, q).wait()
                    if last:
                        self.free(3, i)

                        @pl.loop(0, nz)
                        def _(z):
                            own = self.a2[sl, z, t.a]
                            for q in t.others_a():
                                own = own + self.la[q, z]
                            self.a3[sl, z] = own
                        self.z_send(i, True)
                    else:
                        own = self.a3[sl, t.a]
                        for q in t.others_a():
                            own = own + self.la[q, nz]
                        self.done(i, own)
                elif step == "x":
                    @pl.when(self.line.middle)
                    def _():
                        self.load_x(i, last).wait()
                        far = self.line.far
                        if last:
                            self.a3[sl, far] += self.lx[m]
                        else:
                            for a in range(m):
                                self.a2[sl, far, a] += self.lx[a]
                        self.zhop(i, last, far).start()
                else:
                    self.from_z(lambda p: self.load_z(i, last, p).wait())
                    if not last:
                        self.free(3, i)
                    tmp = []
                    for a in range(1 if last else m):
                        own = self.a3[sl, at.z] if last else self.a2[sl, at.z, a]
                        for p in self.line.others:
                            own = own + jnp.where(self.line.direct(p), self.lz[p, m if last else a], 0.0)
                        tmp.append(own)
                    if last:
                        self.done(i, tmp[0])
                    else:
                        for a in range(m):
                            self.a3[sl, a] = tmp[a]
                        for q in t.others_a():
                            self.ahop(i, False, q).start()
            self.by_type(i, f)

    def step(self, t, f):
        for k in (5, 4, 3, 2, 1):
            i = t - LAG[k]

            @pl.when((i >= 0) & (i < NI))
            def _():
                f(k, i)

    def finish(self):
        for i in range(NI - PS, NI):
            self.hop0(i).wait_send()
        for k, n in ((1, 4), (2, SLOTS), (3, SLOTS), (5, SLOTS)):
            @pl.loop(NI - n, NI)
            def _(i):
                self.sends_done(k, i)

        for lo, hi in ((0, E_U), (E_P, NI)):
            @pl.loop(lo, hi)
            def _(i):
                self.last(i, lambda to, back, own: back().wait_recv())

    def vhop(self, k, q, recv=False):
        a = self.at
        if k == 0:
            return remote(self.v0, self.w0, self.vs.at[0, 0], self.vr.at[0, 0], a.dev(c=1 - a.c))
        me, src, dst, dev = {1: (a.y, self.v1.at[:, q], self.w1, a.dev(y=q)), 2: (a.x, self.v2.at[:, q], self.w2, a.dev(x=q)),
                             3: (a.z, self.v3.at[q], self.w3, a.dev(z=q))}[k]
        o = q if recv else me
        return remote(src, dst.at[o], self.vs.at[k, q], self.vr.at[k, o], dev)

    def vlines(self, k):
        return [0] if k == 0 else self.at.others({1: "y", 2: "x", 3: "z"}[k])

    def small(self, k):
        a = self.at
        if k:
            for q in self.vlines(k - 1):
                self.vhop(k - 1, q, True).wait_recv()
        if k == 1:
            self.v1[...] = self.v0[...] + self.w0[...]
        if k == 2:
            own = self.v1[:, a.y]
            for q in self.vlines(1):
                own = own + self.w1[q]
            self.v2[...] = own
        if k == 3:
            own = self.v2[:, a.x]
            for q in self.vlines(2):
                own = own + self.w2[q]
            self.v3[...] = own
        if k == 4:
            own = self.v3[a.z]
            for q in self.vlines(3):
                own = own + self.w3[q]
            self.ov[...] = own * self.scale
        else:
            for q in self.vlines(k):
                self.vhop(k, q).start()

    def small_finish(self):
        for k in range(4):
            for q in self.vlines(k):
                self.vhop(k, q).wait_send()


BF = jnp.bfloat16
NN = ((1,), (0,))
NT = ((1,), (1,))
TN = ((0,), (0,))
ROW_P, ROW_G1, ROW_S1, ROW_U, ROW_D, ROW_G2, ROW_S2 = 3, 4, 5, 6, 10, 11, 12
X_, C_, N_, A_ = 0, 1, 2, 3


def mx(a, b, dims=NN):
    return lax.dot_general(a, b, (dims, ((), ())), preferred_element_type=F32)


def split(v):
    hi = v.astype(BF)
    return hi, (v - hi.astype(F32)).astype(BF)


def split32(v):
    hi = v.astype(BF).astype(F32)
    return hi, v - hi


def three(ah, al, bh, bl, dims=NN):
    return mx(ah, bh, dims) + mx(ah, bl, dims) + mx(al, bh, dims)


def left_half(shape):
    return lax.broadcasted_iota(jnp.int32, shape, 1) < HD


def pack_hl0(v):
    m = left_half(v.shape)
    h, l = split32(v)
    hr, lr = pltpu.roll(h, HD, 1), pltpu.roll(l, HD, 1)
    zero = jnp.zeros_like(v)
    one = jnp.concatenate([jnp.where(m, h, lr), jnp.where(m, h, zero)], axis=1).astype(BF)
    two = jnp.concatenate([jnp.where(m, lr, h), jnp.where(m, zero, h)], axis=1).astype(BF)
    return one, two


def pack_hhl(v):
    m = left_half(v.shape)
    h, l = split32(v)
    hr = pltpu.roll(h, HD, 1)
    one = jnp.concatenate([jnp.where(m, h, hr), l], axis=1).astype(BF)
    two = jnp.concatenate([jnp.where(m, hr, h), l], axis=1).astype(BF)
    return one, two


def pack_hl(v):
    m = left_half(v.shape)
    h, l = split32(v)
    lr = pltpu.roll(l, HD, 1)
    return jnp.where(m, h, lr).astype(BF), jnp.where(m, lr, h).astype(BF)


def fold(one, two):
    m = left_half(one.shape)
    return jnp.where(m, one, two) + pltpu.roll(jnp.where(m, two, one), HD, 1)


def stack_t(v):
    t = v.T
    out = []
    for k in range(2):
        h, l = split32(t[k * HD:(k + 1) * HD])
        out.append(jnp.concatenate([h, l], axis=0).astype(BF))
    return out


def fold_t(one, two):
    return jnp.concatenate([one[:HD] + one[HD:], two[:HD] + two[HD:]], axis=0).T


def lanes(lane, R, pieces):
    out = None
    for i, (ref, c0) in enumerate(pieces):
        t = ref[:, c0 // 128 * 128:c0 // 128 * 128 + 128]
        shift = (i * R - c0) % 128
        t = pltpu.roll(t, shift, 1) if shift else t
        out = t if out is None else jnp.where(lane == i, t, out)
    return out


def cols(start, size):
    return pl.ds(pl.multiple_of(start, 128), size)


def forward_kernel(n, x_ref, qkv_w, proj_w, up_w, down_w, v_ref, seg_ref, len_ref,
                   out_ref, g_ref, gv_ref, lh_out, ws_out, qkv_out, p_out, sl_out, hat1_out, hat2_out, inv_out, vec_out,
                   lh, wf, ws, qkv, acc, n1, r2, slope, pst, bias, gvv, vec, w_ref, ld_sem, ws_sem, out_sem, p_sem, sl_sem, in_sem, *sems):
    at = Where(n)
    at.greet()
    L, D = x_ref.shape
    HB = D // 2
    ga = Gather(at, w_ref, g_ref, v_ref, gv_ref, sems)
    R = w_ref.shape[1]
    q = 128 // R
    parts = []
    for w in range(3):
        parts += [(2 * w + st, qkv_w.at[:, w * D + st * HB:w * D + (st + 1) * HB]) for st in range(2)]
    parts += [(6 + st, proj_w.at[:, st * HB:(st + 1) * HB]) for st in range(2)]
    parts += [(16 + 2 * j + st, down_w.at[j * R:(j + 1) * R, st * HB:(st + 1) * HB]) for j in range(4) for st in range(2)]
    parts = [pltpu.make_async_copy(src, w_ref.at[i], in_sem.at[k]) for k, (i, src) in enumerate(parts)]
    for part in parts:
        part.start()
    lane = lax.broadcasted_iota(jnp.int32, (R, 128), 1) // R
    for j in range(4):
        for k in range(D // 128):
            t = lanes(lane, R, [(up_w, (k * q + i) * 4 * R + j * R) for i in range(q)])
            w_ref[8 + 2 * j + k * 128 // HB, :, k * 128 % HB:k * 128 % HB + 128] = t
    for part in parts:
        part.wait()
    at.met()
    ga.begin()
    ga.begin_local()

    def lh_copy(s):
        return pltpu.make_async_copy(lh.at[s], lh_out.at[s], out_sem.at[s])

    RB = 128

    @pl.loop(0, L // RB)
    def _(r):
        rows = pl.ds(pl.multiple_of(r * RB, RB), RB)
        h, l = split(x_ref[rows])
        lh[X_, 0, rows] = h
        lh[X_, 1, rows] = l
        kpos = lax.broadcasted_iota(jnp.int32, (RB, L), 0) + r * RB
        qpos = lax.broadcasted_iota(jnp.int32, (RB, L), 1)
        own = seg_ref[:, rows].astype(F32)
        own = jnp.broadcast_to(own, (RB, RB)).T[:, :1]
        allowed = (own == seg_ref[...].astype(F32)) & ((kpos < len_ref[0]) | (kpos == qpos))
        bias[rows] = jnp.where(allowed, 0.0, MASKED)
    lh_copy(X_).start()
    @pl.loop(0, 2 + G_LAG[4])
    def _(t):
        ga.step(t)
    cp = pltpu.make_async_copy(gv_ref, gvv, ld_sem.at[0])
    cp.start()
    cp.wait()
    for k in range(D // 128):
        s = None
        for j in range(q):
            c = k * q + j
            blk = gvv[c // (at.NY * at.NX), (c // at.NX) % at.NY, c % at.NX]
            s = blk if s is None else s + blk
        vec[:, k * 128:(k + 1) * 128] = s
    vcp = pltpu.make_async_copy(vec, vec_out, out_sem.at[7])
    vcp.start()

    def load(w, st):
        return pltpu.make_async_copy(g_ref.at[2 * w + st], wf.at[st], ld_sem.at[st])

    def ws_copy(w, st):
        return pltpu.make_async_copy(ws.at[st], ws_out.at[w, st], ws_sem.at[st])

    def weights(w):
        for st in range(2):
            ga.ready(2 * w + st)
            load(w, st).start()

    def half(w, st, s):
        load(w, st).wait()

        @pl.when(w > 0)
        def _():
            ws_copy(w - 1, st).wait()

        @pl.loop(0, at.NZ)
        def _(z):
            for a in range(at.NY):
                for b in range(at.NX):
                    y, x = (a, b) if st == 0 else (b, a)
                    r0 = pl.multiple_of(((z * at.NY + y) * at.NX + x) * R, R)
                    h, l = split(wf[st, z, a, b])
                    ws[st, 0, pl.ds(r0, R)] = h
                    ws[st, 1, pl.ds(r0, R)] = l
        ws_copy(w, st).start()
        acc[...] = three(lh[s, 0], lh[s, 1], ws[st, 0], ws[st, 1])

    T0 = 2 + G_LAG[4]

    def qkv_copy(w):
        return pltpu.make_async_copy(qkv.at[w], qkv_out.at[w], out_sem.at[8 + w])

    @pl.loop(0, 3)
    def _(w):
        weights(w)
        f = jnp.where(w == 0, 1.0 / math.sqrt(HD), 1.0).astype(F32)
        for st in range(2):
            half(w, st, X_)
            b = vec[pl.ds(w, 1), st * HB:(st + 1) * HB]
            qkv[w, :, st * HB:(st + 1) * HB] = (acc[...] + b) * f
            ga.step(T0 + 2 * w + st)
        qkv_copy(w).start()

    def p_copy(p):
        return pltpu.make_async_copy(pst.at[p % 2], p_out.at[p], p_sem.at[p % 2])

    def attend(p):
        c = cols(p * 128, 128)
        qp, kp, vp = qkv[0, :, c], qkv[1, :, c], qkv[2, :, c]
        qs, ks, vt = pack_hhl(qp), pack_hl0(kp), stack_t(vp)

        @pl.when(p >= 2)
        def _():
            p_copy(p - 2).wait()
        res = []
        for k in range(2):
            s = mx(ks[k], qs[k], NT) + bias[...]
            e = jnp.exp(s - jnp.max(s, axis=0, keepdims=True))
            e = e * (1.0 / jnp.sum(e, axis=0, keepdims=True))
            ph, pll = split(e)
            pst[p % 2, k, 0] = ph
            pst[p % 2, k, 1] = pll
            res.append(mx(vt[k], ph) + mx(vt[k], pll))
        p_copy(p).start()
        h, l = split(fold_t(*res))
        lh[C_, 0, :, c] = h
        lh[C_, 1, :, c] = l

    @pl.loop(0, H // 2)
    def _(p):
        attend(p)

        @pl.when(p % 4 != 3)
        def _():
            ga.step(T0 + 6 + p - p // 4)
    lh_copy(C_).start()

    weights(3)
    for st in range(2):
        half(3, st, C_)
        c = slice(st * HB, (st + 1) * HB)
        n1[:, c] = x_ref[:, c] + acc[...] + vec[ROW_P:ROW_P + 1, c]
    @pl.loop(T0 + 12, T0 + 13)
    def _(t):
        ga.step(t)

    def norm_rows(ref, k, hat_ref, rows):
        v = ref[rows]
        center = v - jnp.mean(v, axis=-1, keepdims=True)
        inverse = lax.rsqrt(jnp.mean(center * center, axis=-1, keepdims=True) + EPSILON)
        hat = center * inverse
        return hat, inverse

    @pl.loop(0, L // RB)
    def _(r):
        rows = pl.ds(pl.multiple_of(r * RB, RB), RB)
        hat, inverse = norm_rows(n1, 0, None, rows)
        r2[rows] = hat
        inv_out[rows, 0:128] = jnp.broadcast_to(inverse, (RB, 128))
        v = hat * vec[ROW_G1:ROW_G1 + 1] + vec[ROW_S1:ROW_S1 + 1]
        n1[rows] = v
        h, l = split(v)
        lh[N_, 0, rows] = h
        lh[N_, 1, rows] = l
    lh_copy(N_).start()
    hcp = pltpu.make_async_copy(r2, hat1_out, out_sem.at[11])
    hcp.start()

    def sl_copy(j, st):
        return pltpu.make_async_copy(slope.at[st], sl_out.at[j, st], sl_sem.at[st])

    @pl.loop(0, 4)
    def _(j):
        weights(4 + j)
        for st in range(2):
            half(4 + j, st, N_)
            c = slice(st * HB, (st + 1) * HB)

            @pl.when(j > 0)
            def _():
                sl_copy(j - 1, st).wait()
            b = vec[pl.ds(ROW_U + j, 1), c]

            @pl.loop(0, L // 64)
            def _(r):
                rows = pl.ds(pl.multiple_of(r * 64, 64), 64)
                u = acc[rows] + b
                phi = 0.5 * (1.0 + lax.erf(u * math.sqrt(0.5)))
                h, l = split(u * phi)
                lh[A_ + j, 0, rows, c] = h
                lh[A_ + j, 1, rows, c] = l
                slope[st, rows] = phi + u * jnp.exp(-0.5 * u * u) * (1.0 / math.sqrt(2.0 * math.pi))
            sl_copy(j, st).start()
            if st == 0:
                ga.step(T0 + 13 + j)
        lh_copy(A_ + j).start()

    hcp.wait()
    r2[...] = n1[...] + vec[ROW_D:ROW_D + 1]

    @pl.loop(0, 4)
    def _(j):
        weights(8 + j)
        for st in range(2):
            half(8 + j, st, A_ + j)
            r2[:, st * HB:(st + 1) * HB] += acc[...]

            @pl.when((j < 3) if st == 0 else (j == 1) | (j == 2))
            def _():
                ga.step(T0 + 17 + j + (j == 2).astype(jnp.int32) if st == 0 else T0 + 17 + 2 * j)

    @pl.loop(0, L // RB)
    def _(r):
        rows = pl.ds(pl.multiple_of(r * RB, RB), RB)
        hat, inverse = norm_rows(r2, 1, None, rows)
        r2[rows] = hat
        inv_out[rows, 128:256] = jnp.broadcast_to(inverse, (RB, 128))
        out_ref[rows] = hat * vec[ROW_G2:ROW_G2 + 1] + vec[ROW_S2:ROW_S2 + 1]
    hcp2 = pltpu.make_async_copy(r2, hat2_out, out_sem.at[11])
    hcp2.start()
    vcp.wait()
    for s in range(7):
        lh_copy(s).wait()
    for w in range(3):
        qkv_copy(w).wait()
    for p in (H // 2 - 2, H // 2 - 1):
        p_copy(p).wait()
    for st in range(2):
        sl_copy(3, st).wait()
        ws_copy(NW - 1, st).wait()
    hcp2.wait()
    ga.finish()


def forward(n, x, qkv, proj, up, down, v, seg, length):
    nz, ny, nx = torus(n)
    R, HB = proj.shape[0], proj.shape[1] // 2
    L, D = x.shape
    S = lambda shape, t=F32: jax.ShapeDtypeStruct(shape, t)
    V = pltpu.VMEM
    ANY = pl.BlockSpec(memory_space=pl.ANY)
    VM = pl.BlockSpec(memory_space=pltpu.VMEM)
    return pl.pallas_call(
        functools.partial(forward_kernel, n),
        out_shape=[S((L, D)), S((NI, nz, ny, nx, R, HB)), S((nz, ny, nx) + v.shape), S((7, 2, L, D), BF),
                   S((NW, 2, 2, D, HB), BF), S((3, L, D)), S((H // 2, 2, 2, L, L), BF), S((4, 2, L, HB)),
                   S((L, D)), S((L, D)), S((L, 256)), S((v.shape[0], D))],
        in_specs=[VM, ANY, ANY, VM, ANY, VM, VM, pl.BlockSpec(memory_space=pltpu.SMEM)],
        out_specs=[VM] + [ANY] * 9 + [VM, ANY],
        scratch_shapes=[V((7, 2, L, D), BF), V((2, nz, ny, nx, R, HB), F32), V((2, 2, D, HB), BF), V((3, L, D), F32),
                        V((L, HB), F32), V((L, D), F32), V((L, D), F32), V((2, L, HB), F32), V((2, 2, 2, L, L), BF),
                        V((L, L), F32), V((nz, ny, nx) + v.shape, F32), V((v.shape[0], D), F32), V((NI, R, HB), F32),
                        DMA((2,)), DMA((2,)), DMA((12,)), DMA((2,)), DMA((2,)), DMA((16,))] + Gather.sems(n),
        compiler_params=pltpu.CompilerParams(collective_id=0, has_side_effects=True, vmem_limit_bytes=63 * 2**20),
        name="forward",
    )(x, qkv, proj, up, down, v, seg, length)


E_PAIR = 9
R_R2, R_U, R_R1, R_Q = 0, 1, 5, 6


def backward_kernel(n, scale, ct_ref, hat2_ref, hat1_ref, inv_ref, lh_ref, ws_ref, qkv_ref, p_ref, sl_ref, vec,
                    dx_ref, qkv_o, proj_o, up_o, down_o, ov_ref, rhs_ref, h0, h1, h2, h3, h4,
                    lbuf, rbuf, wbuf, sbuf, pbuf, qbuf, dr2, du, dn1, fb, dst, small, uo,
                    l_sem, r_sem, w_sem, s_sem, p_sem, q_sem, f_sem, o_sem, d_sem, *rest):
    at = Where(n)
    at.greet()
    bufs, sems = rest[:18], rest[18:]
    L, D = dx_ref.shape
    HB = D // 2
    R = up_o.shape[0]
    RH = R // 2

    def places(e):
        block = lambda ref, r, c: ref.at[pl.ds(pl.multiple_of(r, 8), RH), cols(c, HB)]
        return [(e < E_U, lambda r: block(down_o, e // 2 * R + r, e % 2 * HB)),
                ((e >= E_U) & (e < E_P), lambda r: uo.at[jnp.clip(e - E_U, 0, 7), pl.ds(pl.multiple_of(r, 8), RH)]),
                ((e >= E_P) & (e < E_Q), lambda r: block(proj_o, r, e % 2 * HB)),
                (e >= E_Q, lambda r: block(qkv_o, r, (e - E_Q) % 3 * D + (e - E_Q) // 3 * HB))]

    rd = Reduce(at, places, ov_ref, (h0, h1, h2, h3, h4), bufs, sems, scale)
    RB = 128
    FB = D // at.NZ
    copy = pltpu.make_async_copy

    def f_load(src, k):
        return copy(src, fb.at[k], f_sem.at[k])

    def lhs_slot(e):
        return jnp.where(e < E_U, A_ + e // 2, jnp.where(e < E_P, N_, jnp.where(e < E_Q, C_, X_)))

    def rhs_slot(e):
        return jnp.where(e < E_U, R_R2, jnp.where(e < E_P, R_U + (e - E_U) // 2, jnp.where(e < E_Q, R_R1, R_Q + (e - E_Q) % 3)))

    def rhs_half(e):
        return jnp.where(e < E_Q, e % 2, (e - E_Q) // 3)

    def l_load(e):
        return copy(lh_ref.at[lhs_slot(e)], lbuf.at[e % 2], l_sem.at[e % 2])

    def r_load(e):
        return copy(rhs_ref.at[rhs_slot(e), :, :, cols(rhs_half(e) * HB, HB)], rbuf.at[e % 2], r_sem.at[e % 2])

    def w_load(e, k):
        pairs = jnp.where(e < E_U, jnp.where(e % 2 == 0, 8, 4) + e // 2, 3)
        w = jnp.where(e < E_Q, pairs, (e - E_Q) % 3)
        h = jnp.where(e < E_Q, k, (e - E_Q) // 3)
        return copy(ws_ref.at[w, h], wbuf.at[e % 2, k], w_sem.at[e % 2, k])

    def s_load(j):
        return copy(sl_ref.at[j], sbuf, s_sem)

    def p_load(p):
        return copy(p_ref.at[p], pbuf.at[p % 2], p_sem.at[p % 2])

    def q_load(p):
        return copy(qkv_ref.at[:, :, cols(p * 128, 128)], qbuf.at[p % 2], q_sem.at[p % 2])

    def rhs_store(src, slot, k):
        return copy(src, rhs_ref.at[slot], o_sem.at[k])

    f_load(ct_ref, 0).start()
    f_load(hat2_ref, 1).start()
    l_load(0).start()
    for k in range(2):
        w_load(0, k).start()
    s_load(0).start()
    small[...] = jnp.zeros_like(small)
    f_load(ct_ref, 0).wait()
    f_load(hat2_ref, 1).wait()

    def norm_back(r, g, hat, inverse, gain, row_shift, row_gain):
        gg = g * gain
        small[row_shift:row_shift + 1] += jnp.sum(g, axis=0, keepdims=True)
        small[row_gain:row_gain + 1] += jnp.sum(g * hat, axis=0, keepdims=True)
        return inverse * (gg - jnp.mean(gg, -1, keepdims=True) - hat * jnp.mean(gg * hat, -1, keepdims=True))

    @pl.loop(0, L // RB)
    def _(r):
        rows = pl.ds(pl.multiple_of(r * RB, RB), RB)
        d = norm_back(r, fb[0, rows], fb[1, rows], inv_ref[rows, 128:129], vec[ROW_G2:ROW_G2 + 1], ROW_S2, ROW_G2)
        small[ROW_D:ROW_D + 1] += jnp.sum(d, axis=0, keepdims=True)
        dn1[rows] = d
        h, l = split(d)
        dr2[0, rows] = h
        dr2[1, rows] = l
    rhs_store(dr2, R_R2, 0).start()
    f_load(hat1_ref, 0).start()
    rhs_store(dr2, R_R2, 0).wait()
    r_load(0).start()
    at.met()

    def chunk_da(j, e):
        for k in range(2):
            w_load(e, k).wait()
        s_load(j).wait()

        @pl.when(j > 0)
        def _():
            rhs_store(du, R_U + j - 1, 1).wait()
        for k in range(4):
            b = slice(k * FB, (k + 1) * FB)
            v = three(dr2[0, :, :HB], dr2[1, :, :HB], wbuf[e % 2, 0, 0, b], wbuf[e % 2, 0, 1, b], NT) \
                + three(dr2[0, :, HB:], dr2[1, :, HB:], wbuf[e % 2, 1, 0, b], wbuf[e % 2, 1, 1, b], NT)
            half, off = (k * FB) // HB, (k * FB) % HB
            v = v * sbuf[half, :, off:off + FB]
            small[pl.ds(ROW_U + j, 1), b] = jnp.sum(v, axis=0, keepdims=True)
            h, l = split(v)
            du[0, :, b] = h
            du[1, :, b] = l
        rhs_store(du, R_U + j, 1).start()

        @pl.when(j < 3)
        def _():
            s_load(j + 1).start()

    def nt_into(ref, a, e, b):
        return ref[:, b] + three(a[0, :, :HB], a[1, :, :HB], wbuf[e % 2, 0, 0, b], wbuf[e % 2, 0, 1, b], NT) \
            + three(a[0, :, HB:], a[1, :, HB:], wbuf[e % 2, 1, 0, b], wbuf[e % 2, 1, 1, b], NT)

    def chunk_dn(e):
        for k in range(2):
            w_load(e, k).wait()
        for k in range(4):
            b = slice(k * FB, (k + 1) * FB)
            dn1[:, b] = nt_into(dn1, du, e, b)

    def chunk_norm():
        f_load(hat1_ref, 0).wait()

        @pl.loop(0, L // RB)
        def _(r):
            rows = pl.ds(pl.multiple_of(r * RB, RB), RB)
            d = norm_back(r, dn1[rows], fb[0, rows], inv_ref[rows, 0:1], vec[ROW_G1:ROW_G1 + 1], ROW_S1, ROW_G1)
            small[ROW_P:ROW_P + 1] += jnp.sum(d, axis=0, keepdims=True)
            dn1[rows] = d
            h, l = split(d)
            dr2[0, rows] = h
            dr2[1, rows] = l
        rhs_store(du, R_U + 3, 1).wait()
        rhs_store(dr2, R_R1, 0).start()

    def chunk_dc(e):
        for k in range(2):
            w_load(e, k).wait()
        for k in range(4):
            b = slice(k * FB, (k + 1) * FB)
            fb[1, :, b] = three(dr2[0, :, :HB], dr2[1, :, :HB], wbuf[e % 2, 0, 0, b], wbuf[e % 2, 0, 1, b], NT) \
                + three(dr2[0, :, HB:], dr2[1, :, HB:], wbuf[e % 2, 1, 0, b], wbuf[e % 2, 1, 1, b], NT)
        rhs_store(dr2, R_R1, 0).wait()

    def d_store(p, k):
        return copy(dst.at[p % 2, k], rhs_ref.at[R_Q + k, :, :, cols(p * 128, 128)], d_sem.at[p % 2, k])

    def chunk_pair(p):
        c = cols(p * 128, 128)
        s = p % 2
        p_load(p).wait()
        q_load(p).wait()

        @pl.when(p < H // 2 - 1)
        def _():
            p_load(p + 1).start()
            q_load(p + 1).start()
        qp, kp, vp, dc = qbuf[s, 0], qbuf[s, 1], qbuf[s, 2], fb[1, :, c]
        va, da, kt, qx, dx = pack_hl0(vp), pack_hhl(dc), stack_t(kp), pack_hl(qp), pack_hl(dc)
        dq, dk, dv = [], [], []
        for k in range(2):
            dp = mx(va[k], da[k], NT)
            ph, pll = pbuf[s, k, 0], pbuf[s, k, 1]
            pf = ph.astype(F32) + pll.astype(F32)
            t = pf * dp
            t = t - pf * jnp.sum(t, axis=0, keepdims=True)
            sh, sll = split(t)
            dk.append(mx(sh, qx[k]) + mx(sll, qx[k]))
            dv.append(mx(ph, dx[k]) + mx(pll, dx[k]))
            dq.append(mx(kt[k], sh) + mx(kt[k], sll))
        out = (fold_t(*dq) * (1.0 / math.sqrt(HD)), fold(*dk), fold(*dv))

        @pl.when(p >= 2)
        def _():
            for k in range(3):
                d_store(p - 2, k).wait()
        for k in range(3):
            small[k:k + 1, c] = jnp.sum(out[k], axis=0, keepdims=True)
            h, l = split(out[k])
            dst[s, k, 0] = h
            dst[s, k, 1] = l
            d_store(p, k).start()

    def chunk_dx(e):
        w_load(e, 0).wait()
        for k in range(4):
            b = slice(k * FB, (k + 1) * FB)
            dn1[:, b] += three(rbuf[e % 2, 0], rbuf[e % 2, 1], wbuf[e % 2, 0, 0, b], wbuf[e % 2, 0, 1, b], NT)

    @pl.loop(0, NI + LAG[5])
    def _(e):
        @pl.when(e < NI)
        def _():
            l_load(e).wait()
            r_load(e).wait()

            @pl.when(e >= PS)
            def _():
                rd.hop0(e - PS).wait_send()

            @pl.loop(0, at.NZ)
            def _(z):
                b = cols(z * FB, FB)
                v = three(lbuf[e % 2, 0, :, b], lbuf[e % 2, 1, :, b], rbuf[e % 2, 0], rbuf[e % 2, 1], TN)
                odd = e % 2 == 1
                for y in range(at.NY):
                    for x in range(at.NX):
                        k = (y * at.NX + x) * R
                        rd.p[e % PS, z, jnp.where(odd, x, y), jnp.where(odd, y, x)] = v[k:k + R]
            rd.send(e)

            @pl.when(e < NI - 1)
            def _():
                l_load(e + 1).start()
                r_load(e + 1).start()

            @pl.when((e < E_U) | ((e >= E_Q - 1) & (e < NI - 1)))
            def _():
                w_load(e + 1, 0).start()

            @pl.when(e < E_U)
            def _():
                w_load(e + 1, 1).start()
        rd.step(e, rd.arrive)

        @pl.when((e < E_U) & (e % 2 == 0))
        def _():
            chunk_da(e // 2, e)

        @pl.when((e < E_U) & (e % 2 == 1))
        def _():
            chunk_dn(e)

        @pl.when(e == E_U - 1)
        def _():
            chunk_norm()

        @pl.when(e == E_U)
        def _():
            p_load(0).start()
            q_load(0).start()
            chunk_dc(e)

        @pl.when((e >= E_PAIR) & (e < E_PAIR + H // 2))
        def _():
            chunk_pair(e - E_PAIR)

        @pl.when(e == E_PAIR + H // 2)
        def _():
            for p in (H // 2 - 2, H // 2 - 1):
                for k in range(3):
                    d_store(p, k).wait()
            for z in range(at.NZ):
                for y in range(at.NY):
                    for x in range(at.NX):
                        g = ((z * at.NY + y) * at.NX + x) * 2 * rd.RH // 128
                        rd.v0[z, y, x] = small[:, g * 128:(g + 1) * 128]

        for k in range(5):
            @pl.when(e == E_PAIR + H // 2 + k)
            def _():
                rd.small(k)

        @pl.when((e >= E_Q) & (e < NI))
        def _():
            chunk_dx(e)

        @pl.when(e == NI - 1)
        def _():
            copy(dn1, dx_ref, o_sem.at[0]).start()
        rd.step(e, rd.process)

        @pl.when(e == E_P + LAG[5] + 1)
        def _():
            @pl.loop(E_U, E_P)
            def _(i):
                def f(to, back, own):
                    back().wait_recv()
                rd.last(i, f)
    copy(dn1, dx_ref, o_sem.at[0]).wait()
    rd.finish()
    lane = lax.broadcasted_iota(jnp.int32, (R, 128), 1) // R
    for t in range(4 * D // 128):
        pieces = []
        for i in range(128 // R):
            f0 = t * 128 + i * R
            chip, j = f0 // (4 * R), f0 % (4 * R) // R
            pieces.append((uo.at[2 * j + chip * R // HB], chip * R % HB))
        up_o[:, t * 128:(t + 1) * 128] = lanes(lane, R, pieces)
    rd.small_finish()


def backward(n, R, scale, ct, hat2, hat1, inv, lh, ws, qkv, p, sl, vec):
    L, D = ct.shape
    HB = D // 2
    VR = vec.shape[0]
    S = lambda shape, t=F32: jax.ShapeDtypeStruct(shape, t)
    V = pltpu.VMEM
    ANY = pl.BlockSpec(memory_space=pl.ANY)
    VM = pl.BlockSpec(memory_space=pltpu.VMEM)
    return pl.pallas_call(
        functools.partial(backward_kernel, n, scale),
        out_shape=[S((L, D)), S((R, 3 * D)), S((R, D)), S((R, 4 * D)), S((4 * R, D)), S((VR, 128)), S((9, 2, L, D), BF)] + Reduce.recv_shapes(n, R, HB),
        in_specs=[ANY, ANY, ANY, VM, ANY, ANY, ANY, ANY, ANY, VM],
        out_specs=[ANY, ANY, ANY, VM, ANY, VM] + [ANY] * 6,
        scratch_shapes=[V((2, 2, L, D), BF), V((2, 2, L, HB), BF), V((2, 2, 2, D, HB), BF), V((2, L, HB), F32),
                        V((2, 2, 2, L, L), BF), V((2, 3, L, 128), F32), V((2, L, D), BF), V((2, L, D), BF), V((L, D), F32),
                        V((2, L, D), F32), V((2, 3, 2, L, 128), BF), V((VR, D), F32), V((8, R, HB), F32),
                        DMA((2,)), DMA((2,)), DMA((2, 2)), DMA(()), DMA((2,)), DMA((2,)), DMA((2,)), DMA((2,)), DMA((2, 3))]
        + Reduce.bufs(n, R, HB, VR) + Reduce.sems(n),
        compiler_params=pltpu.CompilerParams(collective_id=1, has_side_effects=True, vmem_limit_bytes=63 * 2**20),
        name="backward",
    )(ct, hat2, hat1, inv, lh, ws, qkv, p, sl, vec)[:6]


VROWS = 16


def lane(R):
    return (lax.axis_index("shard") * R) % 128


def pack_small(before, up_bias, after):
    R = before[0].shape[0]
    rows = jnp.concatenate(before + [up_bias] + after + [jnp.zeros((3 * R,), F32)]).reshape(VROWS, R)
    here = lax.broadcasted_iota(jnp.int32, (VROWS, 128), 1) // R == lax.axis_index("shard") % (128 // R)
    return jnp.where(here, jnp.concatenate([rows] * (128 // R), axis=1), 0.0)


def shards(n, tokens, segment_ids, valid_lengths, qkv_weight, query_bias, value_bias, proj_weight, proj_bias, first_gain,
           first_shift, up_weight, up_bias, down_weight, down_bias, second_gain, second_shift, cotangent):
    amount, length, D = tokens.shape
    R = proj_weight.shape[0]
    x = tokens.reshape(amount * length, D)
    vsh = pack_small([query_bias, jnp.zeros_like(query_bias), value_bias, proj_bias, first_gain, first_shift], up_bias,
                     [down_bias, second_gain, second_shift])
    out, g, gv, lh, ws, qkv, pr, sl, hat1, hat2, inv, v = forward(
        n, x, qkv_weight, proj_weight, up_weight, down_weight, vsh, segment_ids, valid_lengths)
    scale = 1.0 / math.sqrt(amount * length * n * lax.axis_size("rep"))
    dx, gqkv, gproj, gup, gdown, ov = backward(n, R, scale, cotangent.reshape(amount * length, D), hat2, hat1, inv, lh, ws, qkv, pr, sl, v)
    s = lax.dynamic_slice(ov, (0, lane(R)), (VROWS, R))
    return (out.reshape(amount, length, D), dx.reshape(amount, length, D), gqkv, s[0], s[2], gproj, s[3], s[4], s[5], gup,
            s[6:10].reshape(4 * R), gdown, s[10], s[11], s[12])


def solution(mesh):
    n = mesh.shape["shard"]
    one, two, seq = P("shard"), P("shard", None), P(("shard", "rep"), None, None)
    return jax.shard_map(
        functools.partial(shards, n),
        mesh=mesh,
        in_specs=(seq, P(("shard", "rep"), None), P(("shard", "rep")), two, one, one, two, one, one, one, two, one, two, one, one, one, seq),
        out_specs=(seq, seq, two, one, one, two, one, one, one, two, one, two, one, one, one),
        check_vma=False,
    )
```
